32 devices in a mesh: section: 2 (over core), dp: 4 (over y, x), tensor: 4 (over z).
Axes of the slice: x: 2, y: 2, z: 4, core: 2. Of those that a mesh axis runs over, the one named last changes fastest.
Arguments:
- inputs: bfloat16 [2, 1536, 1536], P(None, ('dp', 'tensor')), may hold values from -7 to 7
- cotangent: bfloat16 [2, 1536, 1536], P(None, ('dp', 'tensor')), may hold values from -6 to 6
- seq_lengths: int32 [4, 2, 4], P('dp'), may hold values from 0 to 384, as said below
- gain_attn: bfloat16 [2, 1536], P('section'), may hold values from 0.5 to 1.5
- w_query: bfloat16 [2, 1536, 1536], P('section', None, 'tensor'), may hold values from -0.15309311 to 0.15309311
- w_key: bfloat16 [2, 1536, 768], P('section', None, 'tensor'), may hold values from -0.15309311 to 0.15309311
- w_value: bfloat16 [2, 1536, 768], P('section', None, 'tensor'), may hold values from -0.15625 to 0.15625
- w_out: bfloat16 [2, 1536, 1536], P('section', 'tensor'), may hold values from -0.625 to 0.625
- gain_ffn: bfloat16 [2, 1536], P('section'), may hold values from 0.5 to 1.5
- w_gate: bfloat16 [2, 1536, 4096], P('section', None, 'tensor'), may hold values from -0.15625 to 0.15625
- w_up: bfloat16 [2, 1536, 4096], P('section', None, 'tensor'), may hold values from -0.15625 to 0.15625
- w_down: bfloat16 [2, 4096, 1536], P('section', 'tensor'), may hold values from -0.09375 to 0.09375
Outputs:
- section_out: bfloat16 [2, 2, 1536, 1536], P('section', None, ('dp', 'tensor'))
- in_grad: bfloat16 [2, 2, 1536, 1536], P('section', None, ('dp', 'tensor'))
- grad_gain_attn: float32 [2, 1536], P('section')
- grad_w_query: float32 [2, 1536, 1536], P('section', None, 'tensor')
- grad_w_key: float32 [2, 1536, 768], P('section', None, 'tensor')
- grad_w_value: float32 [2, 1536, 768], P('section', None, 'tensor')
- grad_w_out: float32 [2, 1536, 1536], P('section', 'tensor')
- grad_gain_ffn: float32 [2, 1536], P('section')
- grad_w_gate: float32 [2, 1536, 4096], P('section', None, 'tensor')
- grad_w_up: float32 [2, 1536, 4096], P('section', None, 'tensor')
- grad_w_down: float32 [2, 4096, 1536], P('section', 'tensor')
The draws below stay inside these ranges and needn't reach their ends.
Inputs may be any that keep to these rules, and one draw needn't show every extreme that they name: seq_lengths[d, m, :] are the lengths of the sequences of block (m, d) in order, zeros for unused entries; their sum is at most 384, and in every draw some block holds a single sequence of exactly 384 rows.
All inputs are finite; a program needn't handle non-finite values.
Results may differ from the reference program's by a relative error of at most 0.022.
Values may be sent and summed in bfloat16 or wider, within the bound.
A program may use at most 192 MiB of HBM per device.

```python
import jax
import jax.numpy as jnp
from jax import lax

D = 1536
HEADS = 16
KV_HEADS = 8
HEAD = 96
FF = 4096
MB_ROWS = 384
MICRO = 2
SLOTS = 4
ROWS = 1536
N_SECTION = 2
N_DP = 4


def draw_w_query(key, part):
    base = jax.random.normal(jax.random.fold_in(key, 7), (N_SECTION, D, HEADS * HEAD), jnp.float32)
    return (jnp.clip(base, -6.0, 6.0) * D ** (-0.5)).astype(jnp.bfloat16)


def draw_w_key(key, part):
    noise = jax.random.normal(jax.random.fold_in(key, 11), (N_SECTION, D, KV_HEADS * HEAD), jnp.float32)
    return (jnp.clip(noise, -6.0, 6.0) * D ** (-0.5)).astype(jnp.bfloat16)


def draw_inputs(key, part):
    base = jnp.clip(jax.random.normal(jax.random.fold_in(key, 3), (MICRO, MB_ROWS * N_DP, D), jnp.float32), -6.0, 6.0)
    return base.astype(jnp.bfloat16)


def draw_seq_lengths(key, part):
    block_count = N_DP * MICRO
    raw = jax.random.randint(jax.random.fold_in(key, 21), (block_count, SLOTS), MB_ROWS // 8, MB_ROWS // 2 + 1)
    live_count = jax.random.randint(jax.random.fold_in(key, 22), (block_count, 1), 1, SLOTS + 1)
    raw = jnp.where(jnp.arange(SLOTS)[None, :] < live_count, raw, 0)
    forced = jax.random.randint(jax.random.fold_in(key, 23), (), 0, block_count)
    first_col = jnp.where(jnp.arange(block_count) == forced, MB_ROWS, raw[:, 0])
    raw = jnp.concatenate([first_col[:, None], raw[:, 1:]], axis=1)
    before = jnp.cumsum(raw, axis=1) - raw
    room = jnp.maximum(MB_ROWS - before, 0)
    return jnp.minimum(raw, room).reshape(N_DP, MICRO, SLOTS).astype(jnp.int32)


def block_scale(rng, dims, pieces, smallest, largest):
    gain = 1.0
    for axis_at, parts in pieces:
        heights = jax.random.uniform(jax.random.fold_in(jax.random.fold_in(rng, 6), axis_at), (parts,), jnp.float32, smallest / len(pieces), largest / len(pieces))
        gain = gain * jnp.repeat(jnp.exp(heights), dims[axis_at] // parts).reshape((-1,) + (1,) * (len(dims) - 1 - axis_at))
    return gain


def gaussian(key, shape, scale, limit, cuts=(), held_as=jnp.bfloat16):
    result = jax.random.normal(key, shape, jnp.float32) * scale
    if len(cuts) > 0:
        result = block_scale(key, shape, cuts, -0.22, 0.18) * result
    return jnp.clip(result, min=-limit, max=limit).astype(held_as)


def setup_inputs(seed: int = 0) -> dict:
    splits = jax.random.split(jax.random.key(seed), 13)
    return {
        "inputs": draw_inputs(jax.random.fold_in(splits[12], 71), 0),
        "cotangent": gaussian(splits[1], (MICRO, ROWS, D), 1.0, 6.0, ((1, 16),)),
        "seq_lengths": draw_seq_lengths(jax.random.fold_in(splits[12], 71), 0),
        "gain_attn": jnp.clip(1.0 + 0.1 * jax.random.normal(splits[3], (N_SECTION, D), jnp.float32), 0.5, 1.5).astype(jnp.bfloat16),
        "w_query": draw_w_query(jax.random.fold_in(splits[12], 71), 0),
        "w_key": draw_w_key(jax.random.fold_in(splits[12], 71), 0),
        "w_value": gaussian(splits[6], (N_SECTION, D, KV_HEADS * HEAD), D ** -0.5, 0.15625, ((0, 2), (2, 4))),
        "w_out": gaussian(splits[7], (N_SECTION, HEADS * HEAD, D), (HEADS * HEAD // 16) ** -0.5, 0.625, ((0, 2), (1, 4))),
        "gain_ffn": jnp.clip(1.0 + 0.1 * jax.random.normal(splits[8], (N_SECTION, D), jnp.float32), 0.5, 1.5).astype(jnp.bfloat16),
        "w_gate": gaussian(splits[9], (N_SECTION, D, FF), D ** -0.5, 0.15625, ((0, 2), (2, 4))),
        "w_up": gaussian(splits[10], (N_SECTION, D, FF), D ** -0.5, 0.15625, ((0, 2), (2, 4))),
        "w_down": gaussian(splits[11], (N_SECTION, FF, D), FF ** -0.5, 0.09375, ((0, 2), (1, 4))),
    }


eps = 1e-05
rope_base = 100000.0
neg_fill = -1e+30

@jax.custom_vjp
def low(v):
    return lax.optimization_barrier(v.astype(jnp.bfloat16)).astype(jnp.float32)

@jax.custom_vjp
def low_back(v):
    return v

def low_keep(v):
    return (low(v), None)

def low_pass(kept, grad):
    return (grad,)

def back_keep(v):
    return (v, None)

def back_low(kept, grad):
    return (low(grad),)
low.defvjp(low_keep, low_pass)
low_back.defvjp(back_keep, back_low)

def rms_scale(values):
    return lax.rsqrt(lax.optimization_barrier(jnp.mean(values * values, axis=-1, keepdims=True)) + eps)

def dot_high(left, right):
    return jnp.dot(left, right, precision=lax.Precision.HIGHEST)

def rotate(values, position, direction):
    half_size = values.shape[-1] // 2
    inverse = rope_base ** (-jnp.arange(half_size, dtype=jnp.float32) * 2.0 / values.shape[-1])
    angle = position.astype(jnp.float32)[:, None] * inverse[None, :]
    cosine = jnp.cos(angle)[:, None, :]
    sine = direction * jnp.sin(angle)[:, None, :]
    first = values[..., :half_size]
    second = values[..., half_size:]
    return jnp.concatenate([first * cosine - second * sine, second * cosine + first * sine], axis=-1)

def segment_info(lengths_row, row_count):
    slot_count = lengths_row.shape[0]
    seq_ends = jnp.cumsum(lengths_row).astype(jnp.int32)
    seq_starts = jnp.concatenate([seq_ends - lengths_row.astype(jnp.int32), seq_ends[-1:]]).astype(jnp.int32)
    row_index = jnp.arange(row_count, dtype=jnp.int32)
    segment = lax.optimization_barrier(jnp.sum((row_index[:, None] >= seq_ends[None, :]).astype(jnp.int32), axis=1)).astype(jnp.int32)
    pick = segment[:, None] == jnp.arange(slot_count + 1, dtype=jnp.int32)[None, :]
    position = (row_index - lax.optimization_barrier(jnp.sum(jnp.where(pick, seq_starts[None, :], 0), axis=1))).astype(jnp.int32)
    allowed = (segment[:, None] == segment[None, :]) & (row_index[None, :] <= row_index[:, None]) & (segment[:, None] < slot_count)
    allowed = allowed | (row_index[:, None] == row_index[None, :])
    return (position, allowed)

def layer(resid, position, allowed, params):
    gain_attn, w_query, w_key, w_value, w_out, gain_ffn, w_gate, w_up, w_down = params
    row_count = resid.shape[0]
    normed = low(resid * rms_scale(resid) * gain_attn)
    queries = low(rotate(low_back(dot_high(normed, w_query)).reshape(row_count, HEADS, HEAD), position, 1.0))
    key_rows = low(rotate(low_back(dot_high(normed, w_key)).reshape(row_count, KV_HEADS, HEAD), position, 1.0))
    value_rows = low(low_back(dot_high(normed, w_value))).reshape(row_count, KV_HEADS, HEAD)
    key_full = jnp.repeat(key_rows, HEADS // KV_HEADS, axis=1)
    value_full = jnp.repeat(value_rows, HEADS // KV_HEADS, axis=1)
    scores = low_back(jnp.einsum('rhd,shd->hrs', queries, key_full, precision=lax.Precision.HIGHEST) * HEAD ** (-0.5))
    masked = jnp.where(allowed[None], scores, neg_fill)
    row_max = lax.optimization_barrier(jnp.max(masked, axis=-1, keepdims=True))
    exp_scores = jnp.exp(masked - row_max)
    probs = exp_scores / lax.optimization_barrier(jnp.sum(exp_scores, axis=-1, keepdims=True))
    attended = jnp.einsum('hrs,shd->rhd', low(probs), value_full, precision=lax.Precision.HIGHEST)
    attended = low(low_back(attended.reshape(row_count, HEADS * HEAD)))
    hidden_in = resid + low_back(dot_high(attended, w_out))
    normed_ffn = low(hidden_in * rms_scale(hidden_in) * gain_ffn)
    gate = low_back(dot_high(normed_ffn, w_gate))
    up_proj = low_back(dot_high(normed_ffn, w_up))
    hidden = low(jax.nn.silu(gate) * up_proj)
    return hidden_in + low_back(dot_high(hidden, w_down))

def block_pass(block_in, probe, lengths_row, params_first, params_second):
    position, allowed = segment_info(lengths_row, block_in.shape[0])
    first_out = layer(block_in, position, allowed, params_first)
    second_in = low_back(low(first_out)) + probe
    second_out = layer(second_in, position, allowed, params_second)
    return (first_out, second_out)

def reference(inputs, cotangent, seq_lengths, gain_attn, w_query, w_key, w_value, w_out, gain_ffn, w_gate, w_up, w_down):
    block_count = MICRO * N_DP
    blocks = inputs.astype(jnp.float32).reshape(block_count, MB_ROWS, D)
    cot_blocks = cotangent.astype(jnp.float32).reshape(block_count, MB_ROWS, D)
    lengths = jnp.transpose(seq_lengths, (1, 0, 2)).reshape(block_count, SLOTS).astype(jnp.int32)
    params = tuple((stacked.astype(jnp.float32) for stacked in (gain_attn, w_query, w_key, w_value, w_out, gain_ffn, w_gate, w_up, w_down)))
    probes = jnp.zeros_like(blocks)

    def forward(blocks_in, probes_in, params_in):
        first_params = tuple((stacked[0] for stacked in params_in))
        second_params = tuple((stacked[1] for stacked in params_in))

        def one_block(items):
            return jax.checkpoint(block_pass)(items[0], items[1], items[2], first_params, second_params)
        return lax.map(one_block, (blocks_in, probes_in, lengths))
    outputs, pullback = jax.vjp(forward, blocks, probes, params)
    first_all, second_all = outputs
    grad_blocks, grad_probes, grad_params = pullback((jnp.zeros_like(first_all), cot_blocks))
    section_out = jnp.stack([first_all, second_all]).reshape(2, MICRO, N_DP * MB_ROWS, D).astype(jnp.bfloat16)
    in_grad = jnp.stack([grad_blocks, grad_probes]).reshape(2, MICRO, N_DP * MB_ROWS, D).astype(jnp.bfloat16)
    return (section_out, in_grad, grad_params[0], grad_params[1], grad_params[2], grad_params[3], grad_params[4], grad_params[5], grad_params[6], grad_params[7], grad_params[8])
```

```python
import jax
import jax.numpy as jnp
from jax import lax
from jax.sharding import PartitionSpec as P

HEAD = 96


eps = 1e-05
rope_base = 100000.0
neg_fill = -1e30


def passed_along(shard, axis, by):
    count = lax.axis_size(axis)
    pairs = [(i, i + by) for i in range(count) if 0 <= i + by < count]
    return lax.ppermute(shard, axis, pairs)


def rms_scale(values):
    return lax.rsqrt(jnp.mean(values * values, axis=-1, keepdims=True) + eps)


def matmul_f32(left, right):
    return jnp.dot(left, right, preferred_element_type=jnp.float32)


def rows_product(left, right):
    return lax.dot_general(
        left, right, (((0,), (0,)), ((), ())), preferred_element_type=jnp.float32
    )


def against_product(left, right):
    return lax.dot_general(
        left, right, (((1,), (1,)), ((), ())), preferred_element_type=jnp.float32
    )


def rotate(values, position, direction):
    half_size = values.shape[-1] // 2
    inverse = rope_base ** (-jnp.arange(half_size, dtype=jnp.float32) * 2.0 / values.shape[-1])
    angle = position.astype(jnp.float32)[:, None] * inverse[None, :]
    cosine = jnp.cos(angle)[:, None, :]
    sine = direction * jnp.sin(angle)[:, None, :]
    first = values[..., :half_size]
    second = values[..., half_size:]
    return jnp.concatenate(
        [first * cosine - second * sine, second * cosine + first * sine], axis=-1
    )


def segment_info(lengths_row, row_count):
    slot_count = lengths_row.shape[0]
    seq_ends = jnp.cumsum(lengths_row)
    seq_starts = jnp.concatenate([seq_ends - lengths_row, seq_ends[-1:]])
    row_index = jnp.arange(row_count, dtype=jnp.int32)
    segment = jnp.sum((row_index[:, None] >= seq_ends[None, :]).astype(jnp.int32), axis=1)
    pick = segment[:, None] == jnp.arange(slot_count + 1, dtype=jnp.int32)[None, :]
    position = row_index - jnp.sum(jnp.where(pick, seq_starts[None, :], 0), axis=1)
    allowed = (
        (segment[:, None] == segment[None, :])
        & (row_index[None, :] <= row_index[:, None])
        & (segment[:, None] < slot_count)
    )
    allowed = allowed | (row_index[:, None] == row_index[None, :])
    return (position, allowed)


def collect_rows(values):
    return lax.all_gather(values, "tensor", axis=0, tiled=True)


def collect_again(values):
    return lax.all_gather(values, "tensor", axis=0, tiled=True)


def collect_grads(values):
    return lax.all_gather(values, "tensor", axis=0, tiled=True)


def spread_rows(left, right, share_rows):

    def term(start, count):
        return matmul_f32(left, right)

    return lax.psum_scatter(
        term(jnp.int32(0), share_rows * lax.axis_size("tensor")).astype(jnp.bfloat16),
        "tensor",
        scatter_dimension=0,
        tiled=True,
    ).astype(jnp.float32)


def spread_grads(operand_pairs, share_rows):

    def term(start, count):
        summed = None
        for left, right in operand_pairs:
            part_term = against_product(left, right)
            summed = part_term if summed is None else summed + part_term
        return summed

    return lax.psum_scatter(
        term(jnp.int32(0), share_rows * lax.axis_size("tensor")).astype(jnp.bfloat16),
        "tensor",
        scatter_dimension=0,
        tiled=True,
    ).astype(jnp.float32)


def norm_back(d_normed, resid, scale_rows, gain):
    unit_rows = resid * scale_rows
    gain_part = jnp.sum(d_normed * unit_rows, axis=0)
    d_unit = d_normed * gain
    d_resid = scale_rows * (
        d_unit - unit_rows * jnp.mean(d_unit * unit_rows, axis=-1, keepdims=True)
    )
    return (d_resid, gain_part)


def attend(queries, key_rows, value_rows, allowed):
    full_rows, query_heads, head_size = queries.shape
    kv_count = key_rows.shape[1]
    grouped = queries.reshape(full_rows, kv_count, query_heads // kv_count, head_size)
    scores = jnp.einsum(
        "rkgd,skd->kgrs", grouped, key_rows, preferred_element_type=jnp.float32
    ) * head_size ** (-0.5)
    masked = jnp.where(allowed, scores, neg_fill)
    row_max = jnp.max(masked, axis=-1, keepdims=True)
    exp_scores = jnp.exp(masked - row_max)
    row_total = jnp.sum(exp_scores, axis=-1, keepdims=True)
    probs_low = (exp_scores / row_total).astype(jnp.bfloat16)
    attended = jnp.einsum(
        "kgrs,skd->rkgd", probs_low, value_rows, preferred_element_type=jnp.float32
    )
    return (attended.reshape(full_rows, query_heads * head_size), row_max + jnp.log(row_total))


def attend_back(queries, key_rows, value_rows, log_total, allowed, d_attended):
    full_rows, query_heads, head_size = queries.shape
    kv_count = key_rows.shape[1]
    group_size = query_heads // kv_count
    score_scale = head_size ** (-0.5)
    grouped = queries.reshape(full_rows, kv_count, group_size, head_size)
    scores = (
        jnp.einsum("rkgd,skd->kgrs", grouped, key_rows, preferred_element_type=jnp.float32)
        * score_scale
    )
    probs = jnp.exp(jnp.where(allowed, scores, neg_fill) - log_total)
    d_out = d_attended.reshape(full_rows, kv_count, group_size, head_size)
    d_probs = jnp.einsum("rkgd,skd->kgrs", d_out, value_rows, preferred_element_type=jnp.float32)
    d_scores = (probs * (d_probs - jnp.sum(probs * d_probs, axis=-1, keepdims=True))).astype(
        jnp.bfloat16
    )
    d_values = jnp.einsum(
        "kgrs,rkgd->skd", probs.astype(jnp.bfloat16), d_out, preferred_element_type=jnp.float32
    )
    d_grouped = (
        jnp.einsum("kgrs,skd->rkgd", d_scores, key_rows, preferred_element_type=jnp.float32)
        * score_scale
    )
    d_keys = (
        jnp.einsum("kgrs,rkgd->skd", d_scores, grouped, preferred_element_type=jnp.float32)
        * score_scale
    )
    return (d_grouped.reshape(full_rows, query_heads, head_size), d_keys, d_values)


def layer_forward(resid, position, allowed, weights):
    gain_attn, w_query, w_key, w_value, w_out, gain_ffn, w_gate, w_up, w_down = weights
    share_rows = resid.shape[0]
    scale_attn = rms_scale(resid)
    normed = (resid * scale_attn * gain_attn).astype(jnp.bfloat16)
    normed_all = collect_rows(normed)
    full_rows = normed_all.shape[0]
    queries = rotate(
        matmul_f32(normed_all, w_query).reshape(full_rows, -1, HEAD), position, 1.0
    ).astype(jnp.bfloat16)
    key_rows = rotate(
        matmul_f32(normed_all, w_key).reshape(full_rows, -1, HEAD), position, 1.0
    ).astype(jnp.bfloat16)
    value_rows = matmul_f32(normed_all, w_value).astype(jnp.bfloat16).reshape(full_rows, -1, HEAD)
    attended, log_total = attend(queries, key_rows, value_rows, allowed)
    attended_low = attended.astype(jnp.bfloat16)
    hidden_in = resid + spread_rows(attended_low, w_out, share_rows)
    scale_ffn = rms_scale(hidden_in)
    normed_ffn = (hidden_in * scale_ffn * gain_ffn).astype(jnp.bfloat16)
    normed_ffn_all = collect_rows(normed_ffn)
    gate = matmul_f32(normed_ffn_all, w_gate)
    up_proj = matmul_f32(normed_ffn_all, w_up)
    hidden_low = (jax.nn.silu(gate) * up_proj).astype(jnp.bfloat16)
    result = hidden_in + spread_rows(hidden_low, w_down, share_rows)
    kept = {
        "resid": resid,
        "scale_attn": scale_attn,
        "normed": normed,
        "queries": queries,
        "key_rows": key_rows,
        "value_rows": value_rows,
        "log_total": log_total,
        "attended_low": attended_low,
        "hidden_in": hidden_in,
        "scale_ffn": scale_ffn,
        "normed_ffn": normed_ffn,
        "gate": gate,
        "up_proj": up_proj,
        "hidden_low": hidden_low,
        "position": position,
        "allowed": allowed,
    }
    return (result, kept)


def layer_backward(upstream, kept, weights, accum):
    gain_attn, w_query, w_key, w_value, w_out, gain_ffn, w_gate, w_up, w_down = weights
    (
        acc_gain_attn,
        acc_query,
        acc_key,
        acc_value,
        acc_out,
        acc_gain_ffn,
        acc_gate,
        acc_up,
        acc_down,
    ) = accum
    share_rows = upstream.shape[0]
    ffn_grad_all = collect_grads(upstream.astype(jnp.bfloat16))
    acc_down = acc_down + rows_product(kept["hidden_low"], ffn_grad_all)
    d_hidden = against_product(ffn_grad_all, w_down)
    gate = kept["gate"]
    sigmoid_gate = jax.nn.sigmoid(gate)
    d_gate = (
        d_hidden * kept["up_proj"] * sigmoid_gate * (1.0 + gate * (1.0 - sigmoid_gate))
    ).astype(jnp.bfloat16)
    d_up = (d_hidden * gate * sigmoid_gate).astype(jnp.bfloat16)
    normed_ffn_all = collect_again(kept["normed_ffn"])
    acc_gate = acc_gate + rows_product(normed_ffn_all, d_gate)
    acc_up = acc_up + rows_product(normed_ffn_all, d_up)
    d_normed_ffn = spread_grads(((d_gate, w_gate), (d_up, w_up)), share_rows)
    d_hidden_in, gain_part = norm_back(d_normed_ffn, kept["hidden_in"], kept["scale_ffn"], gain_ffn)
    acc_gain_ffn = acc_gain_ffn + gain_part
    d_hidden_in = upstream + d_hidden_in
    attn_grad_all = collect_grads(d_hidden_in.astype(jnp.bfloat16))
    acc_out = acc_out + rows_product(kept["attended_low"], attn_grad_all)
    d_attended = against_product(attn_grad_all, w_out).astype(jnp.bfloat16)
    d_query, d_keys, d_values = attend_back(
        kept["queries"],
        kept["key_rows"],
        kept["value_rows"],
        kept["log_total"],
        kept["allowed"],
        d_attended,
    )
    full_rows = d_query.shape[0]
    d_query_low = (
        rotate(d_query, kept["position"], -1.0).reshape(full_rows, -1).astype(jnp.bfloat16)
    )
    d_keys_low = rotate(d_keys, kept["position"], -1.0).reshape(full_rows, -1).astype(jnp.bfloat16)
    d_values_low = d_values.reshape(full_rows, -1).astype(jnp.bfloat16)
    normed_all = collect_again(kept["normed"])
    acc_query = acc_query + rows_product(normed_all, d_query_low)
    acc_key = acc_key + rows_product(normed_all, d_keys_low)
    acc_value = acc_value + rows_product(normed_all, d_values_low)
    d_normed = spread_grads(
        ((d_query_low, w_query), (d_keys_low, w_key), (d_values_low, w_value)), share_rows
    )
    d_resid, gain_part = norm_back(d_normed, kept["resid"], kept["scale_attn"], gain_attn)
    acc_gain_attn = acc_gain_attn + gain_part
    d_resid = d_hidden_in + d_resid
    accum = (
        acc_gain_attn,
        acc_query,
        acc_key,
        acc_value,
        acc_out,
        acc_gain_ffn,
        acc_gate,
        acc_up,
        acc_down,
    )
    return (d_resid, accum)


def shards(
    inputs,
    cotangent,
    seq_lengths,
    gain_attn,
    w_query,
    w_key,
    w_value,
    w_out,
    gain_ffn,
    w_gate,
    w_up,
    w_down,
):
    section_index = lax.axis_index("section")
    micro_count = inputs.shape[0]
    share_rows = inputs.shape[1]
    full_rows = share_rows * lax.axis_size("tensor")
    weights = tuple(
        (
            stacked[0].astype(jnp.float32) if stacked.ndim == 2 else stacked[0]
            for stacked in (
                gain_attn,
                w_query,
                w_key,
                w_value,
                w_out,
                gain_ffn,
                w_gate,
                w_up,
                w_down,
            )
        )
    )
    lengths_here = seq_lengths[0]
    outputs_tick = []
    kept_tick = []
    received = jnp.zeros(inputs.shape[1:], jnp.bfloat16)
    for tick_num in range(micro_count + 1):
        batch_num = jnp.clip(tick_num - section_index, 0, micro_count - 1)
        lengths_row = lax.dynamic_index_in_dim(lengths_here, batch_num, 0, keepdims=False)
        position, allowed = segment_info(lengths_row, full_rows)
        entry = jnp.where(
            section_index == 0, inputs[min(tick_num, micro_count - 1)], received
        ).astype(jnp.float32)
        result, kept = layer_forward(entry, position, allowed, weights)
        result_low = result.astype(jnp.bfloat16)
        outputs_tick.append(result_low)
        kept_tick.append(kept)
        if tick_num < micro_count:
            received = passed_along(result_low, "section", 1)
    accum = tuple((jnp.zeros(weight.shape, jnp.float32) for weight in weights))
    grads_tick = []
    received_grad = jnp.zeros(inputs.shape[1:], jnp.bfloat16)
    for back_num in range(micro_count + 1):
        own_grad = cotangent[max(micro_count - 1 - back_num, 0)]
        if back_num == micro_count:
            own_grad = jnp.zeros_like(own_grad)
        upstream = jnp.where(section_index == 1, own_grad, received_grad).astype(jnp.float32)
        d_entry, accum = layer_backward(upstream, kept_tick[micro_count - back_num], weights, accum)
        d_low = d_entry.astype(jnp.bfloat16)
        grads_tick.append(d_low)
        if back_num < micro_count:
            received_grad = passed_along(d_low, "section", -1)
    (
        grad_gain_attn,
        grad_query,
        grad_key,
        grad_value,
        grad_out,
        grad_gain_ffn,
        grad_gate,
        grad_up,
        grad_down,
    ) = accum
    grad_query, grad_key, grad_value, grad_out, grad_gate, grad_up, grad_down = (
        summed.astype(jnp.float32)
        for summed in lax.psum(
            tuple(
                part.astype(jnp.bfloat16)
                for part in (
                    grad_query, grad_key, grad_value, grad_out, grad_gate, grad_up, grad_down
                )
            ),
            "dp",
        )
    )
    grad_gain_attn, grad_gain_ffn = lax.psum((grad_gain_attn, grad_gain_ffn), ("dp", "tensor"))
    section_out = jnp.stack(
        [
            jnp.where(section_index == 0, outputs_tick[batch_num], outputs_tick[batch_num + 1])
            for batch_num in range(micro_count)
        ]
    )[None]
    in_grad = jnp.stack(
        [
            jnp.where(
                section_index == 0,
                grads_tick[micro_count - batch_num],
                grads_tick[micro_count - 1 - batch_num],
            )
            for batch_num in range(micro_count)
        ]
    )[None]
    return (
        section_out,
        in_grad,
        grad_gain_attn[None],
        grad_query[None],
        grad_key[None],
        grad_value[None],
        grad_out[None],
        grad_gain_ffn[None],
        grad_gate[None],
        grad_up[None],
        grad_down[None],
    )


def solution(mesh):
    placed = (
        P(None, ("dp", "tensor"), None),
        P(None, ("dp", "tensor"), None),
        P("dp", None, None),
        P("section", None),
        P("section", None, "tensor"),
        P("section", None, "tensor"),
        P("section", None, "tensor"),
        P("section", "tensor", None),
        P("section", None),
        P("section", None, "tensor"),
        P("section", None, "tensor"),
        P("section", "tensor", None),
    )
    return jax.shard_map(
        shards,
        mesh=mesh,
        in_specs=placed,
        out_specs=(
            P("section", None, ("dp", "tensor"), None),
            P("section", None, ("dp", "tensor"), None),
            P("section", None),
            P("section", None, "tensor"),
            P("section", None, "tensor"),
            P("section", None, "tensor"),
            P("section", "tensor", None),
            P("section", None),
            P("section", None, "tensor"),
            P("section", None, "tensor"),
            P("section", "tensor", None),
        ),
        check_vma=False,
    )
```

```python
import functools

import jax
import jax.numpy as jnp
from jax import lax
from jax.experimental import pallas as pl
from jax.experimental.pallas import tpu as pltpu
from jax.sharding import PartitionSpec as P

HEAD = 96
HALF = HEAD // 2
LANES = 128
CHUNKS = 2
BF16 = jnp.bfloat16
F32 = jnp.float32
MESH = pl.DeviceIdType.MESH
VMEM = pltpu.VMEM
VMEM_SPEC = pl.BlockSpec(memory_space=pltpu.VMEM)
HBM_SPEC = pl.BlockSpec(memory_space=pltpu.HBM)
DMA = pltpu.SemaphoreType.DMA

eps = 1e-05
rope_base = 100000.0
neg_fill = -1e30


def dot_nn(left, right):
    return lax.dot_general(left, right, (((1,), (0,)), ((), ())), preferred_element_type=F32)


def dot_nt(left, right):
    return lax.dot_general(left, right, (((1,), (1,)), ((), ())), preferred_element_type=F32)


def dot_tn(left, right):
    return lax.dot_general(left, right, (((0,), (0,)), ((), ())), preferred_element_type=F32)


def rms_scale(values):
    return lax.rsqrt(jnp.mean(values * values, axis=-1, keepdims=True) + eps)


def norm_back(d_normed, resid, gain):
    scale_rows = rms_scale(resid)
    unit_rows = resid * scale_rows
    gain_part = jnp.sum(d_normed * unit_rows, axis=0, keepdims=True)
    d_unit = d_normed * gain
    inner = jnp.mean(d_unit * unit_rows, axis=-1, keepdims=True)
    return scale_rows * (d_unit - unit_rows * inner), gain_part


class Line:
    def __init__(self, count, full, rbuf, sbuf, gs, gr, ss, sr):
        self.n = count
        self.core = lax.axis_index("section")
        self.me = lax.axis_index("tensor")
        self.full, self.rbuf, self.sbuf = full, rbuf, sbuf
        self.gs, self.gr, self.ss, self.sr = gs, gr, ss, sr
        self.rows = full.shape[1] // CHUNKS

    def span(self, c):
        return pl.ds(c * self.rows, self.rows)

    def neighbour(self, d):
        return self.me + 1 if d == 0 else self.me - 1

    def enter(self, also=()):
        me, n = self.me, self.n
        barrier = pltpu.get_barrier_semaphore()
        for peer in ({"section": 1 - self.core}, *also):
            pl.semaphore_signal(barrier, 1, device_id=peer, device_id_type=MESH)
        for d, there in ((1, me > 0), (0, me < n - 1)):

            @pl.when(there)
            def _():
                pl.semaphore_signal(
                    barrier, 1, device_id={"tensor": self.neighbour(d)}, device_id_type=MESH
                )

        peers = 1 + len(also) + (me > 0).astype(jnp.int32) + (me < n - 1).astype(jnp.int32)
        pl.semaphore_wait(barrier, peers)

    def gather_copy(self, d, step, shard, c):
        ref = self.full.at[shard, self.span(c)]
        return pltpu.make_async_remote_copy(
            ref,
            ref,
            self.gs.at[d, step, c],
            self.gr.at[d, step, c],
            device_id={"tensor": self.neighbour(d)},
            device_id_type=MESH,
        )

    def gather_step(self, step):
        me, n = self.me, self.n
        for c in range(CHUNKS):
            for d in range(2):
                shard = me - step if d == 0 else me + step
                holds = (shard >= 0) & (shard < n)
                onward = (me + 1 < n) if d == 0 else (me > 0)

                @pl.when(holds & (step > 0))
                def _():
                    self.gather_copy(d, step - 1, shard, c).wait_recv()

                @pl.when(holds & onward)
                def _():
                    self.gather_copy(d, step, shard, c).start()

    def gather_end(self):
        me, n = self.me, self.n

        @pl.loop(0, n - 1)
        def _(step):
            for c in range(CHUNKS):
                for d in range(2):
                    shard = me - step if d == 0 else me + step
                    onward = (me + 1 < n) if d == 0 else (me > 0)

                    @pl.when((shard >= 0) & (shard < n) & onward)
                    def _():
                        self.gather_copy(d, step, shard, c).wait_send()

    def sum_copy(self, d, shard, c):
        return pltpu.make_async_remote_copy(
            self.sbuf.at[shard, self.span(c)],
            self.rbuf.at[d, shard, self.span(c)],
            self.ss.at[d, shard, c],
            self.sr.at[d, shard, c],
            device_id={"tensor": self.neighbour(d)},
            device_id_type=MESH,
        )

    def sum_step(self, d, shard, partial):
        me, n = self.me, self.n
        goes = (shard > me) & (shard < n) if d == 0 else (shard >= 0) & (shard < me)
        first = (me == 0) if d == 0 else (me == n - 1)

        @pl.when(goes & first)
        def _():
            mine = partial(shard)
            for c in range(CHUNKS):
                rows = slice(c * self.rows, (c + 1) * self.rows)
                self.sbuf[shard, self.span(c)] = mine[rows].astype(BF16)
                self.sum_copy(d, shard, c).start()

        @pl.when(goes & jnp.logical_not(first))
        def _():
            mine = partial(shard)
            for c in range(CHUNKS):
                rows = slice(c * self.rows, (c + 1) * self.rows)
                self.sum_copy(d, shard, c).wait_recv()
                arrived = self.rbuf[d, shard, self.span(c)].astype(F32)
                self.sbuf[shard, self.span(c)] = (mine[rows] + arrived).astype(BF16)
                self.sum_copy(d, shard, c).start()

    def sum_take(self, total):
        me, n = self.me, self.n
        for d, there in ((0, me > 0), (1, me < n - 1)):

            @pl.when(there)
            def _():
                for c in range(CHUNKS):
                    self.sum_copy(d, me, c).wait_recv()
                    total[self.span(c)] += self.rbuf[d, me, self.span(c)].astype(F32)

    def sum_end(self):
        me, n = self.me, self.n

        @pl.loop(0, n)
        def _(shard):
            for d, goes in ((0, shard > me), (1, shard < me)):

                @pl.when(goes)
                def _():
                    for c in range(CHUNKS):
                        self.sum_copy(d, shard, c).wait_send()


def line_scratch(count, rows, width):
    return [
        VMEM((count, rows, width), BF16),
        VMEM((2, count, rows, width), BF16),
        VMEM((count, rows, width), BF16),
        DMA((2, count, CHUNKS)),
        DMA((2, count, CHUNKS)),
        DMA((2, count, CHUNKS)),
        DMA((2, count, CHUNKS)),
    ]


def rows_then_sums(line, compute, partial, halfway=lambda: None):
    me, n = line.me, line.n

    @pl.loop(0, 2 * n - 1)
    def _(step):
        @pl.when((step > 0) & (step < n))
        def _():
            line.gather_step(step)

        @pl.when(step < n)
        def _():
            @pl.loop(0, 2)
            def _(side):
                shard = jnp.where(side == 0, me - step, me + step)

                @pl.when((shard >= 0) & (shard < n) & ((step > 0) | (side == 0)))
                def _():
                    compute(shard)

        line.sum_step(0, step - me, partial)
        line.sum_step(1, 2 * (n - 1) - step - me, partial)

        @pl.when(step == n - 1)
        def _():
            halfway()


def later_shards(line, compute):
    me, n = line.me, line.n

    @pl.loop(0, n)
    def _(step):
        @pl.when(step > 0)
        def _():
            line.gather_step(step)

        @pl.loop(0, 2)
        def _(side):
            shard = jnp.where(side == 0, me - step, me + step)

            @pl.when((shard >= 0) & (shard < n) & ((step > 0) | (side == 0)))
            def _():
                compute(shard)


def sums_after(line, partial):
    me, n = line.me, line.n

    @pl.loop(0, n - 1)
    def _(step):
        line.sum_step(0, me + n - 1 - step, partial)
        line.sum_step(1, step - (n - 1 - me), partial)


class Weights:
    def __init__(self, layer, sems):
        self.own = lax.axis_index("section") == layer
        self.sems = sems
        self.wanted = []

    def want(self, mine, theirs, target):
        self.wanted.append((mine, theirs, target))

    def start_own(self):
        @pl.when(self.own)
        def _():
            for index, (mine, _theirs, target) in enumerate(self.wanted):
                pltpu.make_async_copy(mine, target, self.sems.at[index]).start()

    def start_other(self, before=lambda: None):
        @pl.when(jnp.logical_not(self.own))
        def _():
            before()
            for index, (_mine, theirs, target) in enumerate(self.wanted):
                pltpu.make_async_copy(theirs, target, self.sems.at[index]).start()

    def start(self):
        self.start_own()
        self.start_other()

    def wait(self):
        for index, (mine, _theirs, target) in enumerate(self.wanted):
            pltpu.make_async_copy(mine, target, self.sems.at[index]).wait()


class Pair:
    def __init__(self, local_sems, send_sems, recv_sems):
        self.core = lax.axis_index("section")
        self.sems = local_sems, send_sems, recv_sems
        self.kept, self.sent = [], []

    def keep(self, source, target):
        copy = pltpu.make_async_copy(source, target, self.sems[0].at[len(self.kept)])
        copy.start()
        self.kept.append(copy)

    def copy(self, source, target, index):
        return pltpu.make_async_remote_copy(
            source,
            target,
            self.sems[1].at[index],
            self.sems[2].at[index],
            device_id={"section": 1 - self.core},
            device_id_type=MESH,
        )

    def send(self, source, target):
        copy = self.copy(source, target, len(self.sent))
        copy.start()
        self.sent.append(copy)

    def share(self, source, pair):
        self.keep(source, pair.at[0])
        self.send(source, pair.at[1])

    def share_half(self, halves, pair):
        self.keep(halves.at[self.core], pair.at[0])
        self.send(halves.at[1 - self.core], pair.at[1])

    def wait(self):
        for copy in self.kept:
            copy.wait()
        for copy in self.sent:
            copy.wait()


def pair_scratch(kept, sent):
    return [DMA((max(kept, 1),)), DMA((max(sent, 1),)), DMA((max(sent, 1),))]


class Cube:
    def __init__(self, layer, count):
        self.bits = count.bit_length() - 1
        assert count == 1 << self.bits
        self.me = lax.axis_index("dp")
        self.core = lax.axis_index("section")
        self.active = self.core == layer
        self.bit = [(self.me // (1 << b)) % 2 for b in range(self.bits)]
        self.down = list(range(self.bits - 1, -1, -1))

    def order(self, colour):
        return list(range(self.bits)) if colour == 0 else self.down

    def peer(self, b):
        return {"dp": self.me + (1 - 2 * self.bit[b]) * (1 << b)}

    def peers(self):
        return [self.peer(b) for b in range(self.bits)]


class Reduce(Cube):
    def __init__(self, layer, count, sources, outs, scratch):
        super().__init__(layer, count)
        self.sources, self.outs = sources, outs
        size = len(sources)
        self.accs = scratch[:size]
        self.recvs = [scratch[size * (t + 1) : size * (t + 2)] for t in range(self.bits)]
        self.local, self.ss, self.sr, self.fs, self.fr = scratch[size * (self.bits + 1) :]
        self.t = 0
        self.place = [
            {b: slice(None) for b in self.down if b != self.order(c)[0]} for c in range(2)
        ]

    def items(self):
        return [(a, c) for a in range(len(self.sources)) for c in range(2)]

    def spot(self, c, changed=()):
        place = {**self.place[c], **dict(changed)}
        return (c, *(place[b] for b in self.down if b in place))

    def first_half(self, a, c, value):
        b = self.order(c)[0]
        index = [slice(None)] * self.bits
        index[self.down.index(b)] = value
        return self.sources[a].at[(c, *index)]

    def copy(self, a, c, t, source):
        return pltpu.make_async_remote_copy(
            source,
            self.recvs[t][a].at[c],
            self.ss.at[a, c, t],
            self.sr.at[a, c, t],
            device_id=self.peer(self.order(c)[t]),
            device_id_type=MESH,
        )

    def kept(self, a, c):
        mine = self.first_half(a, c, self.bit[self.order(c)[0]])
        return pltpu.make_async_copy(mine, self.accs[a].at[c], self.local.at[a, c])

    def start(self):
        for a, c in self.items():
            other = self.first_half(a, c, 1 - self.bit[self.order(c)[0]])
            self.copy(a, c, 0, other).start()
            self.kept(a, c).start()

    def advance(self):
        t = self.t
        if t >= self.bits:
            return
        for a, c in self.items():
            if t == 0:
                self.kept(a, c).wait()
            self.copy(a, c, t, self.recvs[t][a].at[c]).wait_recv()
            acc, spot = self.accs[a], self.spot(c)
            acc[spot] = (acc[spot].astype(F32) + self.recvs[t][a][c].astype(F32)).astype(BF16)
            if t + 1 < self.bits:
                b = self.order(c)[t + 1]
                self.copy(a, c, t + 1, acc.at[self.spot(c, [(b, 1 - self.bit[b])])]).start()
        if t + 1 < self.bits:
            for c in range(2):
                b = self.order(c)[t + 1]
                self.place[c][b] = self.bit[b]
        self.t = t + 1

    def hand_over(self, a, c):
        return pltpu.make_async_remote_copy(
            self.accs[a].at[self.spot(c)],
            self.outs[a].at[self.core, c],
            self.fs.at[a, c],
            self.fr.at[a, c],
            device_id={"section": 1 - self.core},
            device_id_type=MESH,
        )

    def put_away(self, a, c):
        return pltpu.make_async_copy(
            self.accs[a].at[self.spot(c)], self.outs[a].at[self.core, c], self.fs.at[a, c]
        )

    def finish(self):
        while self.t < self.bits:
            self.advance()

        @pl.when(self.active)
        def _():
            for a, c in self.items():
                self.put_away(a, c).start()

        @pl.when(jnp.logical_not(self.active))
        def _():
            for a, c in self.items():
                self.hand_over(a, c).start()

        for a, c in self.items():
            for t in range(self.bits):
                self.copy(a, c, t, self.recvs[t][a].at[c]).wait_send()

        @pl.when(self.active)
        def _():
            for a, c in self.items():
                self.put_away(a, c).wait()
                self.hand_over(a, c).wait_recv()

        @pl.when(jnp.logical_not(self.active))
        def _():
            for a, c in self.items():
                self.hand_over(a, c).wait_send()


class Gather(Cube):
    def __init__(self, layer, count, blocks, outs, sems):
        super().__init__(layer, count)
        self.blocks, self.outs = blocks, outs
        self.keep, self.ss, self.sr = sems
        self.t = 0

    def items(self):
        return [(a, h, c) for a in range(len(self.blocks)) for h in range(2) for c in range(2)]

    def order(self, colour):
        return super().order(colour)[::-1]

    def region(self, a, h, c, t):
        free = self.order(c)[:t]
        index = (slice(None) if b in free else self.bit[b] for b in self.down)
        return self.outs[a].at[(h, c, *index)]

    def copy(self, a, h, c, t):
        target = self.region(a, h, c, t)
        return pltpu.make_async_remote_copy(
            self.blocks[a].at[h, c] if t == 0 else target,
            target,
            self.ss.at[a, h, c, t],
            self.sr.at[a, h, c, t],
            device_id=self.peer(self.order(c)[t]),
            device_id_type=MESH,
        )

    def kept(self, a, h, c):
        return pltpu.make_async_copy(
            self.blocks[a].at[h, c], self.region(a, h, c, 0), self.keep.at[a, h, c]
        )

    def start(self):
        @pl.when(self.active)
        def _():
            for a, h, c in self.items():
                self.copy(a, h, c, 0).start()
                self.kept(a, h, c).start()

    def advance(self):
        t = self.t
        if t >= self.bits:
            return

        @pl.when(self.active)
        def _():
            for a, h, c in self.items():
                if t == 0:
                    self.kept(a, h, c).wait()
                self.copy(a, h, c, t).wait_recv()
                if t + 1 < self.bits:
                    self.copy(a, h, c, t + 1).start()

        self.t = t + 1

    def finish(self):
        while self.t < self.bits:
            self.advance()

        @pl.when(self.active)
        def _():
            for a, h, c in self.items():
                for t in range(self.bits):
                    self.copy(a, h, c, t).wait_send()


def reduce_scratch(count, arrays):
    bits = count.bit_length() - 1
    scratch = []
    for level in (1, *range(1, bits + 1)):
        scratch += [VMEM((2,) + (2,) * (bits - level) + shape[-2:], BF16) for shape in arrays]
    size = len(arrays)
    return scratch + [
        DMA((size, 2)),
        DMA((size, 2, bits)),
        DMA((size, 2, bits)),
        DMA((size, 2)),
        DMA((size, 2)),
    ]


def gather_sems(count, size):
    bits = count.bit_length() - 1
    return [DMA((size, 2, 2)), DMA((size, 2, 2, bits)), DMA((size, 2, 2, bits))]


class Tasks:
    def __init__(self, count, plan):
        self.count = count
        self.reduce = plan.get("reduce")
        self.gather = plan.get("gather")

    def arguments(self):
        args = list(self.reduce[1]) if self.reduce else []
        return args + (list(self.gather[1]) if self.gather else [])

    def outputs(self):
        outs = []
        if self.reduce:
            outs += [((2, 2) + ref.shape[-2:], BF16, HBM_SPEC) for ref in self.reduce[1]]
        if self.gather:
            middle = (2,) * (self.count.bit_length() - 1)
            outs += [
                ((2, 2) + middle + ref.shape[-2:], BF16, HBM_SPEC) for ref in self.gather[1]
            ]
        return outs

    def scratch(self):
        scratch = []
        if self.reduce:
            scratch += reduce_scratch(self.count, [ref.shape for ref in self.reduce[1]])
        if self.gather:
            scratch += [VMEM(ref.shape, BF16) for ref in self.gather[1]]
            scratch += [DMA((len(self.gather[1]),))]
            scratch += gather_sems(self.count, len(self.gather[1]))
        return scratch

    def bind(self, args, outs, scratch):
        self.running = []
        self.loads = []
        count = self.count
        if self.reduce:
            size = len(self.reduce[1])
            used = len(reduce_scratch(count, [ref.shape for ref in self.reduce[1]]))
            self.running.append(
                Reduce(self.reduce[0], count, args[:size], outs[:size], scratch[:used])
            )
            args, outs, scratch = args[size:], outs[size:], scratch[used:]
        if self.gather:
            size = len(self.gather[1])
            blocks = scratch[:size]
            self.loads = [
                pltpu.make_async_copy(args[a], blocks[a], scratch[size].at[a]) for a in range(size)
            ]
            self.running.append(
                Gather(self.gather[0], count, blocks, outs, scratch[size + 1 : size + 4])
            )
        for load in self.loads:
            load.start()

    def peers(self):
        return self.running[0].peers() if self.running else []

    def start(self):
        for load in self.loads:
            load.wait()
        for task in self.running:
            task.start()

    def advance(self):
        for task in self.running:
            task.advance()

    def finish(self):
        for task in self.running:
            task.finish()


def pick_split(columns):
    heads = columns // HEAD
    col = lax.broadcasted_iota(jnp.int32, (columns, heads * LANES), 1)
    row = lax.broadcasted_iota(jnp.int32, (columns, heads * LANES), 0)
    inner = col & 63
    source = (col >> 7) * HEAD + ((col >> 6) & 1) * HALF + inner
    return ((row == source) & (inner < HALF)).astype(F32).astype(BF16)


def pick_plain(columns):
    heads = columns // HEAD
    col = lax.broadcasted_iota(jnp.int32, (columns, heads * LANES), 1)
    row = lax.broadcasted_iota(jnp.int32, (columns, heads * LANES), 0)
    inner = col & 127
    return ((row == (col >> 7) * HEAD + inner) & (inner < HEAD)).astype(F32).astype(BF16)


def rotated(values, cosine, sine):
    return values * cosine + pltpu.roll(values, LANES // 2, 1) * sine


def spread_qkv(wq, wk, wv, wqkv):
    q_wide = wq.shape[1] // HEAD * LANES
    k_wide = wk.shape[1] // HEAD * LANES
    wqkv[:, :q_wide] = dot_nn(wq[...], pick_split(wq.shape[1])).astype(BF16)
    wqkv[:, q_wide : q_wide + k_wide] = dot_nn(wk[...], pick_split(wk.shape[1])).astype(BF16)
    wqkv[:, q_wide + k_wide :] = dot_nn(wv[...], pick_plain(wv.shape[1])).astype(BF16)


def allowed_pairs(seg_col, seg_row):
    full_rows = seg_col.shape[0]
    row = lax.broadcasted_iota(jnp.int32, (full_rows, full_rows), 0)
    col = lax.broadcasted_iota(jnp.int32, (full_rows, full_rows), 1)
    return (seg_col[...] == seg_row[...]) & (col <= row)


def lane_block(index):
    return pl.ds(pl.multiple_of(index * LANES, LANES), LANES)


def head_rows(ref, index):
    return ref[:, :, lane_block(index)].reshape(-1, LANES)


def attn_weights(weights, wo, sources):
    wq0, wq1, wk0, wk1, wv0, wv1, wo0, wo1 = sources[:8]
    wq, wk, wv = sources[8:]
    weights.want(wq0.at[0], wq1.at[0], wq)
    weights.want(wk0.at[0], wk1.at[0], wk)
    weights.want(wv0.at[0], wv1.at[0], wv)
    for h in range(wo.shape[0]):
        rows = pl.ds(h * HEAD, HEAD)
        weights.want(wo0.at[0, rows], wo1.at[0, rows], wo.at[h, pl.ds(0, HEAD)])


def clear_pads(wo):
    for h in range(wo.shape[0]):
        wo[h, HEAD:] = jnp.zeros((LANES - HEAD, wo.shape[2]), BF16)


def probabilities(queries, keys, allowed):
    scores = jnp.where(allowed, dot_nt(queries, keys) * HEAD ** (-0.5), neg_fill)
    exp_scores = jnp.exp(scores - jnp.max(scores, axis=-1, keepdims=True))
    return exp_scores / jnp.sum(exp_scores, axis=-1, keepdims=True)


def attn_fwd_kernel(layer, n, heads, kv_heads, others, *refs):
    x, gain, cos, sin, seg_col, seg_row = refs[:6]
    own = refs[6 : 6 + others]
    at = 6 + others
    if layer == 0:
        h_out, n_out, qkv_out, o_out = refs[at : at + 4]
        other = refs[at + 4 : at + 4 + others]
    else:
        other = refs[at : at + others]
        h_out, n_out, qkv_out, o_out = refs[at + others : at + others + 4]
    at += 4 + others
    (wq, wk, wv, wo, wqkv, qkv, o, osmall, wsem) = refs[at : at + 9]
    pair = Pair(*refs[at + 9 : at + 12])
    line = Line(n, *refs[at + 12 :])
    me = line.me
    group = heads // kv_heads
    weights = Weights(layer, wsem)
    sources = [ref for both in zip(own[:4], other[:4]) for ref in both] + [wq, wk, wv]
    attn_weights(weights, wo, sources)
    resid = x[...].astype(F32)
    line.full[me] = (resid * rms_scale(resid) * gain[...]).astype(BF16)
    clear_pads(wo)
    if layer == 0:
        weights.start_own()
        line.enter()
        line.gather_step(0)
        for mine, theirs in zip(own, other):
            pair.send(mine, theirs)

        def arrived():
            for index in range(4):
                pair.copy(own[index], other[index], index).wait_recv()

        weights.start_other(arrived)
    else:
        weights.start()
        line.enter()
        line.gather_step(0)
    weights.wait()
    spread_qkv(wq, wk, wv, wqkv)

    def compute(shard):
        products = dot_nn(line.full[shard], wqkv[...])
        for head in range(heads + kv_heads):
            lanes = slice(head * LANES, (head + 1) * LANES)
            qkv[shard, :, lanes] = rotated(products[:, lanes], cos[shard], sin[shard]).astype(BF16)
        lanes = slice((heads + kv_heads) * LANES, None)
        qkv[shard, :, lanes] = products[:, lanes].astype(BF16)

    later_shards(line, compute)
    pair.share(line.full, n_out)
    pair.keep(qkv, qkv_out)
    allowed = allowed_pairs(seg_col, seg_row)

    @pl.loop(0, kv_heads)
    def _(g):
        keys = head_rows(qkv, heads + g)
        values = head_rows(qkv, heads + kv_heads + g)
        rows = []
        for member in range(group):
            h = g * group + member
            probs = probabilities(head_rows(qkv, h), keys, allowed)
            attended = dot_nn(probs.astype(BF16), values).astype(BF16)
            o[:, :, lane_block(h)] = attended.reshape(n, -1, LANES)
            rows.append(attended)
        small = dot_nt(jnp.concatenate(rows, axis=1), pick_plain(group * HEAD))
        osmall[g] = small.astype(BF16).reshape(osmall.shape[1:])

    pair.share_half(osmall, o_out)
    wide = wo.shape[0] * LANES

    def partial(shard):
        return dot_nn(o[shard], wo[...].reshape(wide, -1))

    sums_after(line, partial)
    h_out[...] = resid + partial(me)
    line.sum_take(h_out)
    line.gather_end()
    line.sum_end()
    if layer == 0:
        for index, copy in enumerate(pair.sent[:others]):
            copy.wait_send()
            if index >= 4:
                copy.wait_recv()

        @pl.when(weights.own)
        def _():
            for index in range(4):
                pair.copy(own[index], other[index], index).wait_recv()

        pair.sent = pair.sent[others:]
    pair.wait()


def bound(tasks, sizes, refs):
    groups, at = [], 0
    for own, extra in sizes:
        groups.append((refs[at : at + own], refs[at + own : at + own + extra]))
        at += own + extra
    tasks.bind(*(list(extra) for _, extra in groups))
    return [ref for own, _ in groups for ref in own]


def attn_bwd_kernel(layer, n, heads, kv_heads, tasks, sizes, *refs):
    refs = bound(tasks, sizes, refs)
    (dh, x, gain, cos, sin, seg_col, seg_row, qkv_in) = refs[:8]
    own, other = refs[8:12], refs[12:16]
    (dx_out, gain_out, da_out, dqkv_out) = refs[16:20]
    (wq, wk, wv, wo, wqkv, qkv, d_o, dqkv, dsmall, total, wsem, tsem) = refs[20:32]
    pair = Pair(*refs[32:35])
    line = Line(n, *refs[35:])
    me = line.me
    group = heads // kv_heads
    weights = Weights(layer, wsem)
    sources = [ref for both in zip(own, other) for ref in both] + [wq, wk, wv]
    attn_weights(weights, wo, sources)
    weights.start()
    take = pltpu.make_async_copy(qkv_in, qkv, tsem)
    take.start()
    line.full[me] = dh[...].astype(BF16)
    clear_pads(wo)
    line.enter(tasks.peers())
    line.gather_step(0)
    tasks.start()
    weights.wait()
    spread_qkv(wq, wk, wv, wqkv)
    take.wait()
    wide = wo.shape[0] * LANES

    def compute(shard):
        d_o[shard] = dot_nt(line.full[shard], wo[...].reshape(wide, -1)).astype(BF16)

    later_shards(line, compute)
    pair.share(line.full, da_out)
    tasks.advance()
    allowed = allowed_pairs(seg_col, seg_row)
    cosine = cos[...].reshape(-1, LANES)
    sine = -sin[...].reshape(-1, LANES)
    scale = HEAD ** (-0.5)

    @pl.loop(0, kv_heads)
    def _(g):
        keys = head_rows(qkv, heads + g)
        values = head_rows(qkv, heads + kv_heads + g)
        d_keys = d_values = None
        turned = []
        for member in range(group):
            h = g * group + member
            queries = head_rows(qkv, h)
            d_out = head_rows(d_o, h)
            probs = probabilities(queries, keys, allowed)
            d_probs = dot_nt(d_out, values)
            inner = jnp.sum(probs * d_probs, axis=-1, keepdims=True)
            d_scores = (probs * (d_probs - inner)).astype(BF16)
            d_queries = dot_nn(d_scores, keys) * scale
            turned.append(rotated(d_queries, cosine, sine).astype(BF16))
            dqkv[:, :, lane_block(h)] = turned[-1].reshape(n, -1, LANES)
            dk = dot_tn(d_scores, queries)
            dv = dot_tn(probs.astype(BF16), d_out)
            d_keys = dk if d_keys is None else d_keys + dk
            d_values = dv if d_values is None else d_values + dv
        turned.append(rotated(d_keys * scale, cosine, sine).astype(BF16))
        dqkv[:, :, lane_block(heads + g)] = turned[-1].reshape(n, -1, LANES)
        low_values = d_values.astype(BF16)
        dqkv[:, :, lane_block(heads + kv_heads + g)] = low_values.reshape(n, -1, LANES)
        small = dot_nt(jnp.concatenate(turned, axis=1), pick_split((group + 1) * HEAD))
        small_values = dot_nt(low_values, pick_plain(HEAD))
        dsmall[g] = (
            jnp.concatenate([small, small_values], axis=1).astype(BF16).reshape(dsmall.shape[1:])
        )

    pair.share_half(dsmall, dqkv_out)

    def partial(shard):
        return dot_nt(dqkv[shard], wqkv[...])

    sums_after(line, partial)
    total[...] = partial(me)
    tasks.advance()
    line.sum_take(total)
    d_resid, gain_part = norm_back(total[...], x[...].astype(F32), gain[...])
    dx_out[...] = (dh[...] + d_resid).astype(BF16)
    gain_out[...] = gain_part
    line.gather_end()
    line.sum_end()
    pair.wait()
    tasks.finish()


def ffn_fwd_kernel(layer, n, *refs):
    (h, gain, wg0, wg1, wu0, wu1, wd0, wd1) = refs[:8]
    (y_out, n_out, gate_out, up_out, hid_out) = refs[8:13]
    (wg, wu, wd, gate, up, hid, part, wsem) = refs[13:21]
    pair = Pair(*refs[21:24])
    line = Line(n, *refs[24:])
    me = line.me
    weights = Weights(layer, wsem)
    weights.want(wg0.at[0], wg1.at[0], wg)
    weights.want(wu0.at[0], wu1.at[0], wu)
    weights.want(wd0.at[0], wd1.at[0], wd)
    weights.start()
    resid = h[...]
    line.full[me] = (resid * rms_scale(resid) * gain[...]).astype(BF16)
    line.enter()
    line.gather_step(0)
    weights.wait()
    middle = hid.shape[3]

    def compute(shard):
        rows = line.full[shard]
        g = dot_nn(rows, wg[...])
        u = dot_nn(rows, wu[...])
        gate[shard] = g
        up[shard] = u
        low = (g * jax.nn.sigmoid(g) * u).astype(BF16)
        hid[0, shard] = low[:, :middle]
        hid[1, shard] = low[:, middle:]
        part[shard] = dot_nn(low, wd[...])

    rows_then_sums(line, compute, lambda shard: part[shard])
    pair.share(line.full, n_out)
    pair.share_half(hid, hid_out)
    pair.keep(gate, gate_out)
    pair.keep(up, up_out)
    part[me] += h[...]
    line.sum_take(part.at[me])
    y_out[...] = part[me].astype(BF16)
    line.gather_end()
    line.sum_end()
    pair.wait()


def ffn_bwd_kernel(layer, n, tasks, sizes, *refs):
    refs = bound(tasks, sizes, refs)
    (dy, h, gain, gate_in, up_in, wg0, wg1, wu0, wu1, wd0, wd1) = refs[:11]
    (dh_out, gain_out, df_out, dmid_out) = refs[11:15]
    (wg, wu, wd, gate, up, dmid, part, wsem, tsem) = refs[15:24]
    pair = Pair(*refs[24:27])
    line = Line(n, *refs[27:])
    me = line.me
    weights = Weights(layer, wsem)
    weights.want(wd0.at[0], wd1.at[0], wd)
    weights.want(wg0.at[0], wg1.at[0], wg)
    weights.want(wu0.at[0], wu1.at[0], wu)
    weights.start()
    takes = [
        pltpu.make_async_copy(gate_in, gate, tsem.at[0]),
        pltpu.make_async_copy(up_in, up, tsem.at[1]),
    ]
    for take in takes:
        take.start()
    line.full[me] = dy[...]
    line.enter(tasks.peers())
    line.gather_step(0)
    tasks.start()
    weights.wait()
    for take in takes:
        take.wait()
    middle = dmid.shape[3] // 2

    def compute(shard):
        d_hidden = dot_nt(line.full[shard], wd[...])
        g = gate[shard]
        sig = jax.nn.sigmoid(g)
        d_g = (d_hidden * up[shard] * sig * (1.0 + g * (1.0 - sig))).astype(BF16)
        d_u = (d_hidden * g * sig).astype(BF16)
        for core in range(2):
            lanes = slice(core * middle, (core + 1) * middle)
            dmid[core, shard, :, :middle] = d_g[:, lanes]
            dmid[core, shard, :, middle:] = d_u[:, lanes]
        part[shard] = dot_nt(d_g, wg[...]) + dot_nt(d_u, wu[...])

    rows_then_sums(line, compute, lambda shard: part[shard], tasks.advance)
    pair.share(line.full, df_out)
    pair.share_half(dmid, dmid_out)
    tasks.advance()
    line.sum_take(part.at[me])
    d_resid, gain_part = norm_back(part[me], h[...], gain[...])
    dh_out[...] = dy[...].astype(F32) + d_resid
    gain_out[...] = gain_part
    line.gather_end()
    line.sum_end()
    pair.wait()
    tasks.finish()


def run_kernel(body, args, in_specs, outs, scratch, cid, flops, nbytes, name, aliases=None):
    return pl.pallas_call(
        body,
        input_output_aliases=aliases or {},
        name=name,
        in_specs=in_specs,
        out_shape=[jax.ShapeDtypeStruct(shape, dtype) for shape, dtype, _ in outs],
        out_specs=[spec for _, _, spec in outs],
        scratch_shapes=scratch,
        cost_estimate=pl.CostEstimate(flops=flops, bytes_accessed=nbytes, transcendentals=0),
        compiler_params=pltpu.CompilerParams(
            collective_id=cid, has_side_effects=True, vmem_limit_bytes=44 << 20
        ),
    )(*args)


def attn_forward(layer, n, x, gain, tables, own, other):
    rows, width = x.shape
    heads = own[0].shape[2] // HEAD
    kv_heads = own[1].shape[2] // HEAD
    wide = (heads + 2 * kv_heads) * LANES
    small = heads // kv_heads * HEAD
    args = [x, gain, *tables, *own]
    specs = [VMEM_SPEC] * 6 + [HBM_SPEC] * len(own)
    outs = [
        ((rows, width), F32, VMEM_SPEC),
        ((2, n, rows, width), BF16, HBM_SPEC),
        ((n, rows, wide), BF16, HBM_SPEC),
        ((2, n, rows, small), BF16, HBM_SPEC),
    ]
    if other is None:
        outs += [(weight.shape, weight.dtype, HBM_SPEC) for weight in own]
    else:
        args += [*other]
        specs += [HBM_SPEC] * len(other)
    scratch = (
        [
            VMEM((width, heads * HEAD), BF16),
            VMEM((width, kv_heads * HEAD), BF16),
            VMEM((width, kv_heads * HEAD), BF16),
            VMEM((heads, LANES, width), BF16),
            VMEM((width, wide), BF16),
            VMEM((n, rows, wide), BF16),
            VMEM((n, rows, heads * LANES), BF16),
            VMEM((kv_heads, n, rows, small), BF16),
            DMA((3 + heads,)),
        ]
        + pair_scratch(3, 2 + (len(own) if other is None else 0))
        + line_scratch(n, rows, width)
    )
    body = functools.partial(attn_fwd_kernel, layer, n, heads, kv_heads, len(own))
    flops = 2 * n * rows * width * wide * 3 // 2
    return run_kernel(body, args, specs, outs, scratch, 1 + layer, flops, 8 << 20, f"attn_fwd{layer}")


def attn_backward(layer, n, dh, x, gain, tables, qkv, own, other, tasks):
    rows, width = x.shape
    heads = own[0].shape[2] // HEAD
    kv_heads = own[1].shape[2] // HEAD
    wide = (heads + 2 * kv_heads) * LANES
    small = (heads // kv_heads + 2) * HEAD
    args = [dh, x, gain, *tables, qkv, *own, *other]
    specs = [VMEM_SPEC] * 7 + [HBM_SPEC] * 9
    outs = [
        ((rows, width), BF16, VMEM_SPEC),
        ((1, width), F32, VMEM_SPEC),
        ((2, n, rows, width), BF16, HBM_SPEC),
        ((2, n, rows, small), BF16, HBM_SPEC),
    ]
    scratch = (
        [
            VMEM((width, heads * HEAD), BF16),
            VMEM((width, kv_heads * HEAD), BF16),
            VMEM((width, kv_heads * HEAD), BF16),
            VMEM((heads, LANES, width), BF16),
            VMEM((width, wide), BF16),
            VMEM((n, rows, wide), BF16),
            VMEM((n, rows, heads * LANES), BF16),
            VMEM((n, rows, wide), BF16),
            VMEM((kv_heads, n, rows, small), BF16),
            VMEM((rows, width), F32),
            DMA((3 + heads,)),
            DMA,
        ]
        + pair_scratch(2, 2)
        + line_scratch(n, rows, width)
    )
    body = functools.partial(attn_bwd_kernel, layer, n, heads, kv_heads)
    flops = 2 * n * rows * width * wide * 2
    return run_with_tasks(
        body, tasks, args, specs, outs, scratch, 3 + layer, flops, 8 << 20, f"attn_bwd{layer}"
    )


def ffn_forward(layer, n, h, gain, own, other):
    rows, width = h.shape
    hidden = own[0].shape[2]
    args = [h, gain]
    for mine, theirs in zip(own, other):
        args += [mine, theirs]
    specs = [VMEM_SPEC] * 2 + [HBM_SPEC] * 6
    outs = [
        ((rows, width), BF16, VMEM_SPEC),
        ((2, n, rows, width), BF16, HBM_SPEC),
        ((n, rows, hidden), F32, HBM_SPEC),
        ((n, rows, hidden), F32, HBM_SPEC),
        ((2, n, rows, hidden // 2), BF16, HBM_SPEC),
    ]
    scratch = (
        [
            VMEM((width, hidden), BF16),
            VMEM((width, hidden), BF16),
            VMEM((hidden, width), BF16),
            VMEM((n, rows, hidden), F32),
            VMEM((n, rows, hidden), F32),
            VMEM((2, n, rows, hidden // 2), BF16),
            VMEM((n, rows, width), F32),
            DMA((3,)),
        ]
        + pair_scratch(4, 2)
        + line_scratch(n, rows, width)
    )
    body = functools.partial(ffn_fwd_kernel, layer, n)
    flops = 6 * n * rows * width * hidden
    return run_kernel(body, args, specs, outs, scratch, 5 + layer, flops, 16 << 20, f"ffn_fwd{layer}")


def ffn_backward(layer, n, dy, h, gain, gate, up, own, other, tasks):
    rows, width = h.shape
    hidden = own[0].shape[2]
    args = [dy, h, gain, gate, up]
    for mine, theirs in zip(own, other):
        args += [mine, theirs]
    specs = [VMEM_SPEC] * 3 + [HBM_SPEC] * 8
    outs = [
        ((rows, width), F32, VMEM_SPEC),
        ((1, width), F32, VMEM_SPEC),
        ((2, n, rows, width), BF16, HBM_SPEC),
        ((2, n, rows, hidden), BF16, HBM_SPEC),
    ]
    scratch = (
        [
            VMEM((width, hidden), BF16),
            VMEM((width, hidden), BF16),
            VMEM((hidden, width), BF16),
            VMEM((n, rows, hidden), F32),
            VMEM((n, rows, hidden), F32),
            VMEM((2, n, rows, hidden), BF16),
            VMEM((n, rows, width), F32),
            DMA((3,)),
            DMA((2,)),
        ]
        + pair_scratch(2, 2)
        + line_scratch(n, rows, width)
    )
    body = functools.partial(ffn_bwd_kernel, layer, n)
    flops = 6 * n * rows * width * hidden
    return run_with_tasks(
        body, tasks, args, specs, outs, scratch, 7 + layer, flops, 16 << 20, f"ffn_bwd{layer}"
    )


def run_with_tasks(body, tasks, args, specs, outs, scratch, cid, flops, nbytes, name):
    more_args, more_outs, more_scratch = tasks.arguments(), tasks.outputs(), tasks.scratch()
    sizes = (
        (len(args), len(more_args)),
        (len(outs), len(more_outs)),
        (len(scratch), len(more_scratch)),
    )
    return run_kernel(
        functools.partial(body, tasks, sizes),
        args + more_args,
        specs + [HBM_SPEC] * len(more_args),
        outs + more_outs,
        scratch + more_scratch,
        cid,
        flops,
        nbytes,
        name,
    )


def tail_kernel(n, count, sizes, *refs):
    ffn_size, attn_size = sizes
    at = 0

    def take(number):
        nonlocal at
        at += number
        return list(refs[at - number : at])

    (gains,) = take(1)
    ffn_blocks, attn_arrays, _aliased = take(ffn_size), take(attn_size), take(ffn_size + attn_size)
    (gains_out,) = take(1)
    ffn_outs, attn_outs = take(ffn_size), take(attn_size)
    by_tensor, by_dp, by_core = take(3)
    small_sems = take(2)
    ffn_vmem, attn_vmem = take(ffn_size), take(attn_size)
    (load_sem,) = take(1)
    ffn_sems, attn_sems = take(3), take(3)
    reduce = Reduce(0, count, attn_arrays, attn_vmem, take(len(refs) - at))
    gather_ffn = Gather(0, count, ffn_vmem, ffn_outs, ffn_sems)
    gather_attn = Gather(0, count, attn_vmem, attn_outs, attn_sems)
    loads = [
        pltpu.make_async_copy(ffn_blocks[a], ffn_vmem[a], load_sem.at[a]) for a in range(ffn_size)
    ]
    for load in loads:
        load.start()
    axes = (("tensor", n, by_tensor), ("dp", count, by_dp), ("section", 2, by_core))
    barrier = pltpu.get_barrier_semaphore()
    peers = 0
    for axis, size, _ in axes:
        place = lax.axis_index(axis)
        for shift in range(1, size):
            pl.semaphore_signal(
                barrier, 1, device_id={axis: (place + shift) % size}, device_id_type=MESH
            )
            peers += 1
    pl.semaphore_wait(barrier, peers)

    def small(stage, shift):
        axis, size, slots = axes[stage]
        place = lax.axis_index(axis)
        ref = slots.at[place]
        return pltpu.make_async_remote_copy(
            ref,
            ref,
            small_sems[0].at[stage, shift],
            small_sems[1].at[stage, shift],
            device_id={axis: (place + shift) % size},
            device_id_type=MESH,
        )

    def small_start(stage, value):
        axis, size, slots = axes[stage]
        slots[lax.axis_index(axis)] = value
        for shift in range(1, size):
            small(stage, shift).start()

    def small_end(stage):
        _, size, slots = axes[stage]
        for shift in range(1, size):
            small(stage, shift).wait()
        value = slots[0]
        for index in range(1, size):
            value = value + slots[index]
        return value

    small_start(0, gains[...])
    reduce.start()
    for load in loads:
        load.wait()
    gather_ffn.start()
    small_start(1, small_end(0))
    reduce.advance()
    small_start(2, small_end(1))
    gather_ffn.advance()
    reduce.finish()
    gather_attn.start()
    gains_out[...] = small_end(2)
    gather_attn.advance()
    gather_ffn.finish()
    gather_attn.finish()


def tail(n, count, gains, ffn_blocks, attn_arrays, ffn_full, attn_full):
    sizes = (len(ffn_blocks), len(attn_arrays))
    args = [gains, *ffn_blocks, *attn_arrays, *ffn_full, *attn_full]
    specs = [VMEM_SPEC] + [HBM_SPEC] * (len(args) - 1)
    outs = [(gains.shape, F32, VMEM_SPEC)]
    outs += [(full.shape, BF16, HBM_SPEC) for full in (*ffn_full, *attn_full)]
    scratch = [VMEM((size,) + gains.shape, F32) for size in (n, count, 2)]
    scratch += [DMA((3, max(n, count, 2)))] * 2
    scratch += [VMEM(block.shape, BF16) for block in ffn_blocks]
    scratch += [VMEM((2, 2) + array.shape[-2:], BF16) for array in attn_arrays]
    scratch += [DMA((sizes[0],))]
    scratch += gather_sems(count, sizes[0]) + gather_sems(count, sizes[1])
    scratch += reduce_scratch(count, [array.shape for array in attn_arrays])
    first = 1 + sizes[0] + sizes[1]
    aliases = {first + index: 1 + index for index in range(sum(sizes))}
    body = functools.partial(tail_kernel, n, count, sizes)
    return run_kernel(body, args, specs, outs, scratch, 9, 1 << 20, 16 << 20, "tail", aliases)


def swap(values):
    return lax.ppermute(values, "section", [(0, 1), (1, 0)])


def segment_tables(lengths_row, n, rows):
    full_rows = n * rows
    slot_count = lengths_row.shape[0]
    seq_ends = jnp.cumsum(lengths_row)
    row_index = jnp.arange(full_rows, dtype=jnp.int32)
    segment = jnp.sum((row_index[:, None] >= seq_ends[None, :]).astype(jnp.int32), axis=1)
    starts = jnp.concatenate([seq_ends - lengths_row, seq_ends[-1:]])
    chosen = segment[:, None] == jnp.arange(slot_count + 1, dtype=jnp.int32)[None, :]
    position = row_index - jnp.sum(jnp.where(chosen, starts[None, :], 0), axis=1)
    segment = jnp.where(segment < slot_count, segment, slot_count + row_index)
    lane = jnp.arange(LANES, dtype=jnp.int32)
    inner = lane % (LANES // 2)
    inverse = rope_base ** (-inner.astype(F32) * 2.0 / HEAD)
    angle = position.astype(F32)[:, None] * inverse[None, :]
    live = (inner < HALF)[None, :]
    sign = jnp.where(lane < LANES // 2, -1.0, 1.0)[None, :]
    cosine = jnp.where(live, jnp.cos(angle), 0.0)
    sine = jnp.where(live, sign * jnp.sin(angle), 0.0)
    shape = (n, rows, LANES)
    return cosine.reshape(shape), sine.reshape(shape), segment[:, None], segment[None, :]


def shards(
    inputs,
    cotangent,
    seq_lengths,
    gain_attn,
    w_query,
    w_key,
    w_value,
    w_out,
    gain_ffn,
    w_gate,
    w_up,
    w_down,
):
    section = lax.axis_index("section")
    first = section == 0
    n = lax.axis_size("tensor")
    rows, width = inputs.shape[1:]

    def mine(stacked):
        return jnp.where(first, stacked[0], stacked[1])

    attn_own = (w_query, w_key, w_value, w_out)
    ffn_own = (w_gate, w_up, w_down)
    gains = jnp.concatenate([gain_attn, gain_ffn], axis=0)
    gains_other = swap(gains)
    gains_by_layer = [
        jnp.where(first, gains, gains_other).astype(F32),
        jnp.where(first, gains_other, gains).astype(F32),
    ]
    tables = segment_tables(mine(seq_lengths[0]), n, rows)

    x = mine(inputs)
    kept = []
    outs = []
    for layer in range(2):
        gain_a, gain_f = gains_by_layer[layer][0:1], gains_by_layer[layer][1:2]
        if layer == 0:
            h, n_all, qkv, o, *swapped = attn_forward(
                layer, n, x, gain_a, tables, attn_own + ffn_own, None
            )
            attn_other, ffn_other = tuple(swapped[:4]), tuple(swapped[4:])
        else:
            h, n_all, qkv, o = attn_forward(layer, n, x, gain_a, tables, attn_own, attn_other)
        y, n2_all, gate, up, hid = ffn_forward(layer, n, h, gain_f, ffn_own, ffn_other)
        kept.append((x, h, n_all, qkv, o, n2_all, gate, up, hid, gain_a, gain_f))
        outs.append(y)
        x = y

    count = lax.axis_size("dp")
    cube = (2,) + (2,) * (count.bit_length() - 1)

    def weight_grad(left, right):
        left = left.reshape(-1, left.shape[-1])
        right = right.reshape(-1, right.shape[-1])
        return dot_tn(left, right).astype(BF16)

    def blocked(array):
        return array.reshape(*cube, -1, array.shape[-1])

    dy = mine(cotangent)
    in_grads = [None, None]
    gain_parts = [None, None]
    sums = {}
    ffn_grad = attn_grad = None
    for layer in (1, 0):
        x, h, n_all, qkv, o, n2_all, gate, up, hid, gain_a, gain_f = kept[layer]
        plan = {}
        if layer == 0:
            plan = {"reduce": (1, attn_grad), "gather": (1, sums["ffn1"])}
        dh, gf_part, df_all, dmid, *more = ffn_backward(
            layer, n, dy, h, gain_f, gate, up, ffn_own, ffn_other, Tasks(count, plan)
        )
        if layer == 0:
            sums["attn1"], ffn_full = more[:2], more[2:]
        ffn_grad = [blocked(weight_grad(n2_all, dmid)), blocked(weight_grad(hid, df_all))]
        plan = {"reduce": (layer, ffn_grad)}
        if layer == 0:
            plan["gather"] = (1, sums["attn1"])
        dx, ga_part, da_all, dqkv, *more = attn_backward(
            layer, n, dh, x, gain_a, tables, qkv, attn_own, attn_other, Tasks(count, plan)
        )
        sums[f"ffn{layer}"] = more[:2]
        if layer == 0:
            attn_full = more[2:]
        attn_grad = [blocked(weight_grad(n_all, dqkv)), blocked(weight_grad(o, da_all))]
        gain_parts[layer] = jnp.concatenate([ga_part, gf_part], axis=0)
        in_grads[layer] = dx
        dy = dx
    gain_sums, g_mid, g_down, g_qkv, g_out = tail(
        n,
        count,
        jnp.concatenate(gain_parts, axis=0),
        sums["ffn0"],
        attn_grad,
        ffn_full,
        attn_full,
    )
    gain_own = jnp.where(first, gain_sums[0:2], gain_sums[2:4])
    g_mid, g_qkv = (array.reshape(2, -1, array.shape[-1]) for array in (g_mid, g_qkv))
    g_down, g_out = (array.reshape(-1, array.shape[-1]).astype(F32)[None] for array in (g_down, g_out))

    def columns(array, start, size):
        parts = [array[core, :, start : start + size].astype(F32) for core in range(2)]
        return jnp.concatenate(parts, axis=1)[None]

    mid = w_gate.shape[2] // 2
    g_gate, g_up = columns(g_mid, 0, mid), columns(g_mid, mid, mid)
    q_half, k_half = w_query.shape[2] // 2, w_key.shape[2] // 2
    g_query = columns(g_qkv, 0, q_half)
    g_key, g_value = (columns(g_qkv, q_half + at, k_half) for at in (0, k_half))

    def by_layer(values):
        keep = jnp.where(first, values[0], values[1])
        got = swap(jnp.where(first, values[1], values[0]))
        return jnp.stack([jnp.where(first, keep, got), jnp.where(first, got, keep)])[None]

    return (
        by_layer(outs),
        by_layer(in_grads),
        gain_own[0:1],
        g_query,
        g_key,
        g_value,
        g_out,
        gain_own[1:2],
        g_gate,
        g_up,
        g_down,
    )


def solution(mesh):
    placed = (
        P(None, ("dp", "tensor"), None),
        P(None, ("dp", "tensor"), None),
        P("dp", None, None),
        P("section", None),
        P("section", None, "tensor"),
        P("section", None, "tensor"),
        P("section", None, "tensor"),
        P("section", "tensor", None),
        P("section", None),
        P("section", None, "tensor"),
        P("section", None, "tensor"),
        P("section", "tensor", None),
    )
    return jax.shard_map(
        shards,
        mesh=mesh,
        in_specs=placed,
        out_specs=(
            P("section", None, ("dp", "tensor"), None),
            P("section", None, ("dp", "tensor"), None),
            P("section", None),
            P("section", None, "tensor"),
            P("section", None, "tensor"),
            P("section", None, "tensor"),
            P("section", "tensor", None),
            P("section", None),
            P("section", None, "tensor"),
            P("section", None, "tensor"),
            P("section", "tensor", None),
        ),
        check_vma=False,
    )
```

```python
import functools

import jax
import jax.numpy as jnp
from jax import lax
from jax.experimental import pallas as pl
from jax.experimental.pallas import tpu as pltpu
from jax.sharding import PartitionSpec as P

HEAD = 96
HALF = HEAD // 2
LANES = 128
CHUNKS = 3
BF16 = jnp.bfloat16
F32 = jnp.float32
MESH = pl.DeviceIdType.MESH
VMEM = pltpu.VMEM
VMEM_SPEC = pl.BlockSpec(memory_space=pltpu.VMEM)
LOAD, LOAD_MINE = "load", "load mine"
HBM_SPEC = pl.BlockSpec(memory_space=pltpu.HBM)
DMA = pltpu.SemaphoreType.DMA

eps = 1e-05
rope_base = 100000.0
neg_fill = -1e30


def dot_nn(left, right):
    return lax.dot_general(left, right, (((1,), (0,)), ((), ())), preferred_element_type=F32)


def dot_nt(left, right):
    return lax.dot_general(left, right, (((1,), (1,)), ((), ())), preferred_element_type=F32)


def dot_tn(left, right):
    return lax.dot_general(left, right, (((0,), (0,)), ((), ())), preferred_element_type=F32)


def rms_scale(values):
    return lax.rsqrt(jnp.mean(values * values, axis=-1, keepdims=True) + eps)


def norm_back(d_normed, resid, gain):
    scale_rows = rms_scale(resid)
    unit_rows = resid * scale_rows
    gain_part = jnp.sum(d_normed * unit_rows, axis=0, keepdims=True)
    d_unit = d_normed * gain
    inner = jnp.mean(d_unit * unit_rows, axis=-1, keepdims=True)
    return scale_rows * (d_unit - unit_rows * inner), gain_part


class Line:
    def __init__(self, count, full, rbuf, sbuf, gs, gr, ss, sr):
        self.n = count
        self.core = lax.axis_index("section")
        self.me = lax.axis_index("tensor")
        self.full, self.rbuf, self.sbuf = full, rbuf, sbuf
        self.gs, self.gr, self.ss, self.sr = gs, gr, ss, sr
        self.rows = full.shape[1] // CHUNKS

    def span(self, c):
        return pl.ds(c * self.rows, self.rows)

    def neighbour(self, d):
        return self.me + 1 if d == 0 else self.me - 1

    def enter(self, also=()):
        me, n = self.me, self.n
        barrier = pltpu.get_barrier_semaphore()
        for peer in ({"section": 1 - self.core}, *also):
            pl.semaphore_signal(barrier, 1, device_id=peer, device_id_type=MESH)
        for d, there in ((1, me > 0), (0, me < n - 1)):

            @pl.when(there)
            def _():
                pl.semaphore_signal(
                    barrier, 1, device_id={"tensor": self.neighbour(d)}, device_id_type=MESH
                )

        peers = 1 + len(also) + (me > 0).astype(jnp.int32) + (me < n - 1).astype(jnp.int32)
        pl.semaphore_wait(barrier, peers)

    def gather_copy(self, d, step, shard, c):
        ref = self.full.at[shard, self.span(c)]
        return pltpu.make_async_remote_copy(
            ref,
            ref,
            self.gs.at[d, step, c],
            self.gr.at[d, step, c],
            device_id={"tensor": self.neighbour(d)},
            device_id_type=MESH,
        )

    def gather_step(self, step):
        me, n = self.me, self.n
        for c in range(CHUNKS):
            for d in range(2):
                shard = me - step if d == 0 else me + step
                holds = (shard >= 0) & (shard < n)
                onward = (me + 1 < n) if d == 0 else (me > 0)

                @pl.when(holds & (step > 0))
                def _():
                    self.gather_copy(d, step - 1, shard, c).wait_recv()

                @pl.when(holds & onward)
                def _():
                    self.gather_copy(d, step, shard, c).start()

    def gather_end(self):
        me, n = self.me, self.n

        @pl.loop(0, n - 1)
        def _(step):
            for c in range(CHUNKS):
                for d in range(2):
                    shard = me - step if d == 0 else me + step
                    onward = (me + 1 < n) if d == 0 else (me > 0)

                    @pl.when((shard >= 0) & (shard < n) & onward)
                    def _():
                        self.gather_copy(d, step, shard, c).wait_send()

    def sum_copy(self, d, shard, c):
        return pltpu.make_async_remote_copy(
            self.sbuf.at[shard, self.span(c)],
            self.rbuf.at[d, shard, self.span(c)],
            self.ss.at[d, shard, c],
            self.sr.at[d, shard, c],
            device_id={"tensor": self.neighbour(d)},
            device_id_type=MESH,
        )

    def sum_step(self, d, shard, partial):
        me, n = self.me, self.n
        goes = (shard > me) & (shard < n) if d == 0 else (shard >= 0) & (shard < me)
        first = (me == 0) if d == 0 else (me == n - 1)

        @pl.when(goes & first)
        def _():
            mine = partial(shard)
            for c in range(CHUNKS):
                rows = slice(c * self.rows, (c + 1) * self.rows)
                self.sbuf[shard, self.span(c)] = mine[rows].astype(BF16)
                self.sum_copy(d, shard, c).start()

        @pl.when(goes & jnp.logical_not(first))
        def _():
            mine = partial(shard)
            for c in range(CHUNKS):
                rows = slice(c * self.rows, (c + 1) * self.rows)
                self.sum_copy(d, shard, c).wait_recv()
                arrived = self.rbuf[d, shard, self.span(c)].astype(F32)
                self.sbuf[shard, self.span(c)] = (mine[rows] + arrived).astype(BF16)
                self.sum_copy(d, shard, c).start()

    def sum_take(self, total):
        me, n = self.me, self.n
        for d, there in ((0, me > 0), (1, me < n - 1)):

            @pl.when(there)
            def _():
                for c in range(CHUNKS):
                    self.sum_copy(d, me, c).wait_recv()
                    total[self.span(c)] += self.rbuf[d, me, self.span(c)].astype(F32)

    def sum_end(self):
        me, n = self.me, self.n

        @pl.loop(0, n)
        def _(shard):
            for d, goes in ((0, shard > me), (1, shard < me)):

                @pl.when(goes)
                def _():
                    for c in range(CHUNKS):
                        self.sum_copy(d, shard, c).wait_send()


def line_scratch(count, rows, width):
    return [
        VMEM((count, rows, width), BF16),
        VMEM((2, count, rows, width), BF16),
        VMEM((count, rows, width), BF16),
        DMA((2, count, CHUNKS)),
        DMA((2, count, CHUNKS)),
        DMA((2, count, CHUNKS)),
        DMA((2, count, CHUNKS)),
    ]


def rows_then_sums(line, compute, partial, halfway=lambda: None):
    me, n = line.me, line.n

    @pl.loop(0, 2 * n - 1)
    def _(step):
        @pl.when((step > 0) & (step < n))
        def _():
            line.gather_step(step)

        @pl.when(step == n - 1)
        def _():
            halfway()

        @pl.when(step < n)
        def _():
            @pl.loop(0, 2)
            def _(side):
                shard = jnp.where(side == 0, me - step, me + step)

                @pl.when((shard >= 0) & (shard < n) & ((step > 0) | (side == 0)))
                def _():
                    compute(shard)

        line.sum_step(0, step - me, partial)
        line.sum_step(1, 2 * (n - 1) - step - me, partial)


def later_shards(line, compute):
    me, n = line.me, line.n

    @pl.loop(0, n)
    def _(step):
        @pl.when(step > 0)
        def _():
            line.gather_step(step)

        @pl.loop(0, 2)
        def _(side):
            shard = jnp.where(side == 0, me - step, me + step)

            @pl.when((shard >= 0) & (shard < n) & ((step > 0) | (side == 0)))
            def _():
                compute(shard)


def sums_after(line, partial, each=lambda step: None):
    me, n = line.me, line.n

    @pl.loop(0, n - 1)
    def _(step):
        line.sum_step(0, me + n - 1 - step, partial)
        line.sum_step(1, step - (n - 1 - me), partial)
        each(step)


def sums_alone(line, compute, partial, halfway):
    me, n = line.me, line.n

    @pl.loop(0, n)
    def _(step):
        @pl.loop(0, 2)
        def _(side):
            shard = jnp.where(side == 0, me + n - 1 - step, step - (n - 1 - me))
            first = jnp.where(side == 0, me, 0)
            last = jnp.where(side == 0, n, me)

            @pl.when((shard >= first) & (shard < last))
            def _():
                compute(shard)

        line.sum_step(0, me + n - 1 - step, partial)
        line.sum_step(1, step - (n - 1 - me), partial)

        @pl.when(step == n - 2)
        def _():
            halfway()


class Weights:
    def __init__(self, layer, sems):
        self.own = lax.axis_index("section") == layer
        self.sems = sems
        self.wanted = []

    def want(self, mine, theirs, target):
        self.wanted.append((mine, theirs, target))

    def start_own(self):
        @pl.when(self.own)
        def _():
            for index, (mine, _theirs, target) in enumerate(self.wanted):
                pltpu.make_async_copy(mine, target, self.sems.at[index]).start()

    def start_other(self, before=lambda: None):
        @pl.when(jnp.logical_not(self.own))
        def _():
            before()
            for index, (_mine, theirs, target) in enumerate(self.wanted):
                pltpu.make_async_copy(theirs, target, self.sems.at[index]).start()

    def start(self):
        self.start_own()
        self.start_other()

    def wait(self):
        for index, (mine, _theirs, target) in enumerate(self.wanted):
            pltpu.make_async_copy(mine, target, self.sems.at[index]).wait()


class Pair:
    def __init__(self, local_sems, send_sems, recv_sems):
        self.core = lax.axis_index("section")
        self.sems = local_sems, send_sems, recv_sems
        self.kept, self.sent = [], []
        self.streams = []

    def keep(self, source, target):
        copy = pltpu.make_async_copy(source, target, self.sems[0].at[len(self.kept), 0])
        copy.start()
        self.kept.append(copy)

    def copy(self, source, target, index, part=0):
        return pltpu.make_async_remote_copy(
            source,
            target,
            self.sems[1].at[index, part],
            self.sems[2].at[index, part],
            device_id={"section": 1 - self.core},
            device_id_type=MESH,
        )

    def send(self, source, target):
        copy = self.copy(source, target, len(self.sent))
        copy.start()
        self.sent.append(copy)

    def share_half(self, halves, pair):
        self.keep(halves.at[self.core], pair.at[0])
        self.send(halves.at[1 - self.core], pair.at[1])

    def stream_keep(self, source, target):
        self.streams.append((source, target, len(self.kept), None))
        self.kept.append(None)

    def stream_share(self, source, pair):
        self.stream_keep(source, pair.at[0])
        self.streams.append((source, pair.at[1], None, len(self.sent)))
        self.sent.append(None)

    def stream_share_half(self, halves, pair):
        self.stream_keep(halves.at[self.core], pair.at[0])
        self.streams.append((halves.at[1 - self.core], pair.at[1], None, len(self.sent)))
        self.sent.append(None)

    def streamed(self, shard):
        copies = []
        for source, target, kept, sent in self.streams:
            pieces = source.at[shard], target.at[shard]
            if sent is None:
                copies.append(pltpu.make_async_copy(*pieces, self.sems[0].at[kept, shard]))
            else:
                copies.append(self.copy(*pieces, sent, shard))
        return copies

    def stream(self, shard):
        for copy in self.streamed(shard):
            copy.start()

    def wait(self, count=0):
        for copy in self.kept + self.sent:
            if copy is not None:
                copy.wait()
        if self.streams:

            @pl.loop(0, count)
            def _(shard):
                for copy in self.streamed(shard):
                    copy.wait()


def pair_scratch(count, kept, sent):
    return [DMA((max(kept, 1), count)), DMA((max(sent, 1), count)), DMA((max(sent, 1), count))]


class Cube:
    def __init__(self, layer, count):
        self.bits = count.bit_length() - 1
        assert count == 1 << self.bits
        self.me = lax.axis_index("dp")
        self.core = lax.axis_index("section")
        self.active = self.core == layer
        self.bit = [(self.me // (1 << b)) % 2 for b in range(self.bits)]
        self.down = list(range(self.bits - 1, -1, -1))

    def order(self, colour):
        return list(range(self.bits)) if colour == 0 else self.down

    def peer(self, b):
        return {"dp": self.me + (1 - 2 * self.bit[b]) * (1 << b)}

    def peers(self):
        return [self.peer(b) for b in range(self.bits)]


class Reduce(Cube):
    def __init__(self, layer, count, sources, outs, scratch):
        super().__init__(layer, count)
        self.sources, self.outs = sources, outs
        size = len(sources)
        self.accs = scratch[:size]
        self.recvs = [scratch[size * (t + 1) : size * (t + 2)] for t in range(self.bits)]
        self.local, self.ss, self.sr, self.fs = scratch[size * (self.bits + 1) :]
        self.t = 0
        self.place = [
            {b: slice(None) for b in self.down if b != self.order(c)[0]} for c in range(2)
        ]

    def items(self):
        return [(a, c) for a in range(len(self.sources)) for c in range(2)]

    def spot(self, c, changed=()):
        place = {**self.place[c], **dict(changed)}
        return (c, *(place[b] for b in self.down if b in place))

    def first_half(self, a, c, value):
        b = self.order(c)[0]
        index = [slice(None)] * self.bits
        index[self.down.index(b)] = value
        return self.sources[a].at[(c, *index)]

    def copy(self, a, c, t, source):
        return pltpu.make_async_remote_copy(
            source,
            self.recvs[t][a].at[c],
            self.ss.at[a, c, t],
            self.sr.at[a, c, t],
            device_id=self.peer(self.order(c)[t]),
            device_id_type=MESH,
        )

    def kept(self, a, c):
        mine = self.first_half(a, c, self.bit[self.order(c)[0]])
        return pltpu.make_async_copy(mine, self.accs[a].at[c], self.local.at[a, c])

    def start(self):
        for a, c in self.items():
            other = self.first_half(a, c, 1 - self.bit[self.order(c)[0]])
            self.copy(a, c, 0, other).start()
            self.kept(a, c).start()

    def advance(self):
        t = self.t
        if t >= self.bits:
            return
        for a, c in self.items():
            if t == 0:
                self.kept(a, c).wait()
            self.copy(a, c, t, self.recvs[t][a].at[c]).wait_recv()
            acc, spot = self.accs[a], self.spot(c)
            acc[spot] = (acc[spot].astype(F32) + self.recvs[t][a][c].astype(F32)).astype(BF16)
            if t + 1 < self.bits:
                b = self.order(c)[t + 1]
                self.copy(a, c, t + 1, acc.at[self.spot(c, [(b, 1 - self.bit[b])])]).start()
        if t + 1 < self.bits:
            for c in range(2):
                b = self.order(c)[t + 1]
                self.place[c][b] = self.bit[b]
        self.t = t + 1

    def put_away(self, a, c):
        return pltpu.make_async_copy(
            self.accs[a].at[self.spot(c)], self.outs[a].at[c], self.fs.at[a, c]
        )

    def finish(self):
        while self.t < self.bits:
            self.advance()
        for a, c in self.items():
            self.put_away(a, c).start()
        for a, c in self.items():
            for t in range(self.bits):
                self.copy(a, c, t, self.recvs[t][a].at[c]).wait_send()
        for a, c in self.items():
            self.put_away(a, c).wait()


class Gather(Cube):
    def __init__(self, layer, count, blocks, outs, sems):
        super().__init__(layer, count)
        self.blocks, self.outs = blocks, outs
        self.keep, self.ss, self.sr, self.hs, self.hr = sems
        self.t = 0
        off_layer = 1 - self.core if layer == 1 else self.core
        self.slot = self.core * (1 - off_layer) + 2 * off_layer

    def items(self):
        return [(a, c) for a in range(len(self.blocks)) for c in range(2)]

    def order(self, colour):
        return super().order(colour)[::-1]

    def region(self, a, c, t, half, flipped=None):
        order = self.order(c)
        index = []
        for b in self.down:
            if b in order[:t]:
                index.append(slice(None))
            else:
                index.append(1 - self.bit[b] if flipped == order.index(b) else self.bit[b])
        return self.outs[a].at[(half, c, *index)]

    def copy(self, a, c, t):
        target = self.region(a, c, t, self.slot)
        return pltpu.make_async_remote_copy(
            self.blocks[a].at[c] if t == 0 else target,
            target,
            self.ss.at[a, c, t],
            self.sr.at[a, c, t],
            device_id=self.peer(self.order(c)[t]),
            device_id_type=MESH,
        )

    def kept(self, a, c):
        return pltpu.make_async_copy(
            self.blocks[a].at[c], self.region(a, c, 0, self.slot), self.keep.at[a, c]
        )

    def hand_over(self, a, c, t):
        if t == 0:
            source, target = self.blocks[a].at[c], self.region(a, c, 0, self.core)
        else:
            source = self.region(a, c, t - 1, self.slot, t - 1)
            target = self.region(a, c, t - 1, self.core, t - 1)
        return pltpu.make_async_remote_copy(
            source,
            target,
            self.hs.at[a, c, t],
            self.hr.at[a, c, t],
            device_id={"section": 1 - self.core},
            device_id_type=MESH,
        )

    def pass_on(self, t):
        @pl.when(jnp.logical_not(self.active))
        def _():
            for a, c in self.items():
                self.hand_over(a, c, t).start()

    def start(self):
        for a, c in self.items():
            self.copy(a, c, 0).start()
            self.kept(a, c).start()
        self.pass_on(0)

    def advance(self):
        t = self.t
        if t >= self.bits:
            return
        for a, c in self.items():
            if t == 0:
                self.kept(a, c).wait()
            self.copy(a, c, t).wait_recv()
            if t + 1 < self.bits:
                self.copy(a, c, t + 1).start()
        self.pass_on(t + 1)
        self.t = t + 1

    def finish(self):
        while self.t < self.bits:
            self.advance()
        for a, c in self.items():
            for t in range(self.bits):
                self.copy(a, c, t).wait_send()

        @pl.when(self.active)
        def _():
            for a, c in self.items():
                for t in range(self.bits + 1):
                    self.hand_over(a, c, t).wait_recv()

        @pl.when(jnp.logical_not(self.active))
        def _():
            for a, c in self.items():
                for t in range(self.bits + 1):
                    self.hand_over(a, c, t).wait_send()


def reduce_scratch(count, arrays):
    bits = count.bit_length() - 1
    scratch = []
    for level in (1, *range(1, bits + 1)):
        scratch += [VMEM((2,) + (2,) * (bits - level) + shape[-2:], BF16) for shape in arrays]
    size = len(arrays)
    return scratch + [
        DMA((size, 2)),
        DMA((size, 2, bits)),
        DMA((size, 2, bits)),
        DMA((size, 2)),
    ]


def gather_sems(count, size):
    bits = count.bit_length() - 1
    return [
        DMA((size, 2)),
        DMA((size, 2, bits)),
        DMA((size, 2, bits)),
        DMA((size, 2, bits + 1)),
        DMA((size, 2, bits + 1)),
    ]


class Tasks:
    def __init__(self, count, plan):
        self.count = count
        self.reduce = plan.get("reduce")
        self.gather = plan.get("gather")

    def arguments(self):
        args = list(self.reduce[1]) if self.reduce else []
        return args + (list(self.gather[1]) if self.gather else [])

    def outputs(self):
        outs = []
        if self.reduce:
            outs += [((2,) + ref.shape[-2:], BF16, HBM_SPEC) for ref in self.reduce[1]]
        if self.gather:
            middle = (2,) * (self.count.bit_length() - 1)
            outs += [
                ((3, 2) + middle + ref.shape[-2:], BF16, HBM_SPEC) for ref in self.gather[1]
            ]
        return outs

    def scratch(self):
        scratch = []
        if self.reduce:
            scratch += reduce_scratch(self.count, [ref.shape for ref in self.reduce[1]])
        if self.gather:
            scratch += [VMEM(ref.shape, BF16) for ref in self.gather[1]]
            scratch += [DMA((len(self.gather[1]),))]
            scratch += gather_sems(self.count, len(self.gather[1]))
        return scratch

    def bind(self, args, outs, scratch):
        self.running = []
        self.loads = []
        count = self.count
        if self.reduce:
            size = len(self.reduce[1])
            used = len(reduce_scratch(count, [ref.shape for ref in self.reduce[1]]))
            self.running.append(
                Reduce(self.reduce[0], count, args[:size], outs[:size], scratch[:used])
            )
            args, outs, scratch = args[size:], outs[size:], scratch[used:]
        if self.gather:
            size = len(self.gather[1])
            blocks = scratch[:size]
            self.loads = [
                pltpu.make_async_copy(args[a], blocks[a], scratch[size].at[a]) for a in range(size)
            ]
            self.running.append(
                Gather(self.gather[0], count, blocks, outs, scratch[size + 1 : size + 6])
            )
        for load in self.loads:
            load.start()

    def peers(self):
        return self.running[0].peers() if self.running else []

    def start(self):
        for load in self.loads:
            load.wait()
        for task in self.running:
            task.start()

    def advance(self):
        for task in self.running:
            task.advance()

    def finish(self):
        for task in self.running:
            task.finish()


def pick_split(columns):
    heads = columns // HEAD
    col = lax.broadcasted_iota(jnp.int32, (columns, heads * LANES), 1)
    row = lax.broadcasted_iota(jnp.int32, (columns, heads * LANES), 0)
    inner = col & 63
    source = (col >> 7) * HEAD + ((col >> 6) & 1) * HALF + inner
    return ((row == source) & (inner < HALF)).astype(F32).astype(BF16)


def pick_plain(columns):
    heads = columns // HEAD
    col = lax.broadcasted_iota(jnp.int32, (columns, heads * LANES), 1)
    row = lax.broadcasted_iota(jnp.int32, (columns, heads * LANES), 0)
    inner = col & 127
    return ((row == (col >> 7) * HEAD + inner) & (inner < HEAD)).astype(F32).astype(BF16)


def rotated(values, cosine, sine):
    return values * cosine + pltpu.roll(values, LANES // 2, 1) * sine


def spread_qkv(wq, wk, wv, wqkv):
    q_wide = wq.shape[1] // HEAD * LANES
    k_wide = wk.shape[1] // HEAD * LANES
    wqkv[:, :q_wide] = dot_nn(wq[...], pick_split(wq.shape[1])).astype(BF16)
    wqkv[:, q_wide : q_wide + k_wide] = dot_nn(wk[...], pick_split(wk.shape[1])).astype(BF16)
    wqkv[:, q_wide + k_wide :] = dot_nn(wv[...], pick_plain(wv.shape[1])).astype(BF16)


def allowed_pairs(seg_col, seg_row):
    full_rows = seg_col.shape[0]
    row = lax.broadcasted_iota(jnp.int32, (full_rows, full_rows), 0)
    col = lax.broadcasted_iota(jnp.int32, (full_rows, full_rows), 1)
    return (seg_col[...] == seg_row[...]) & (col <= row)


def lane_block(index):
    return pl.ds(pl.multiple_of(index * LANES, LANES), LANES)


def head_rows(ref, index):
    return ref[:, :, lane_block(index)].reshape(-1, LANES)


def attn_weights(weights, wo, sources):
    wq0, wq1, wk0, wk1, wv0, wv1, wo0, wo1 = sources[:8]
    wq, wk, wv = sources[8:]
    weights.want(wq0.at[0], wq1.at[0], wq)
    weights.want(wk0.at[0], wk1.at[0], wk)
    weights.want(wv0.at[0], wv1.at[0], wv)
    for h in range(wo.shape[0]):
        rows = pl.ds(h * HEAD, HEAD)
        weights.want(wo0.at[0, rows], wo1.at[0, rows], wo.at[h, pl.ds(0, HEAD)])


def clear_pads(wo):
    for h in range(wo.shape[0]):
        wo[h, HEAD:] = jnp.zeros((LANES - HEAD, wo.shape[2]), BF16)


def probabilities(queries, keys, allowed):
    scores = jnp.where(allowed, dot_nt(queries, keys) * HEAD ** (-0.5), neg_fill)
    exp_scores = jnp.exp(scores - jnp.max(scores, axis=-1, keepdims=True))
    return exp_scores / jnp.sum(exp_scores, axis=-1, keepdims=True)


def attn_fwd_kernel(layer, n, heads, kv_heads, others, loads_done, *refs):
    ahead = layer == 1
    x, gain, cos, sin, seg_col, seg_row = refs[:6]
    at = 6
    if ahead:
        rows_ahead = refs[at]
        at += 1
    own = refs[at : at + others]
    at += others
    if layer == 0:
        h_out, h_save, n_out, qkv_out, o_out = refs[at : at + 5]
        other = refs[at + 5 : at + 5 + others]
    else:
        other = refs[at : at + others]
        h_out, h_save, n_out, qkv_out, o_out, ahead_out = refs[at + others : at + others + 6]
        at += 1
    at += 5 + others
    (wq, wk, wv, wo, wqkv, qkv, o, osmall, wsem) = refs[at : at + 9]
    pair = Pair(*refs[at + 9 : at + 12])
    at += 12
    if ahead:
        second = Line(n, refs[at], None, None, *refs[at + 1 : at + 3], None, None)
        at += 3
    line = Line(n, *refs[at:])
    me = line.me
    group = heads // kv_heads
    weights = Weights(layer, wsem)
    sources = [ref for both in zip(own[:4], other[:4]) for ref in both] + [wq, wk, wv]
    attn_weights(weights, wo, sources)
    if layer == 0:
        weights.start_own()
    else:
        weights.start()
    loads_done()
    resid = x[...].astype(F32)
    line.full[me] = (resid * rms_scale(resid) * gain[...]).astype(BF16)
    clear_pads(wo)
    if ahead:
        second.full[me] = rows_ahead[...]
    if layer == 0:
        line.enter()
        line.gather_step(0)
        for mine, theirs in zip(own, other):
            pair.send(mine, theirs)

        def arrived():
            for index in range(4):
                pair.copy(own[index], other[index], index).wait_recv()

        weights.start_other(arrived)
    else:
        line.enter()
        line.gather_step(0)
    weights.wait()
    spread_qkv(wq, wk, wv, wqkv)

    def compute(shard):
        products = dot_nn(line.full[shard], wqkv[...])
        for head in range(heads + kv_heads):
            lanes = slice(head * LANES, (head + 1) * LANES)
            qkv[shard, :, lanes] = rotated(products[:, lanes], cos[shard], sin[shard]).astype(BF16)
        lanes = slice((heads + kv_heads) * LANES, None)
        qkv[shard, :, lanes] = products[:, lanes].astype(BF16)
        pair.stream(shard)

    pair.stream_share(line.full, n_out)
    pair.stream_keep(qkv, qkv_out)
    later_shards(line, compute)
    if ahead:
        second.gather_step(0)
    allowed = allowed_pairs(seg_col, seg_row)

    @pl.loop(0, kv_heads)
    def _(g):
        keys = head_rows(qkv, heads + g)
        values = head_rows(qkv, heads + kv_heads + g)
        rows = []
        for member in range(group):
            h = g * group + member
            probs = probabilities(head_rows(qkv, h), keys, allowed)
            attended = dot_nn(probs.astype(BF16), values).astype(BF16)
            o[:, :, lane_block(h)] = attended.reshape(n, -1, LANES)
            rows.append(attended)
        small = dot_nt(jnp.concatenate(rows, axis=1), pick_plain(group * HEAD))
        osmall[g] = small.astype(BF16).reshape(osmall.shape[1:])

    pair.share_half(osmall, o_out)
    wide = wo.shape[0] * LANES

    def partial(shard):
        return dot_nn(o[shard], wo[...].reshape(wide, -1))

    if ahead:
        sums_after(line, partial, lambda step: second.gather_step(step + 1))
        pair.keep(second.full, ahead_out.at[0])
        pair.send(second.full, ahead_out.at[1])
    else:
        sums_after(line, partial)
    h_out[...] = resid + partial(me)
    line.sum_take(h_out)
    pair.keep(h_out, h_save)
    if ahead:
        second.gather_end()
    line.gather_end()
    line.sum_end()
    if layer == 0:
        for index, copy in enumerate(pair.sent[:others]):
            copy.wait_send()
            if index >= 4:
                copy.wait_recv()

        @pl.when(weights.own)
        def _():
            for index in range(4):
                pair.copy(own[index], other[index], index).wait_recv()

        pair.sent[:others] = [None] * others
    pair.wait(n)


def bound(tasks, sizes, refs):
    groups, at = [], 0
    for own, extra in sizes:
        groups.append((refs[at : at + own], refs[at + own : at + own + extra]))
        at += own + extra
    tasks.bind(*(list(extra) for _, extra in groups))
    return [ref for own, _ in groups for ref in own]


def attn_bwd_kernel(layer, n, heads, kv_heads, tasks, sizes, loads_done, *refs):
    refs = bound(tasks, sizes, refs)
    (dh, x, gain, cos, sin, seg_col, seg_row, qkv_in) = refs[:8]
    own, other = refs[8:12], refs[12:16]
    (dx_out, dx_save, gain_out, da_out, dqkv_out) = refs[16:21]
    (wq, wk, wv, wo, wqkv, qkv, d_o, dqkv, dsmall, total, wsem, tsem) = refs[21:33]
    pair = Pair(*refs[33:36])
    line = Line(n, *refs[36:])
    me = line.me
    group = heads // kv_heads
    weights = Weights(layer, wsem)
    sources = [ref for both in zip(own, other) for ref in both] + [wq, wk, wv]
    attn_weights(weights, wo, sources)
    weights.start()
    take = pltpu.make_async_copy(qkv_in, qkv, tsem)
    take.start()
    line.full[me] = dh[...].astype(BF16)
    clear_pads(wo)
    line.enter(tasks.peers())
    line.gather_step(0)
    tasks.start()
    loads_done()
    weights.wait()
    spread_qkv(wq, wk, wv, wqkv)
    take.wait()
    wide = wo.shape[0] * LANES

    def compute(shard):
        d_o[shard] = dot_nt(line.full[shard], wo[...].reshape(wide, -1)).astype(BF16)
        pair.stream(shard)

    pair.stream_share(line.full, da_out)
    later_shards(line, compute)
    allowed = allowed_pairs(seg_col, seg_row)
    cosine = cos[...].reshape(-1, LANES)
    sine = -sin[...].reshape(-1, LANES)
    scale = HEAD ** (-0.5)

    @pl.loop(0, kv_heads)
    def _(g):
        keys = head_rows(qkv, heads + g)
        values = head_rows(qkv, heads + kv_heads + g)
        d_keys = d_values = None
        turned = []
        for member in range(group):
            h = g * group + member
            queries = head_rows(qkv, h)
            d_out = head_rows(d_o, h)
            probs = probabilities(queries, keys, allowed)
            d_probs = dot_nt(d_out, values)
            inner = jnp.sum(probs * d_probs, axis=-1, keepdims=True)
            d_scores = (probs * (d_probs - inner)).astype(BF16)
            d_queries = dot_nn(d_scores, keys) * scale
            turned.append(rotated(d_queries, cosine, sine).astype(BF16))
            dqkv[:, :, lane_block(h)] = turned[-1].reshape(n, -1, LANES)
            dk = dot_tn(d_scores, queries)
            dv = dot_tn(probs.astype(BF16), d_out)
            d_keys = dk if d_keys is None else d_keys + dk
            d_values = dv if d_values is None else d_values + dv
        turned.append(rotated(d_keys * scale, cosine, sine).astype(BF16))
        dqkv[:, :, lane_block(heads + g)] = turned[-1].reshape(n, -1, LANES)
        low_values = d_values.astype(BF16)
        dqkv[:, :, lane_block(heads + kv_heads + g)] = low_values.reshape(n, -1, LANES)
        small = dot_nt(jnp.concatenate(turned, axis=1), pick_split((group + 1) * HEAD))
        small_values = dot_nt(low_values, pick_plain(HEAD))
        dsmall[g] = (
            jnp.concatenate([small, small_values], axis=1).astype(BF16).reshape(dsmall.shape[1:])
        )

    pair.share_half(dsmall, dqkv_out)

    def partial(shard):
        return dot_nt(dqkv[shard], wqkv[...])

    sums_after(line, partial, lambda step: pl.when(step == 0)(tasks.advance))
    total[...] = partial(me)
    line.sum_take(total)
    d_resid, gain_part = norm_back(total[...], x[...].astype(F32), gain[...])
    dx_out[...] = (dh[...] + d_resid).astype(BF16)
    gain_out[...] = gain_part
    pair.keep(dx_out, dx_save)
    line.gather_end()
    line.sum_end()
    pair.wait(n)
    tasks.finish()


def ffn_fwd_kernel(layer, n, loads_done, *refs):
    (h, gain, wg0, wg1, wu0, wu1, wd0, wd1) = refs[:8]
    (y_out, y_save, n_out, gate_out, up_out, hid_out) = refs[8:14]
    (wg, wu, wd, gate, up, hid, part, wsem) = refs[14:22]
    pair = Pair(*refs[22:25])
    line = Line(n, *refs[25:])
    me = line.me
    weights = Weights(layer, wsem)
    weights.want(wg0.at[0], wg1.at[0], wg)
    weights.want(wu0.at[0], wu1.at[0], wu)
    weights.want(wd0.at[0], wd1.at[0], wd)
    weights.start()
    loads_done()
    resid = h[...]
    line.full[me] = (resid * rms_scale(resid) * gain[...]).astype(BF16)
    line.enter()
    line.gather_step(0)
    weights.wait()
    middle = hid.shape[3]

    def compute(shard):
        rows = line.full[shard]
        g = dot_nn(rows, wg[...])
        u = dot_nn(rows, wu[...])
        gate[shard] = g
        up[shard] = u
        low = (g * jax.nn.sigmoid(g) * u).astype(BF16)
        hid[0, shard] = low[:, :middle]
        hid[1, shard] = low[:, middle:]
        pair.stream(shard)
        part[shard] = dot_nn(low, wd[...])

    pair.stream_share(line.full, n_out)
    pair.stream_share_half(hid, hid_out)
    pair.stream_keep(gate, gate_out)
    pair.stream_keep(up, up_out)
    rows_then_sums(line, compute, lambda shard: part[shard])
    part[me] += h[...]
    line.sum_take(part.at[me])
    y_out[...] = part[me].astype(BF16)
    pair.keep(y_out, y_save)
    line.gather_end()
    line.sum_end()
    pair.wait(n)


def ffn_bwd_kernel(layer, n, tasks, sizes, loads_done, *refs):
    refs = bound(tasks, sizes, refs)
    gathered = layer == 1
    (dy, h, gain, gate_in, up_in, wg0, wg1, wu0, wu1, wd0, wd1) = refs[:11]
    if gathered:
        (df_all, dh_out, gain_out, dmid_out) = refs[11:15]
    else:
        (dh_out, gain_out, df_all, dmid_out) = refs[11:15]
    (wg, wu, wd, gate, up, dmid, part, wsem, tsem) = refs[15:24]
    pair = Pair(*refs[24:27])
    line = Line(n, *refs[27:])
    me = line.me
    weights = Weights(layer, wsem)
    weights.want(wd0.at[0], wd1.at[0], wd)
    weights.want(wg0.at[0], wg1.at[0], wg)
    weights.want(wu0.at[0], wu1.at[0], wu)
    weights.start()
    takes = [
        pltpu.make_async_copy(gate_in, gate, tsem.at[0]),
        pltpu.make_async_copy(up_in, up, tsem.at[1]),
    ]
    if gathered:
        takes.append(pltpu.make_async_copy(df_all.at[0], line.full, tsem.at[2]))
    for take in takes:
        take.start()
    loads_done()
    if gathered:
        line.enter(tasks.peers())
    else:
        line.full[me] = dy[...]
        line.enter(tasks.peers())
        line.gather_step(0)
    tasks.start()
    weights.wait()
    for take in takes:
        take.wait()
    middle = dmid.shape[3] // 2

    def compute(shard):
        d_hidden = dot_nt(line.full[shard], wd[...])
        g = gate[shard]
        sig = jax.nn.sigmoid(g)
        d_g = (d_hidden * up[shard] * sig * (1.0 + g * (1.0 - sig))).astype(BF16)
        d_u = (d_hidden * g * sig).astype(BF16)
        for core in range(2):
            lanes = slice(core * middle, (core + 1) * middle)
            dmid[core, shard, :, :middle] = d_g[:, lanes]
            dmid[core, shard, :, middle:] = d_u[:, lanes]
        pair.stream(shard)
        part[shard] = dot_nt(d_g, wg[...]) + dot_nt(d_u, wu[...])

    pair.stream_share_half(dmid, dmid_out)
    if gathered:
        sums_alone(line, compute, lambda shard: part[shard], tasks.advance)
    else:
        pair.stream_share(line.full, df_all)
        rows_then_sums(line, compute, lambda shard: part[shard], tasks.advance)
    line.sum_take(part.at[me])
    d_resid, gain_part = norm_back(part[me], h[...], gain[...])
    dh_out[...] = dy[...].astype(F32) + d_resid
    gain_out[...] = gain_part
    if not gathered:
        line.gather_end()
    line.sum_end()
    pair.wait(n)
    tasks.finish()


def run_kernel(body, args, in_specs, outs, scratch, cid, flops, nbytes, name, aliases=None):
    loaded = [index for index, spec in enumerate(in_specs) if spec in (LOAD, LOAD_MINE)]
    buffers = [
        VMEM(args[index].shape[1:] if in_specs[index] == LOAD_MINE else args[index].shape, args[index].dtype)
        for index in loaded
    ]
    inputs, results, own = len(args), len(outs), len(scratch)

    def kernel(*refs):
        places = list(refs[: inputs + results + own])
        extra = refs[inputs + results + own :]
        copies = []
        for number, index in enumerate(loaded):
            source = refs[index]
            if in_specs[index] == LOAD_MINE:
                source = source.at[lax.axis_index("section")]
            copies.append(pltpu.make_async_copy(source, extra[number], extra[-1].at[number]))
            places[index] = extra[number]
        for copy in copies:
            copy.start()

        def loads_done():
            for copy in copies:
                copy.wait()

        body(loads_done, *places)

    return pl.pallas_call(
        kernel,
        name=name,
        in_specs=[HBM_SPEC if spec in (LOAD, LOAD_MINE) else spec for spec in in_specs],
        out_shape=[jax.ShapeDtypeStruct(shape, dtype) for shape, dtype, _ in outs],
        out_specs=[spec for _, _, spec in outs],
        scratch_shapes=[*scratch, *buffers, DMA((max(len(loaded), 1),))],
        input_output_aliases=aliases or {},
        cost_estimate=pl.CostEstimate(flops=flops, bytes_accessed=nbytes, transcendentals=0),
        compiler_params=pltpu.CompilerParams(
            collective_id=cid, has_side_effects=True, vmem_limit_bytes=44 << 20
        ),
    )(*args)


def attn_forward(layer, n, x, gain, tables, own, other, rows_ahead):
    rows, width = x.shape[-2:]
    heads = own[0].shape[2] // HEAD
    kv_heads = own[1].shape[2] // HEAD
    wide = (heads + 2 * kv_heads) * LANES
    small = heads // kv_heads * HEAD
    args = [x, gain, *tables]
    specs = [LOAD_MINE if x.ndim == 3 else VMEM_SPEC] + [LOAD] * 5
    if layer == 1:
        args.append(rows_ahead)
        specs.append(LOAD_MINE)
    args += own
    specs += [HBM_SPEC] * len(own)
    outs = [
        ((rows, width), F32, VMEM_SPEC),
        ((rows, width), F32, HBM_SPEC),
        ((2, n, rows, width), BF16, HBM_SPEC),
        ((n, rows, wide), BF16, HBM_SPEC),
        ((2, n, rows, small), BF16, HBM_SPEC),
    ]
    if other is None:
        outs += [(weight.shape, weight.dtype, HBM_SPEC) for weight in own]
    else:
        args += [*other]
        specs += [HBM_SPEC] * len(other)
        outs.append(((2, n, rows, width), BF16, HBM_SPEC))
    scratch = (
        [
            VMEM((width, heads * HEAD), BF16),
            VMEM((width, kv_heads * HEAD), BF16),
            VMEM((width, kv_heads * HEAD), BF16),
            VMEM((heads, LANES, width), BF16),
            VMEM((width, wide), BF16),
            VMEM((n, rows, wide), BF16),
            VMEM((n, rows, heads * LANES), BF16),
            VMEM((kv_heads, n, rows, small), BF16),
            DMA((3 + heads,)),
        ]
        + pair_scratch(n, 5, 3 + (len(own) if other is None else 0))
        + ([VMEM((n, rows, width), BF16)] + [DMA((2, n, CHUNKS))] * 2 if layer == 1 else [])
        + line_scratch(n, rows, width)
    )
    body = functools.partial(attn_fwd_kernel, layer, n, heads, kv_heads, len(own))
    flops = 2 * n * rows * width * wide * 3 // 2
    return run_kernel(body, args, specs, outs, scratch, 1 + layer, flops, 8 << 20, f"attn_fwd{layer}")


def attn_backward(layer, n, dh, x, gain, tables, qkv, own, other, tasks):
    rows, width = dh.shape
    heads = own[0].shape[2] // HEAD
    kv_heads = own[1].shape[2] // HEAD
    wide = (heads + 2 * kv_heads) * LANES
    small = (heads // kv_heads + 2) * HEAD
    args = [dh, x, gain, *tables, qkv, *own, *other]
    specs = [VMEM_SPEC, LOAD_MINE if x.ndim == 3 else LOAD] + [LOAD] * 5 + [HBM_SPEC] * 9
    outs = [
        ((rows, width), BF16, VMEM_SPEC),
        ((rows, width), BF16, HBM_SPEC),
        ((1, width), F32, VMEM_SPEC),
        ((2, n, rows, width), BF16, HBM_SPEC),
        ((2, n, rows, small), BF16, HBM_SPEC),
    ]
    scratch = (
        [
            VMEM((width, heads * HEAD), BF16),
            VMEM((width, kv_heads * HEAD), BF16),
            VMEM((width, kv_heads * HEAD), BF16),
            VMEM((heads, LANES, width), BF16),
            VMEM((width, wide), BF16),
            VMEM((n, rows, wide), BF16),
            VMEM((n, rows, heads * LANES), BF16),
            VMEM((n, rows, wide), BF16),
            VMEM((kv_heads, n, rows, small), BF16),
            VMEM((rows, width), F32),
            DMA((3 + heads,)),
            DMA,
        ]
        + pair_scratch(n, 3, 2)
        + line_scratch(n, rows, width)
    )
    body = functools.partial(attn_bwd_kernel, layer, n, heads, kv_heads)
    flops = 2 * n * rows * width * wide * 2
    return run_with_tasks(
        body, tasks, args, specs, outs, scratch, 3 + layer, flops, 8 << 20, f"attn_bwd{layer}"
    )


def ffn_forward(layer, n, h, gain, own, other):
    rows, width = h.shape
    hidden = own[0].shape[2]
    args = [h, gain]
    for mine, theirs in zip(own, other):
        args += [mine, theirs]
    specs = [VMEM_SPEC, LOAD] + [HBM_SPEC] * 6
    outs = [
        ((rows, width), BF16, VMEM_SPEC),
        ((rows, width), BF16, HBM_SPEC),
        ((2, n, rows, width), BF16, HBM_SPEC),
        ((n, rows, hidden), F32, HBM_SPEC),
        ((n, rows, hidden), F32, HBM_SPEC),
        ((2, n, rows, hidden // 2), BF16, HBM_SPEC),
    ]
    scratch = (
        [
            VMEM((width, hidden), BF16),
            VMEM((width, hidden), BF16),
            VMEM((hidden, width), BF16),
            VMEM((n, rows, hidden), F32),
            VMEM((n, rows, hidden), F32),
            VMEM((2, n, rows, hidden // 2), BF16),
            VMEM((n, rows, width), F32),
            DMA((3,)),
        ]
        + pair_scratch(n, 5, 2)
        + line_scratch(n, rows, width)
    )
    body = functools.partial(ffn_fwd_kernel, layer, n)
    flops = 6 * n * rows * width * hidden
    return run_kernel(body, args, specs, outs, scratch, 5 + layer, flops, 16 << 20, f"ffn_fwd{layer}")


def ffn_backward(layer, n, dy, h, gain, gate, up, own, other, tasks, df_all):
    rows, width = h.shape
    hidden = own[0].shape[2]
    args = [dy, h, gain, gate, up]
    for mine, theirs in zip(own, other):
        args += [mine, theirs]
    specs = [LOAD_MINE if dy.ndim == 3 else VMEM_SPEC, LOAD, LOAD] + [HBM_SPEC] * 8
    outs = [
        ((rows, width), F32, VMEM_SPEC),
        ((1, width), F32, VMEM_SPEC),
        ((2, n, rows, hidden), BF16, HBM_SPEC),
    ]
    if layer == 1:
        args.append(df_all)
        specs.append(HBM_SPEC)
    else:
        outs.insert(2, ((2, n, rows, width), BF16, HBM_SPEC))
    scratch = (
        [
            VMEM((width, hidden), BF16),
            VMEM((width, hidden), BF16),
            VMEM((hidden, width), BF16),
            VMEM((n, rows, hidden), F32),
            VMEM((n, rows, hidden), F32),
            VMEM((2, n, rows, hidden), BF16),
            VMEM((n, rows, width), F32),
            DMA((3,)),
            DMA((3,)),
        ]
        + pair_scratch(n, 2, 2)
        + line_scratch(n, rows, width)
    )
    body = functools.partial(ffn_bwd_kernel, layer, n)
    flops = 6 * n * rows * width * hidden
    return run_with_tasks(
        body, tasks, args, specs, outs, scratch, 7 + layer, flops, 16 << 20, f"ffn_bwd{layer}"
    )


def run_with_tasks(body, tasks, args, specs, outs, scratch, cid, flops, nbytes, name):
    more_args, more_outs, more_scratch = tasks.arguments(), tasks.outputs(), tasks.scratch()
    sizes = (
        (len(args), len(more_args)),
        (len(outs), len(more_outs)),
        (len(scratch), len(more_scratch)),
    )
    return run_kernel(
        functools.partial(body, tasks, sizes),
        args + more_args,
        specs + [HBM_SPEC] * len(more_args),
        outs + more_outs,
        scratch + more_scratch,
        cid,
        flops,
        nbytes,
        name,
    )


def tail_kernel(n, count, sizes, loads_done, *refs):
    ffn_size, attn_size = sizes
    at = 0

    def take(number):
        nonlocal at
        at += number
        return list(refs[at - number : at])

    gains = take(4)
    rows = take(4)
    ffn_blocks, attn_arrays, _aliased = take(ffn_size), take(attn_size), take(ffn_size + attn_size)
    (gains_out, section_out, in_grad) = take(3)
    ffn_outs, attn_outs = take(ffn_size), take(attn_size)
    by_tensor, by_dp, by_core = take(3)
    small_sems = take(2)
    ffn_vmem, attn_vmem = take(ffn_size), take(attn_size)
    (load_sem,) = take(1)
    ffn_sems, attn_sems, row_sems = take(5), take(5), take(3)
    reduce = Reduce(0, count, attn_arrays, attn_vmem, take(len(refs) - at))
    gather_ffn = Gather(0, count, ffn_vmem, ffn_outs, ffn_sems)
    gather_attn = Gather(0, count, attn_vmem, attn_outs, attn_sems)
    loads = [
        pltpu.make_async_copy(ffn_blocks[a], ffn_vmem[a], load_sem.at[a]) for a in range(ffn_size)
    ]
    for load in loads:
        load.start()
    axes = (("tensor", n, by_tensor), ("dp", count, by_dp), ("section", 2, by_core))
    barrier = pltpu.get_barrier_semaphore()
    peers = 0
    for axis, size, _ in axes:
        place = lax.axis_index(axis)
        for shift in range(1, size):
            pl.semaphore_signal(
                barrier, 1, device_id={axis: (place + shift) % size}, device_id_type=MESH
            )
            peers += 1
    pl.semaphore_wait(barrier, peers)

    def small(stage, shift):
        axis, size, slots = axes[stage]
        place = lax.axis_index(axis)
        ref = slots.at[place]
        return pltpu.make_async_remote_copy(
            ref,
            ref,
            small_sems[0].at[stage, shift],
            small_sems[1].at[stage, shift],
            device_id={axis: (place + shift) % size},
            device_id_type=MESH,
        )

    def small_start(stage, value):
        axis, size, slots = axes[stage]
        slots[lax.axis_index(axis)] = value
        for shift in range(1, size):
            small(stage, shift).start()

    def small_end(stage):
        _, size, slots = axes[stage]
        for shift in range(1, size):
            small(stage, shift).wait()
        value = slots[0]
        for index in range(1, size):
            value = value + slots[index]
        return value

    loads_done()
    small_start(0, jnp.concatenate([gain[...] for gain in gains], axis=0))
    for load in loads:
        load.wait()
    gather_ffn.start()
    reduce.start()
    core = lax.axis_index("section")

    def row_target(index):
        return (section_out, in_grad)[index // 2].at[core]

    def row_keep(index):
        return pltpu.make_async_copy(rows[index], row_target(index), row_sems[0].at[index])

    def row_send(index):
        return pltpu.make_async_remote_copy(
            rows[index],
            row_target(index),
            row_sems[1].at[index],
            row_sems[2].at[index],
            device_id={"section": 1 - core},
            device_id_type=MESH,
        )

    for index in range(4):

        @pl.when(core == index % 2)
        def _():
            row_keep(index).start()

        @pl.when(core != index % 2)
        def _():
            row_send(index).start()

    small_start(1, small_end(0))
    reduce.advance()
    small_start(2, small_end(1))
    gather_ffn.advance()
    reduce.finish()
    gather_attn.start()
    gains_out[...] = small_end(2)
    gather_attn.advance()
    gather_ffn.finish()
    gather_attn.finish()
    for index in range(4):

        @pl.when(core == index % 2)
        def _():
            row_keep(index).wait()
            row_send(index).wait_recv()

        @pl.when(core != index % 2)
        def _():
            row_send(index).wait_send()


def tail(n, count, gains, rows, ffn_blocks, attn_arrays, ffn_full, attn_full):
    sizes = (len(ffn_blocks), len(attn_arrays))
    args = [*gains, *rows, *ffn_blocks, *attn_arrays, *ffn_full, *attn_full]
    specs = [LOAD] * 8 + [HBM_SPEC] * (len(args) - 8)
    together = (4, gains[0].shape[1])
    outs = [(together, F32, VMEM_SPEC)]
    outs += [((2,) + rows[0].shape, BF16, HBM_SPEC)] * 2
    outs += [(full.shape, BF16, HBM_SPEC) for full in (*ffn_full, *attn_full)]
    scratch = [VMEM((size,) + together, F32) for size in (n, count, 2)]
    scratch += [DMA((3, max(n, count, 2)))] * 2
    scratch += [VMEM(block.shape, BF16) for block in ffn_blocks]
    scratch += [VMEM((2,) + array.shape[-2:], BF16) for array in attn_arrays]
    scratch += [DMA((sizes[0],))]
    scratch += gather_sems(count, sizes[0]) + gather_sems(count, sizes[1]) + [DMA((4,))] * 3
    scratch += reduce_scratch(count, [array.shape for array in attn_arrays])
    first = 8 + sizes[0] + sizes[1]
    aliases = {first + index: 3 + index for index in range(sum(sizes))}
    body = functools.partial(tail_kernel, n, count, sizes)
    return run_kernel(body, args, specs, outs, scratch, 9, 1 << 20, 16 << 20, "tail", aliases)


def swap(values):
    return lax.ppermute(values, "section", [(0, 1), (1, 0)])


def segment_tables(lengths_row, n, rows):
    full_rows = n * rows
    slot_count = lengths_row.shape[0]
    seq_ends = jnp.cumsum(lengths_row)
    row_index = jnp.arange(full_rows, dtype=jnp.int32)
    segment = jnp.sum((row_index[:, None] >= seq_ends[None, :]).astype(jnp.int32), axis=1)
    starts = jnp.concatenate([seq_ends - lengths_row, seq_ends[-1:]])
    chosen = segment[:, None] == jnp.arange(slot_count + 1, dtype=jnp.int32)[None, :]
    position = row_index - jnp.sum(jnp.where(chosen, starts[None, :], 0), axis=1)
    segment = jnp.where(segment < slot_count, segment, slot_count + row_index)
    lane = jnp.arange(LANES, dtype=jnp.int32)
    inner = lane % (LANES // 2)
    inverse = rope_base ** (-inner.astype(F32) * 2.0 / HEAD)
    angle = position.astype(F32)[:, None] * inverse[None, :]
    live = (inner < HALF)[None, :]
    sign = jnp.where(lane < LANES // 2, -1.0, 1.0)[None, :]
    cosine = jnp.where(live, jnp.cos(angle), 0.0)
    sine = jnp.where(live, sign * jnp.sin(angle), 0.0)
    shape = (n, rows, LANES)
    return cosine.reshape(shape), sine.reshape(shape), segment[:, None], segment[None, :]


def shards(
    inputs,
    cotangent,
    seq_lengths,
    gain_attn,
    w_query,
    w_key,
    w_value,
    w_out,
    gain_ffn,
    w_gate,
    w_up,
    w_down,
):
    section = lax.axis_index("section")
    first = section == 0
    n = lax.axis_size("tensor")
    rows = inputs.shape[1]
    attn_own = (w_query, w_key, w_value, w_out)
    ffn_own = (w_gate, w_up, w_down)
    gains = jnp.concatenate([gain_attn, gain_ffn], axis=0)
    gains_other = swap(gains)
    gains_by_layer = [
        jnp.where(first, gains, gains_other).astype(F32),
        jnp.where(first, gains_other, gains).astype(F32),
    ]
    tables = segment_tables(jnp.where(first, seq_lengths[0, 0], seq_lengths[0, 1]), n, rows)

    x = x_saved = inputs
    kept = []
    outs = []
    for layer in range(2):
        gain_a, gain_f = gains_by_layer[layer][0:1], gains_by_layer[layer][1:2]
        if layer == 0:
            h, h_saved, n_all, qkv, o, *swapped = attn_forward(
                layer, n, x, gain_a, tables, attn_own + ffn_own, None, None
            )
            attn_other, ffn_other = tuple(swapped[:4]), tuple(swapped[4:])
        else:
            h, h_saved, n_all, qkv, o, df_ahead = attn_forward(
                layer, n, x, gain_a, tables, attn_own, attn_other, cotangent
            )
        y, y_saved, n2_all, gate, up, hid = ffn_forward(layer, n, h, gain_f, ffn_own, ffn_other)
        kept.append((x_saved, h_saved, n_all, qkv, o, n2_all, gate, up, hid, gain_a, gain_f))
        outs.append(y_saved)
        x, x_saved = y, y_saved

    count = lax.axis_size("dp")
    cube = (2,) + (2,) * (count.bit_length() - 1)

    def weight_grad(left, right):
        left = left.reshape(-1, left.shape[-1])
        right = right.reshape(-1, right.shape[-1])
        return dot_tn(left, right).astype(BF16)

    def blocked(array):
        return array.reshape(*cube, -1, array.shape[-1])

    dy = cotangent
    in_grads = [None, None]
    gain_parts = [None, None]
    for layer in (1, 0):
        x, h, n_all, qkv, o, n2_all, gate, up, hid, gain_a, gain_f = kept[layer]
        if layer == 1:
            g_down = blocked(weight_grad(hid, df_ahead))
            plan = {"reduce": (1, [g_down])}
            dh, gf_part, dmid, sum_down = ffn_backward(
                layer, n, dy, h, gain_f, gate, up, ffn_own, ffn_other, Tasks(count, plan), df_ahead
            )
            g_mid = blocked(weight_grad(n2_all, dmid))
            plan = {"reduce": (1, [g_mid]), "gather": (1, [sum_down])}
        else:
            plan = {"reduce": (1, attn_grad), "gather": (1, [sum_mid])}
            dh, gf_part, df_all, dmid, *sum_attn, mid_full = ffn_backward(
                layer, n, dy, h, gain_f, gate, up, ffn_own, ffn_other, Tasks(count, plan), None
            )
            g_mid, g_down = blocked(weight_grad(n2_all, dmid)), blocked(weight_grad(hid, df_all))
            plan = {"reduce": (0, [g_mid, g_down]), "gather": (1, sum_attn)}
        dx, dx_saved, ga_part, da_all, dqkv, *more = attn_backward(
            layer, n, dh, x, gain_a, tables, qkv, attn_own, attn_other, Tasks(count, plan)
        )
        if layer == 1:
            sum_mid, down_full = more
        else:
            sum_ffn, attn_full = more[:2], more[2:]
        attn_grad = [blocked(weight_grad(dqkv, n_all)), blocked(weight_grad(o, da_all))]
        gain_parts[layer] = [ga_part, gf_part]
        in_grads[layer] = dx_saved
        dy = dx
    gain_sums, section_out, in_grad, g_mid, g_down, g_qkv, g_out = tail(
        n,
        count,
        gain_parts[0] + gain_parts[1],
        outs + in_grads,
        sum_ffn,
        attn_grad,
        [mid_full, down_full],
        attn_full,
    )
    gain_own = jnp.where(first, gain_sums[0:2], gain_sums[2:4])
    g_mid, g_qkv = (array.reshape(3, -1, array.shape[-1]) for array in (g_mid, g_qkv))
    g_down, g_out = (
        array[:2].astype(F32).reshape(1, -1, array.shape[-1]) for array in (g_down, g_out)
    )

    def columns(start, size):
        parts = [g_mid[core, :, start : start + size].astype(F32) for core in range(2)]
        return jnp.concatenate(parts, axis=1)[None]

    def turned(start, size):
        parts = [g_qkv[core, start : start + size].astype(F32) for core in range(2)]
        return jnp.concatenate(parts, axis=0).T[None]

    mid = w_gate.shape[2] // 2
    g_gate, g_up = columns(0, mid), columns(mid, mid)
    q_half, k_half = w_query.shape[2] // 2, w_key.shape[2] // 2
    g_query = turned(0, q_half)
    g_key, g_value = turned(q_half, k_half), turned(q_half + k_half, k_half)
    return (
        section_out[None],
        in_grad[None],
        gain_own[0:1],
        g_query,
        g_key,
        g_value,
        g_out,
        gain_own[1:2],
        g_gate,
        g_up,
        g_down,
    )


def solution(mesh):
    placed = (
        P(None, ("dp", "tensor"), None),
        P(None, ("dp", "tensor"), None),
        P("dp", None, None),
        P("section", None),
        P("section", None, "tensor"),
        P("section", None, "tensor"),
        P("section", None, "tensor"),
        P("section", "tensor", None),
        P("section", None),
        P("section", None, "tensor"),
        P("section", None, "tensor"),
        P("section", "tensor", None),
    )
    return jax.shard_map(
        shards,
        mesh=mesh,
        in_specs=placed,
        out_specs=(
            P("section", None, ("dp", "tensor"), None),
            P("section", None, ("dp", "tensor"), None),
            P("section", None),
            P("section", None, "tensor"),
            P("section", None, "tensor"),
            P("section", None, "tensor"),
            P("section", "tensor", None),
            P("section", None),
            P("section", None, "tensor"),
            P("section", None, "tensor"),
            P("section", "tensor", None),
        ),
        check_vma=False,
    )
```

```python
import functools

import jax
import jax.numpy as jnp
from jax import lax
from jax.experimental import pallas as pl
from jax.experimental.pallas import tpu as pltpu
from jax.sharding import PartitionSpec as P

HEAD = 96
HALF = HEAD // 2
LANES = 128
CHUNKS = 3
BF16 = jnp.bfloat16
F32 = jnp.float32
MESH = pl.DeviceIdType.MESH
VMEM = pltpu.VMEM
VMEM_SPEC = pl.BlockSpec(memory_space=pltpu.VMEM)
LOAD, LOAD_MINE = "load", "load mine"
VMEM_LIMITS = {"attn_fwd0": 61, "tail": 61}
HBM_SPEC = pl.BlockSpec(memory_space=pltpu.HBM)
DMA = pltpu.SemaphoreType.DMA

eps = 1e-05
rope_base = 100000.0
neg_fill = -1e30


def dot_nn(left, right):
    return lax.dot_general(left, right, (((1,), (0,)), ((), ())), preferred_element_type=F32)


def dot_nt(left, right):
    return lax.dot_general(left, right, (((1,), (1,)), ((), ())), preferred_element_type=F32)


def dot_tn(left, right):
    return lax.dot_general(left, right, (((0,), (0,)), ((), ())), preferred_element_type=F32)


def rms_scale(values):
    return lax.rsqrt(jnp.mean(values * values, axis=-1, keepdims=True) + eps)


def norm_back(d_normed, resid, gain):
    scale_rows = rms_scale(resid)
    unit_rows = resid * scale_rows
    gain_part = jnp.sum(d_normed * unit_rows, axis=0, keepdims=True)
    d_unit = d_normed * gain
    inner = jnp.mean(d_unit * unit_rows, axis=-1, keepdims=True)
    return scale_rows * (d_unit - unit_rows * inner), gain_part


class Line:
    def __init__(self, count, full, rbuf, sbuf, gs, gr, ss, sr):
        self.n = count
        self.core = lax.axis_index("section")
        self.me = lax.axis_index("tensor")
        self.full, self.rbuf, self.sbuf = full, rbuf, sbuf
        self.gs, self.gr, self.ss, self.sr = gs, gr, ss, sr
        self.rows = full.shape[1] // CHUNKS

    def span(self, c):
        return pl.ds(c * self.rows, self.rows)

    def neighbour(self, d):
        return self.me + 1 if d == 0 else self.me - 1

    def enter(self, also=()):
        me, n = self.me, self.n
        barrier = pltpu.get_barrier_semaphore()
        for peer in ({"section": 1 - self.core}, *also):
            pl.semaphore_signal(barrier, 1, device_id=peer, device_id_type=MESH)
        for d, there in ((1, me > 0), (0, me < n - 1)):

            @pl.when(there)
            def _():
                pl.semaphore_signal(
                    barrier, 1, device_id={"tensor": self.neighbour(d)}, device_id_type=MESH
                )

        peers = 1 + len(also) + (me > 0).astype(jnp.int32) + (me < n - 1).astype(jnp.int32)
        pl.semaphore_wait(barrier, peers)

    def gather_copy(self, d, step, shard, c):
        ref = self.full.at[shard, self.span(c)]
        return pltpu.make_async_remote_copy(
            ref,
            ref,
            self.gs.at[d, step, c],
            self.gr.at[d, step, c],
            device_id={"tensor": self.neighbour(d)},
            device_id_type=MESH,
        )

    def gather_step(self, step):
        me, n = self.me, self.n
        for c in range(CHUNKS):
            for d in range(2):
                shard = me - step if d == 0 else me + step
                holds = (shard >= 0) & (shard < n)
                onward = (me + 1 < n) if d == 0 else (me > 0)

                @pl.when(holds & (step > 0))
                def _():
                    self.gather_copy(d, step - 1, shard, c).wait_recv()

                @pl.when(holds & onward)
                def _():
                    self.gather_copy(d, step, shard, c).start()

    def gather_end(self):
        me, n = self.me, self.n

        @pl.loop(0, n - 1)
        def _(step):
            for c in range(CHUNKS):
                for d in range(2):
                    shard = me - step if d == 0 else me + step
                    onward = (me + 1 < n) if d == 0 else (me > 0)

                    @pl.when((shard >= 0) & (shard < n) & onward)
                    def _():
                        self.gather_copy(d, step, shard, c).wait_send()

    def sum_copy(self, d, shard, c):
        return pltpu.make_async_remote_copy(
            self.sbuf.at[shard, self.span(c)],
            self.rbuf.at[d, shard, self.span(c)],
            self.ss.at[d, shard, c],
            self.sr.at[d, shard, c],
            device_id={"tensor": self.neighbour(d)},
            device_id_type=MESH,
        )

    def sum_step(self, d, shard, partial):
        me, n = self.me, self.n
        goes = (shard > me) & (shard < n) if d == 0 else (shard >= 0) & (shard < me)
        first = (me == 0) if d == 0 else (me == n - 1)

        @pl.when(goes)
        def _():
            for c in range(CHUNKS):
                mine = partial[shard, self.span(c)]

                @pl.when(first)
                def _():
                    self.sbuf[shard, self.span(c)] = mine.astype(BF16)

                @pl.when(jnp.logical_not(first))
                def _():
                    self.sum_copy(d, shard, c).wait_recv()
                    arrived = self.rbuf[d, shard, self.span(c)].astype(F32)
                    self.sbuf[shard, self.span(c)] = (mine + arrived).astype(BF16)

                self.sum_copy(d, shard, c).start()

    def sum_take(self, total):
        me, n = self.me, self.n
        for d, there in ((0, me > 0), (1, me < n - 1)):

            @pl.when(there)
            def _():
                for c in range(CHUNKS):
                    self.sum_copy(d, me, c).wait_recv()
                    total[self.span(c)] += self.rbuf[d, me, self.span(c)].astype(F32)

    def sum_end(self):
        me, n = self.me, self.n

        @pl.loop(0, n)
        def _(shard):
            for d, goes in ((0, shard > me), (1, shard < me)):

                @pl.when(goes)
                def _():
                    for c in range(CHUNKS):
                        self.sum_copy(d, shard, c).wait_send()


def line_scratch(count, rows, width):
    return [
        VMEM((count, rows, width), BF16),
        VMEM((2, count, rows, width), BF16),
        VMEM((count, rows, width), BF16),
        DMA((2, count, CHUNKS)),
        DMA((2, count, CHUNKS)),
        DMA((2, count, CHUNKS)),
        DMA((2, count, CHUNKS)),
    ]


def rows_then_sums(line, compute, partial, halfway=lambda: None):
    me, n = line.me, line.n

    @pl.loop(0, 2 * n - 1)
    def _(step):
        @pl.when((step > 0) & (step < n))
        def _():
            line.gather_step(step)

        @pl.when(step == n - 1)
        def _():
            halfway()

        @pl.when(step < n)
        def _():
            @pl.loop(0, 2)
            def _(side):
                shard = jnp.where(side == 0, me - step, me + step)

                @pl.when((shard >= 0) & (shard < n) & ((step > 0) | (side == 0)))
                def _():
                    compute(shard)

        line.sum_step(0, step - me, partial)
        line.sum_step(1, 2 * (n - 1) - step - me, partial)


def later_shards(line, compute):
    me, n = line.me, line.n

    @pl.loop(0, n)
    def _(step):
        @pl.when(step > 0)
        def _():
            line.gather_step(step)

        @pl.loop(0, 2)
        def _(side):
            shard = jnp.where(side == 0, me - step, me + step)

            @pl.when((shard >= 0) & (shard < n) & ((step > 0) | (side == 0)))
            def _():
                compute(shard)


def sums_alone(line, compute, partial, each):
    me, n = line.me, line.n

    @pl.loop(0, n)
    def _(step):
        @pl.loop(0, 2)
        def _(side):
            shard = jnp.where(side == 0, me + n - 1 - step, step - (n - 1 - me))
            first = jnp.where(side == 0, me, 0)
            last = jnp.where(side == 0, n, me)

            @pl.when((shard >= first) & (shard < last))
            def _():
                compute(shard)

        line.sum_step(0, me + n - 1 - step, partial)
        line.sum_step(1, step - (n - 1 - me), partial)
        each(step)


class Weights:
    def __init__(self, layer, sems):
        self.own = lax.axis_index("section") == layer
        self.sems = sems
        self.wanted = []

    def want(self, mine, theirs, target):
        self.wanted.append((mine, theirs, target))

    def start_own(self):
        @pl.when(self.own)
        def _():
            for index, (mine, _theirs, target) in enumerate(self.wanted):
                pltpu.make_async_copy(mine, target, self.sems.at[index]).start()

    def start_other(self, before=lambda: None):
        @pl.when(jnp.logical_not(self.own))
        def _():
            before()
            for index, (_mine, theirs, target) in enumerate(self.wanted):
                pltpu.make_async_copy(theirs, target, self.sems.at[index]).start()

    def start(self):
        self.start_own()
        self.start_other()

    def wait(self):
        for index, (mine, _theirs, target) in enumerate(self.wanted):
            pltpu.make_async_copy(mine, target, self.sems.at[index]).wait()


class Pair:
    def __init__(self, local_sems, send_sems, recv_sems):
        self.core = lax.axis_index("section")
        self.sems = local_sems, send_sems, recv_sems
        self.kept, self.sent = [], []
        self.streams = []

    def keep(self, source, target):
        copy = pltpu.make_async_copy(source, target, self.sems[0].at[len(self.kept), 0])
        copy.start()
        self.kept.append(copy)

    def copy(self, source, target, index, part=0):
        return pltpu.make_async_remote_copy(
            source,
            target,
            self.sems[1].at[index, part],
            self.sems[2].at[index, part],
            device_id={"section": 1 - self.core},
            device_id_type=MESH,
        )

    def send(self, source, target):
        copy = self.copy(source, target, len(self.sent))
        copy.start()
        self.sent.append(copy)

    def share_half(self, halves, pair):
        self.keep(halves.at[self.core], pair.at[0])
        self.send(halves.at[1 - self.core], pair.at[1])

    def stream_keep(self, source, target):
        self.streams.append((source, target, len(self.kept), None))
        self.kept.append(None)

    def stream_share(self, source, pair):
        self.stream_keep(source, pair.at[0])
        self.streams.append((source, pair.at[1], None, len(self.sent)))
        self.sent.append(None)

    def stream_share_half(self, halves, pair):
        self.stream_keep(halves.at[self.core], pair.at[0])
        self.streams.append((halves.at[1 - self.core], pair.at[1], None, len(self.sent)))
        self.sent.append(None)

    def streamed(self, shard):
        copies = []
        for source, target, kept, sent in self.streams:
            pieces = source.at[shard], target.at[shard]
            if sent is None:
                copies.append(pltpu.make_async_copy(*pieces, self.sems[0].at[kept, shard]))
            else:
                copies.append(self.copy(*pieces, sent, shard))
        return copies

    def stream(self, shard):
        for copy in self.streamed(shard):
            copy.start()

    def wait(self, count=0):
        for copy in self.kept + self.sent:
            if copy is not None:
                copy.wait()
        if self.streams:

            @pl.loop(0, count)
            def _(shard):
                for copy in self.streamed(shard):
                    copy.wait()


def pair_scratch(count, kept, sent):
    return [DMA((max(kept, 1), count)), DMA((max(sent, 1), count)), DMA((max(sent, 1), count))]


class Cube:
    def __init__(self, layer, count):
        self.bits = count.bit_length() - 1
        assert count == 1 << self.bits
        self.me = lax.axis_index("dp")
        self.core = lax.axis_index("section")
        self.active = self.core == layer
        self.bit = [(self.me // (1 << b)) % 2 for b in range(self.bits)]
        self.down = list(range(self.bits - 1, -1, -1))

    def order(self, colour):
        return list(range(self.bits)) if colour == 0 else self.down

    def peer(self, b):
        return {"dp": self.me + (1 - 2 * self.bit[b]) * (1 << b)}

    def peers(self):
        return [self.peer(b) for b in range(self.bits)]


class Reduce(Cube):
    def __init__(self, layer, count, sources, outs, scratch):
        super().__init__(layer, count)
        self.sources, self.outs = sources, outs
        size = len(sources)
        self.accs = scratch[:size]
        self.recvs = [scratch[size * (t + 1) : size * (t + 2)] for t in range(self.bits)]
        self.local, self.ss, self.sr, self.fs = scratch[size * (self.bits + 1) :]
        self.t = 0
        self.place = [
            {b: slice(None) for b in self.down if b != self.order(c)[0]} for c in range(2)
        ]

    def items(self):
        return [(a, c) for a in range(len(self.sources)) for c in range(2)]

    def spot(self, c, changed=()):
        place = {**self.place[c], **dict(changed)}
        return (c, *(place[b] for b in self.down if b in place))

    def first_half(self, a, c, value):
        b = self.order(c)[0]
        index = [slice(None)] * self.bits
        index[self.down.index(b)] = value
        return self.sources[a].at[(c, *index)]

    def copy(self, a, c, t, source):
        return pltpu.make_async_remote_copy(
            source,
            self.recvs[t][a].at[c],
            self.ss.at[a, c, t],
            self.sr.at[a, c, t],
            device_id=self.peer(self.order(c)[t]),
            device_id_type=MESH,
        )

    def kept(self, a, c):
        mine = self.first_half(a, c, self.bit[self.order(c)[0]])
        return pltpu.make_async_copy(mine, self.accs[a].at[c], self.local.at[a, c])

    def start(self):
        for a, c in self.items():
            other = self.first_half(a, c, 1 - self.bit[self.order(c)[0]])
            self.copy(a, c, 0, other).start()
            self.kept(a, c).start()

    def advance(self):
        t = self.t
        if t >= self.bits:
            return
        for a, c in self.items():
            if t == 0:
                self.kept(a, c).wait()
            self.copy(a, c, t, self.recvs[t][a].at[c]).wait_recv()
            acc, spot = self.accs[a], self.spot(c)
            acc[spot] = (acc[spot].astype(F32) + self.recvs[t][a][c].astype(F32)).astype(BF16)
            if t + 1 < self.bits:
                b = self.order(c)[t + 1]
                self.copy(a, c, t + 1, acc.at[self.spot(c, [(b, 1 - self.bit[b])])]).start()
        if t + 1 < self.bits:
            for c in range(2):
                b = self.order(c)[t + 1]
                self.place[c][b] = self.bit[b]
        self.t = t + 1

    def put_away(self, a, c):
        return pltpu.make_async_copy(
            self.accs[a].at[self.spot(c)], self.outs[a].at[c], self.fs.at[a, c]
        )

    def finish(self):
        while self.t < self.bits:
            self.advance()
        for a, c in self.items():
            self.put_away(a, c).start()
        for a, c in self.items():
            for t in range(self.bits):
                self.copy(a, c, t, self.recvs[t][a].at[c]).wait_send()
        for a, c in self.items():
            self.put_away(a, c).wait()


class Gather(Cube):
    def __init__(self, layer, count, blocks, outs, sems):
        super().__init__(layer, count)
        self.blocks, self.outs = blocks, outs
        self.keep, self.ss, self.sr, self.hs, self.hr = sems
        self.t = 0
        off_layer = 1 - self.core if layer == 1 else self.core
        self.slot = self.core * (1 - off_layer) + 2 * off_layer

    def items(self):
        return [(a, c) for a in range(len(self.blocks)) for c in range(2)]

    def order(self, colour):
        return super().order(colour)[::-1]

    def region(self, a, c, t, half, flipped=None):
        order = self.order(c)
        index = []
        for b in self.down:
            if b in order[:t]:
                index.append(slice(None))
            else:
                index.append(1 - self.bit[b] if flipped == order.index(b) else self.bit[b])
        return self.outs[a].at[(half, c, *index)]

    def copy(self, a, c, t):
        target = self.region(a, c, t, self.slot)
        return pltpu.make_async_remote_copy(
            self.blocks[a].at[c] if t == 0 else target,
            target,
            self.ss.at[a, c, t],
            self.sr.at[a, c, t],
            device_id=self.peer(self.order(c)[t]),
            device_id_type=MESH,
        )

    def kept(self, a, c):
        return pltpu.make_async_copy(
            self.blocks[a].at[c], self.region(a, c, 0, self.slot), self.keep.at[a, c]
        )

    def hand_over(self, a, c, t):
        if t == 0:
            source, target = self.blocks[a].at[c], self.region(a, c, 0, self.core)
        else:
            source = self.region(a, c, t - 1, self.slot, t - 1)
            target = self.region(a, c, t - 1, self.core, t - 1)
        return pltpu.make_async_remote_copy(
            source,
            target,
            self.hs.at[a, c, t],
            self.hr.at[a, c, t],
            device_id={"section": 1 - self.core},
            device_id_type=MESH,
        )

    def pass_on(self, t):
        @pl.when(jnp.logical_not(self.active))
        def _():
            for a, c in self.items():
                self.hand_over(a, c, t).start()

    def start(self):
        for a, c in self.items():
            self.copy(a, c, 0).start()
            self.kept(a, c).start()
        self.pass_on(0)

    def advance(self):
        t = self.t
        if t >= self.bits:
            return
        for a, c in self.items():
            if t == 0:
                self.kept(a, c).wait()
            self.copy(a, c, t).wait_recv()
            if t + 1 < self.bits:
                self.copy(a, c, t + 1).start()
        self.pass_on(t + 1)
        self.t = t + 1

    def finish(self):
        while self.t < self.bits:
            self.advance()
        for a, c in self.items():
            for t in range(self.bits):
                self.copy(a, c, t).wait_send()

        @pl.when(self.active)
        def _():
            for a, c in self.items():
                for t in range(self.bits + 1):
                    self.hand_over(a, c, t).wait_recv()

        @pl.when(jnp.logical_not(self.active))
        def _():
            for a, c in self.items():
                for t in range(self.bits + 1):
                    self.hand_over(a, c, t).wait_send()


def reduce_scratch(count, arrays):
    bits = count.bit_length() - 1
    scratch = []
    for level in (1, *range(1, bits + 1)):
        scratch += [VMEM((2,) + (2,) * (bits - level) + shape[-2:], BF16) for shape in arrays]
    size = len(arrays)
    return scratch + [
        DMA((size, 2)),
        DMA((size, 2, bits)),
        DMA((size, 2, bits)),
        DMA((size, 2)),
    ]


def gather_sems(count, size):
    bits = count.bit_length() - 1
    return [
        DMA((size, 2)),
        DMA((size, 2, bits)),
        DMA((size, 2, bits)),
        DMA((size, 2, bits + 1)),
        DMA((size, 2, bits + 1)),
    ]


class Tasks:
    def __init__(self, count, plan):
        self.count = count
        self.reduce = plan.get("reduce")
        self.gather = plan.get("gather")

    def arguments(self):
        args = list(self.reduce[1]) if self.reduce else []
        return args + (list(self.gather[1]) if self.gather else [])

    def outputs(self):
        outs = []
        if self.reduce:
            outs += [((2,) + ref.shape[-2:], BF16, HBM_SPEC) for ref in self.reduce[1]]
        if self.gather:
            middle = (2,) * (self.count.bit_length() - 1)
            outs += [
                ((3, 2) + middle + ref.shape[-2:], BF16, HBM_SPEC) for ref in self.gather[1]
            ]
        return outs

    def scratch(self):
        scratch = []
        if self.reduce:
            scratch += reduce_scratch(self.count, [ref.shape for ref in self.reduce[1]])
        if self.gather:
            scratch += [VMEM(ref.shape, BF16) for ref in self.gather[1]]
            scratch += [DMA((len(self.gather[1]),))]
            scratch += gather_sems(self.count, len(self.gather[1]))
        return scratch

    def bind(self, args, outs, scratch):
        self.running = []
        self.loads = []
        count = self.count
        if self.reduce:
            size = len(self.reduce[1])
            used = len(reduce_scratch(count, [ref.shape for ref in self.reduce[1]]))
            self.running.append(
                Reduce(self.reduce[0], count, args[:size], outs[:size], scratch[:used])
            )
            args, outs, scratch = args[size:], outs[size:], scratch[used:]
        if self.gather:
            size = len(self.gather[1])
            blocks = scratch[:size]
            self.loads = [
                pltpu.make_async_copy(args[a], blocks[a], scratch[size].at[a]) for a in range(size)
            ]
            self.running.append(
                Gather(self.gather[0], count, blocks, outs, scratch[size + 1 : size + 6])
            )
        for load in self.loads:
            load.start()

    def peers(self):
        return self.running[0].peers() if self.running else []

    def start(self):
        for load in self.loads:
            load.wait()
        for task in self.running:
            task.start()

    def advance(self):
        for task in self.running:
            task.advance()

    def finish(self):
        for task in self.running:
            task.finish()


def pick_split(columns):
    heads = columns // HEAD
    col = lax.broadcasted_iota(jnp.int32, (columns, heads * LANES), 1)
    row = lax.broadcasted_iota(jnp.int32, (columns, heads * LANES), 0)
    inner = col & 63
    source = (col >> 7) * HEAD + ((col >> 6) & 1) * HALF + inner
    return ((row == source) & (inner < HALF)).astype(F32).astype(BF16)


def pick_plain(columns):
    heads = columns // HEAD
    col = lax.broadcasted_iota(jnp.int32, (columns, heads * LANES), 1)
    row = lax.broadcasted_iota(jnp.int32, (columns, heads * LANES), 0)
    inner = col & 127
    return ((row == (col >> 7) * HEAD + inner) & (inner < HEAD)).astype(F32).astype(BF16)


def rotated(values, cosine, sine):
    return values * cosine + pltpu.roll(values, LANES // 2, 1) * sine


def spread_qkv(wq, wk, wv, wqkv):
    small = wk.shape[0]
    q_wide = wq.shape[1] // HEAD * LANES
    k_wide = small // HEAD * LANES
    pick_q, pick_k, pick_v = pick_split(wq.shape[1]), pick_split(small), pick_plain(small)
    size = 2 * LANES

    @pl.loop(0, wq.shape[0] // size)
    def _(block):
        rows = pl.ds(pl.multiple_of(block * size, size), size)
        wqkv[rows, :q_wide] = dot_nn(wq[rows], pick_q).astype(BF16)
        wqkv[rows, q_wide : q_wide + k_wide] = dot_tn(wk[:, rows], pick_k).astype(BF16)
        wqkv[rows, q_wide + k_wide :] = dot_tn(wv[:, rows], pick_v).astype(BF16)


def allowed_pairs(seg_col, seg_row):
    full_rows = seg_col.shape[0]
    row = lax.broadcasted_iota(jnp.int32, (full_rows, full_rows), 0)
    col = lax.broadcasted_iota(jnp.int32, (full_rows, full_rows), 1)
    return (seg_col[...] == seg_row[...]) & (col <= row)


def lane_block(index):
    return pl.ds(pl.multiple_of(index * LANES, LANES), LANES)


def head_rows(ref, index):
    return ref[:, :, lane_block(index)].reshape(-1, LANES)


def attn_weights(weights, wo, sources):
    wq0, wq1, wk0, wk1, wv0, wv1, wo0, wo1 = sources[:8]
    wq, wk, wv = sources[8:]
    weights.want(wq0.at[0], wq1.at[0], wq)
    weights.want(wk0.at[0], wk1.at[0], wk)
    weights.want(wv0.at[0], wv1.at[0], wv)
    for h in range(wo.shape[0]):
        rows = pl.ds(h * HEAD, HEAD)
        weights.want(wo0.at[0, rows], wo1.at[0, rows], wo.at[h, pl.ds(0, HEAD)])


def clear_pads(wo):
    for h in range(wo.shape[0]):
        wo[h, HEAD:] = jnp.zeros((LANES - HEAD, wo.shape[2]), BF16)


def probabilities(queries, keys, allowed):
    scores = jnp.where(allowed, dot_nt(queries, keys) * HEAD ** (-0.5), neg_fill)
    exp_scores = jnp.exp(scores - jnp.max(scores, axis=-1, keepdims=True))
    return exp_scores / jnp.sum(exp_scores, axis=-1, keepdims=True)


def attn_fwd_kernel(layer, n, heads, kv_heads, others, loads_done, *refs):
    ahead = layer == 1
    x, gain, cos, sin, seg_col, seg_row = refs[:6]
    at = 6
    if ahead:
        rows_ahead = refs[at]
        at += 1
    own = refs[at : at + others]
    at += others
    if layer == 0:
        h_out, h_save, n_out, qkv_out, o_out = refs[at : at + 5]
        other = refs[at + 5 : at + 5 + others]
    else:
        other = refs[at : at + others]
        h_out, h_save, n_out, qkv_out, o_out, ahead_out = refs[at + others : at + others + 6]
        at += 1
    at += 5 + others
    (wq, wk, wv, wo, wqkv, qkv, o, osmall, part, wsem) = refs[at : at + 10]
    pair = Pair(*refs[at + 10 : at + 13])
    at += 13
    if ahead:
        second = Line(n, refs[at], None, None, *refs[at + 1 : at + 3], None, None)
        at += 3
    line = Line(n, *refs[at:])
    me = line.me
    group = heads // kv_heads
    weights = Weights(layer, wsem)
    sources = [ref for both in zip(own[:4], other[:4]) for ref in both] + [wq, wk, wv]
    attn_weights(weights, wo, sources)
    if layer == 0:
        weights.start_own()
    else:
        weights.start()
    loads_done()
    resid = x[...].astype(F32)
    line.full[me] = (resid * rms_scale(resid) * gain[...]).astype(BF16)
    clear_pads(wo)
    if ahead:
        second.full[me] = rows_ahead[...]
    if layer == 0:
        line.enter()
        line.gather_step(0)
        for mine, theirs in zip(own, other):
            pair.send(mine, theirs)

        def arrived():
            for index in range(4):
                pair.copy(own[index], other[index], index).wait_recv()

        weights.start_other(arrived)
    else:
        line.enter()
        line.gather_step(0)
    weights.wait()
    spread_qkv(wq, wk, wv, wqkv)

    def compute(shard):
        products = dot_nn(line.full[shard], wqkv[...])
        for head in range(heads + kv_heads):
            lanes = slice(head * LANES, (head + 1) * LANES)
            qkv[shard, :, lanes] = rotated(products[:, lanes], cos[shard], sin[shard]).astype(BF16)
        lanes = slice((heads + kv_heads) * LANES, None)
        qkv[shard, :, lanes] = products[:, lanes].astype(BF16)
        pair.stream(shard)

    pair.stream_share(line.full, n_out)
    pair.stream_keep(qkv, qkv_out)
    later_shards(line, compute)
    if ahead:
        second.gather_step(0)
    allowed = allowed_pairs(seg_col, seg_row)

    @pl.loop(0, kv_heads)
    def _(g):
        keys = head_rows(qkv, heads + g)
        values = head_rows(qkv, heads + kv_heads + g)
        rows = []
        for member in range(group):
            h = g * group + member
            probs = probabilities(head_rows(qkv, h), keys, allowed)
            attended = dot_nn(probs.astype(BF16), values).astype(BF16)
            o[:, :, lane_block(h)] = attended.reshape(n, -1, LANES)
            rows.append(attended)
        small = dot_nt(jnp.concatenate(rows, axis=1), pick_plain(group * HEAD))
        osmall[g] = small.astype(BF16).reshape(osmall.shape[1:])

    pair.share_half(osmall, o_out)
    wide = wo.shape[0] * LANES

    def project(shard):
        part[shard] = dot_nn(o[shard], wo[...].reshape(wide, -1))

    if ahead:

        def each(step):
            @pl.when(step < n - 1)
            def _():
                second.gather_step(step + 1)

        sums_alone(line, project, part, each)
        pair.keep(second.full, ahead_out.at[0])
        pair.send(second.full, ahead_out.at[1])
    else:
        sums_alone(line, project, part, lambda step: None)
    h_out[...] = x[...].astype(F32) + part[me]
    line.sum_take(h_out)
    pair.keep(h_out, h_save)
    if ahead:
        second.gather_end()
    line.gather_end()
    line.sum_end()
    if layer == 0:
        for index, copy in enumerate(pair.sent[:others]):
            copy.wait_send()
            if index >= 4:
                copy.wait_recv()

        @pl.when(weights.own)
        def _():
            for index in range(4):
                pair.copy(own[index], other[index], index).wait_recv()

        pair.sent[:others] = [None] * others
    pair.wait(n)


def bound(tasks, sizes, refs):
    groups, at = [], 0
    for own, extra in sizes:
        groups.append((refs[at : at + own], refs[at + own : at + own + extra]))
        at += own + extra
    tasks.bind(*(list(extra) for _, extra in groups))
    return [ref for own, _ in groups for ref in own]


def attn_bwd_kernel(layer, n, heads, kv_heads, tasks, sizes, loads_done, *refs):
    refs = bound(tasks, sizes, refs)
    (dh, x, gain, cos, sin, seg_col, seg_row, qkv_in) = refs[:8]
    own, other = refs[8:12], refs[12:16]
    (dx_out, dx_save, gain_out, da_out, dqkv_out) = refs[16:21]
    (wq, wk, wv, wo, wqkv, qkv, d_o, dqkv, dsmall, part, wsem, tsem) = refs[21:33]
    pair = Pair(*refs[33:36])
    line = Line(n, *refs[36:])
    me = line.me
    group = heads // kv_heads
    weights = Weights(layer, wsem)
    sources = [ref for both in zip(own, other) for ref in both] + [wq, wk, wv]
    attn_weights(weights, wo, sources)
    weights.start()
    take = pltpu.make_async_copy(qkv_in, qkv, tsem)
    take.start()
    line.full[me] = dh[...].astype(BF16)
    clear_pads(wo)
    line.enter(tasks.peers())
    line.gather_step(0)
    tasks.start()
    loads_done()
    weights.wait()
    spread_qkv(wq, wk, wv, wqkv)
    take.wait()
    wide = wo.shape[0] * LANES

    def compute(shard):
        d_o[shard] = dot_nt(line.full[shard], wo[...].reshape(wide, -1)).astype(BF16)
        pair.stream(shard)

    pair.stream_share(line.full, da_out)
    later_shards(line, compute)
    allowed = allowed_pairs(seg_col, seg_row)
    cosine = cos[...].reshape(-1, LANES)
    sine = -sin[...].reshape(-1, LANES)
    scale = HEAD ** (-0.5)

    @pl.loop(0, kv_heads)
    def _(g):
        keys = head_rows(qkv, heads + g)
        values = head_rows(qkv, heads + kv_heads + g)
        d_keys = d_values = None
        turned = []
        for member in range(group):
            h = g * group + member
            queries = head_rows(qkv, h)
            d_out = head_rows(d_o, h)
            probs = probabilities(queries, keys, allowed)
            d_probs = dot_nt(d_out, values)
            inner = jnp.sum(probs * d_probs, axis=-1, keepdims=True)
            d_scores = (probs * (d_probs - inner)).astype(BF16)
            d_queries = dot_nn(d_scores, keys) * scale
            turned.append(rotated(d_queries, cosine, sine).astype(BF16))
            dqkv[:, :, lane_block(h)] = turned[-1].reshape(n, -1, LANES)
            dk = dot_tn(d_scores, queries)
            dv = dot_tn(probs.astype(BF16), d_out)
            d_keys = dk if d_keys is None else d_keys + dk
            d_values = dv if d_values is None else d_values + dv
        turned.append(rotated(d_keys * scale, cosine, sine).astype(BF16))
        dqkv[:, :, lane_block(heads + g)] = turned[-1].reshape(n, -1, LANES)
        low_values = d_values.astype(BF16)
        dqkv[:, :, lane_block(heads + kv_heads + g)] = low_values.reshape(n, -1, LANES)
        small = dot_nt(jnp.concatenate(turned, axis=1), pick_split((group + 1) * HEAD))
        small_values = dot_nt(low_values, pick_plain(HEAD))
        dsmall[g] = (
            jnp.concatenate([small, small_values], axis=1).astype(BF16).reshape(dsmall.shape[1:])
        )

    pair.share_half(dsmall, dqkv_out)

    def project(shard):
        part[shard] = dot_nt(dqkv[shard], wqkv[...])

    sums_alone(line, project, part, lambda step: pl.when(step == 0)(tasks.advance))
    line.sum_take(part.at[me])
    d_resid, gain_part = norm_back(part[me], x[...].astype(F32), gain[...])
    dx_out[...] = (dh[...] + d_resid).astype(BF16)
    gain_out[...] = gain_part
    pair.keep(dx_out, dx_save)
    line.gather_end()
    line.sum_end()
    pair.wait(n)
    tasks.finish()


def ffn_fwd_kernel(layer, n, loads_done, *refs):
    (h, gain, wg0, wg1, wu0, wu1, wd0, wd1) = refs[:8]
    (y_out, y_save, n_out, gate_out, up_out, hid_out) = refs[8:14]
    (wg, wu, wd, gate, up, hid, part, wsem) = refs[14:22]
    pair = Pair(*refs[22:25])
    line = Line(n, *refs[25:])
    me = line.me
    weights = Weights(layer, wsem)
    weights.want(wg0.at[0], wg1.at[0], wg)
    weights.want(wu0.at[0], wu1.at[0], wu)
    weights.want(wd0.at[0], wd1.at[0], wd)
    weights.start()
    loads_done()
    resid = h[...]
    line.full[me] = (resid * rms_scale(resid) * gain[...]).astype(BF16)
    line.enter()
    line.gather_step(0)
    weights.wait()
    middle = hid.shape[3]

    def compute(shard):
        rows = line.full[shard]
        g = dot_nn(rows, wg[...])
        u = dot_nn(rows, wu[...])
        gate[shard] = g
        up[shard] = u
        low = (g * jax.nn.sigmoid(g) * u).astype(BF16)
        hid[0, shard] = low[:, :middle]
        hid[1, shard] = low[:, middle:]
        pair.stream(shard)
        part[shard] = dot_nn(low, wd[...])

    pair.stream_share(line.full, n_out)
    pair.stream_share_half(hid, hid_out)
    pair.stream_keep(gate, gate_out)
    pair.stream_keep(up, up_out)
    rows_then_sums(line, compute, part)
    part[me] += h[...]
    line.sum_take(part.at[me])
    y_out[...] = part[me].astype(BF16)
    pair.keep(y_out, y_save)
    line.gather_end()
    line.sum_end()
    pair.wait(n)


def ffn_bwd_kernel(layer, n, tasks, sizes, loads_done, *refs):
    refs = bound(tasks, sizes, refs)
    gathered = layer == 1
    (dy, h, gain, gate_in, up_in, wg0, wg1, wu0, wu1, wd0, wd1) = refs[:11]
    if gathered:
        (df_all, dh_out, gain_out, dmid_out) = refs[11:15]
    else:
        (dh_out, gain_out, df_all, dmid_out) = refs[11:15]
    (wg, wu, wd, gate, up, dmid, part, wsem, tsem) = refs[15:24]
    pair = Pair(*refs[24:27])
    line = Line(n, *refs[27:])
    me = line.me
    weights = Weights(layer, wsem)
    weights.want(wd0.at[0], wd1.at[0], wd)
    weights.want(wg0.at[0], wg1.at[0], wg)
    weights.want(wu0.at[0], wu1.at[0], wu)
    weights.start()
    takes = [
        pltpu.make_async_copy(gate_in, gate, tsem.at[0]),
        pltpu.make_async_copy(up_in, up, tsem.at[1]),
    ]
    if gathered:
        takes.append(pltpu.make_async_copy(df_all.at[0], line.full, tsem.at[2]))
    for take in takes:
        take.start()
    loads_done()
    if gathered:
        line.enter(tasks.peers())
    else:
        line.full[me] = dy[...]
        line.enter(tasks.peers())
        line.gather_step(0)
    tasks.start()
    weights.wait()
    for take in takes:
        take.wait()
    middle = dmid.shape[3] // 2

    def compute(shard):
        d_hidden = dot_nt(line.full[shard], wd[...])
        g = gate[shard]
        sig = jax.nn.sigmoid(g)
        d_g = (d_hidden * up[shard] * sig * (1.0 + g * (1.0 - sig))).astype(BF16)
        d_u = (d_hidden * g * sig).astype(BF16)
        for core in range(2):
            lanes = slice(core * middle, (core + 1) * middle)
            dmid[core, shard, :, :middle] = d_g[:, lanes]
            dmid[core, shard, :, middle:] = d_u[:, lanes]
        pair.stream(shard)
        part[shard] = dot_nt(d_g, wg[...]) + dot_nt(d_u, wu[...])

    pair.stream_share_half(dmid, dmid_out)
    if gathered:
        sums_alone(line, compute, part, lambda step: pl.when(step == n - 2)(tasks.advance))
    else:
        pair.stream_share(line.full, df_all)
        rows_then_sums(line, compute, part, tasks.advance)
    line.sum_take(part.at[me])
    d_resid, gain_part = norm_back(part[me], h[...], gain[...])
    dh_out[...] = dy[...].astype(F32) + d_resid
    gain_out[...] = gain_part
    if not gathered:
        line.gather_end()
    line.sum_end()
    pair.wait(n)
    tasks.finish()


def run_kernel(body, args, in_specs, outs, scratch, cid, flops, nbytes, name, aliases=None):
    loaded = [index for index, spec in enumerate(in_specs) if spec in (LOAD, LOAD_MINE)]
    buffers = [
        VMEM(args[index].shape[1:] if in_specs[index] == LOAD_MINE else args[index].shape, args[index].dtype)
        for index in loaded
    ]
    inputs, results, own = len(args), len(outs), len(scratch)

    def kernel(*refs):
        places = list(refs[: inputs + results + own])
        extra = refs[inputs + results + own :]
        copies = []
        for number, index in enumerate(loaded):
            source = refs[index]
            if in_specs[index] == LOAD_MINE:
                source = source.at[lax.axis_index("section")]
            copies.append(pltpu.make_async_copy(source, extra[number], extra[-1].at[number]))
            places[index] = extra[number]
        for copy in copies:
            copy.start()

        def loads_done():
            for copy in copies:
                copy.wait()

        body(loads_done, *places)

    return pl.pallas_call(
        kernel,
        name=name,
        in_specs=[HBM_SPEC if spec in (LOAD, LOAD_MINE) else spec for spec in in_specs],
        out_shape=[jax.ShapeDtypeStruct(shape, dtype) for shape, dtype, _ in outs],
        out_specs=[spec for _, _, spec in outs],
        scratch_shapes=[*scratch, *buffers, DMA((max(len(loaded), 1),))],
        input_output_aliases=aliases or {},
        cost_estimate=pl.CostEstimate(flops=flops, bytes_accessed=nbytes, transcendentals=0),
        compiler_params=pltpu.CompilerParams(
            collective_id=cid, has_side_effects=True, vmem_limit_bytes=VMEM_LIMITS.get(name, 44) << 20
        ),
    )(*args)


def attn_forward(layer, n, x, gain, tables, own, other, rows_ahead):
    rows, width = x.shape[-2:]
    heads = own[0].shape[2] // HEAD
    kv_heads = own[1].shape[1] // HEAD
    wide = (heads + 2 * kv_heads) * LANES
    small = heads // kv_heads * HEAD
    args = [x, gain, *tables]
    specs = [LOAD_MINE] + [VMEM_SPEC] * 5 if layer == 0 else [VMEM_SPEC] + [LOAD] * 5
    if layer == 1:
        args.append(rows_ahead)
        specs.append(LOAD_MINE)
    args += own
    specs += [HBM_SPEC] * len(own)
    outs = [
        ((rows, width), F32, VMEM_SPEC),
        ((rows, width), F32, HBM_SPEC),
        ((2, n, rows, width), BF16, HBM_SPEC),
        ((n, rows, wide), BF16, HBM_SPEC),
        ((2, n, rows, small), BF16, HBM_SPEC),
    ]
    if other is None:
        outs += [(weight.shape, weight.dtype, HBM_SPEC) for weight in own]
    else:
        args += [*other]
        specs += [HBM_SPEC] * len(other)
        outs.append(((2, n, rows, width), BF16, HBM_SPEC))
    scratch = (
        [
            VMEM((width, heads * HEAD), BF16),
            VMEM((kv_heads * HEAD, width), BF16),
            VMEM((kv_heads * HEAD, width), BF16),
            VMEM((heads, LANES, width), BF16),
            VMEM((width, wide), BF16),
            VMEM((n, rows, wide), BF16),
            VMEM((n, rows, heads * LANES), BF16),
            VMEM((kv_heads, n, rows, small), BF16),
            VMEM((n, rows, width), F32),
            DMA((3 + heads,)),
        ]
        + pair_scratch(n, 5, 3 + (len(own) if other is None else 0))
        + ([VMEM((n, rows, width), BF16)] + [DMA((2, n, CHUNKS))] * 2 if layer == 1 else [])
        + line_scratch(n, rows, width)
    )
    body = functools.partial(attn_fwd_kernel, layer, n, heads, kv_heads, len(own))
    flops = 2 * n * rows * width * wide * 3 // 2
    return run_kernel(body, args, specs, outs, scratch, 1 + layer, flops, 8 << 20, f"attn_fwd{layer}")


def attn_backward(layer, n, dh, x, gain, tables, qkv, own, other, tasks):
    rows, width = dh.shape
    heads = own[0].shape[2] // HEAD
    kv_heads = own[1].shape[1] // HEAD
    wide = (heads + 2 * kv_heads) * LANES
    small = (heads // kv_heads + 2) * HEAD
    args = [dh, x, gain, *tables, qkv, *own, *other]
    specs = [VMEM_SPEC, LOAD_MINE if x.ndim == 3 else LOAD] + [LOAD] * 5 + [HBM_SPEC] * 9
    outs = [
        ((rows, width), BF16, VMEM_SPEC),
        ((rows, width), BF16, HBM_SPEC),
        ((1, width), F32, VMEM_SPEC),
        ((2, n, rows, width), BF16, HBM_SPEC),
        ((2, n, rows, small), BF16, HBM_SPEC),
    ]
    scratch = (
        [
            VMEM((width, heads * HEAD), BF16),
            VMEM((kv_heads * HEAD, width), BF16),
            VMEM((kv_heads * HEAD, width), BF16),
            VMEM((heads, LANES, width), BF16),
            VMEM((width, wide), BF16),
            VMEM((n, rows, wide), BF16),
            VMEM((n, rows, heads * LANES), BF16),
            VMEM((n, rows, wide), BF16),
            VMEM((kv_heads, n, rows, small), BF16),
            VMEM((n, rows, width), F32),
            DMA((3 + heads,)),
            DMA,
        ]
        + pair_scratch(n, 3, 2)
        + line_scratch(n, rows, width)
    )
    body = functools.partial(attn_bwd_kernel, layer, n, heads, kv_heads)
    flops = 2 * n * rows * width * wide * 2
    return run_with_tasks(
        body, tasks, args, specs, outs, scratch, 3 + layer, flops, 8 << 20, f"attn_bwd{layer}"
    )


def ffn_forward(layer, n, h, gain, own, other):
    rows, width = h.shape
    hidden = own[0].shape[2]
    args = [h, gain]
    for mine, theirs in zip(own, other):
        args += [mine, theirs]
    specs = [VMEM_SPEC, LOAD] + [HBM_SPEC] * 6
    outs = [
        ((rows, width), BF16, VMEM_SPEC),
        ((rows, width), BF16, HBM_SPEC),
        ((2, n, rows, width), BF16, HBM_SPEC),
        ((n, rows, hidden), F32, HBM_SPEC),
        ((n, rows, hidden), F32, HBM_SPEC),
        ((2, n, rows, hidden // 2), BF16, HBM_SPEC),
    ]
    scratch = (
        [
            VMEM((width, hidden), BF16),
            VMEM((width, hidden), BF16),
            VMEM((hidden, width), BF16),
            VMEM((n, rows, hidden), F32),
            VMEM((n, rows, hidden), F32),
            VMEM((2, n, rows, hidden // 2), BF16),
            VMEM((n, rows, width), F32),
            DMA((3,)),
        ]
        + pair_scratch(n, 5, 2)
        + line_scratch(n, rows, width)
    )
    body = functools.partial(ffn_fwd_kernel, layer, n)
    flops = 6 * n * rows * width * hidden
    return run_kernel(body, args, specs, outs, scratch, 5 + layer, flops, 16 << 20, f"ffn_fwd{layer}")


def ffn_backward(layer, n, dy, h, gain, gate, up, own, other, tasks, df_all):
    rows, width = h.shape
    hidden = own[0].shape[2]
    args = [dy, h, gain, gate, up]
    for mine, theirs in zip(own, other):
        args += [mine, theirs]
    specs = [LOAD_MINE if dy.ndim == 3 else VMEM_SPEC, LOAD, LOAD] + [HBM_SPEC] * 8
    outs = [
        ((rows, width), F32, VMEM_SPEC),
        ((1, width), F32, VMEM_SPEC),
        ((2, n, rows, hidden), BF16, HBM_SPEC),
    ]
    if layer == 1:
        args.append(df_all)
        specs.append(HBM_SPEC)
    else:
        outs.insert(2, ((2, n, rows, width), BF16, HBM_SPEC))
    scratch = (
        [
            VMEM((width, hidden), BF16),
            VMEM((width, hidden), BF16),
            VMEM((hidden, width), BF16),
            VMEM((n, rows, hidden), F32),
            VMEM((n, rows, hidden), F32),
            VMEM((2, n, rows, hidden), BF16),
            VMEM((n, rows, width), F32),
            DMA((3,)),
            DMA((3,)),
        ]
        + pair_scratch(n, 2, 2)
        + line_scratch(n, rows, width)
    )
    body = functools.partial(ffn_bwd_kernel, layer, n)
    flops = 6 * n * rows * width * hidden
    return run_with_tasks(
        body, tasks, args, specs, outs, scratch, 7 + layer, flops, 16 << 20, f"ffn_bwd{layer}"
    )


def run_with_tasks(body, tasks, args, specs, outs, scratch, cid, flops, nbytes, name):
    more_args, more_outs, more_scratch = tasks.arguments(), tasks.outputs(), tasks.scratch()
    sizes = (
        (len(args), len(more_args)),
        (len(outs), len(more_outs)),
        (len(scratch), len(more_scratch)),
    )
    return run_kernel(
        functools.partial(body, tasks, sizes),
        args + more_args,
        specs + [HBM_SPEC] * len(more_args),
        outs + more_outs,
        scratch + more_scratch,
        cid,
        flops,
        nbytes,
        name,
    )


def tail_kernel(n, count, sizes, loads_done, *refs):
    ffn_size, attn_size = sizes
    at = 0

    def take(number):
        nonlocal at
        at += number
        return list(refs[at - number : at])

    gains = take(4)
    rows = take(4)
    ffn_blocks, attn_arrays, _aliased = take(ffn_size), take(attn_size), take(ffn_size + attn_size)
    (gains_out, section_out, in_grad) = take(3)
    ffn_outs, attn_outs = take(ffn_size), take(attn_size)
    by_tensor, by_dp, by_core = take(3)
    small_sems = take(2)
    ffn_vmem, attn_vmem = take(ffn_size), take(attn_size)
    (load_sem,) = take(1)
    ffn_sems, attn_sems, row_sems = take(5), take(5), take(3)
    reduce = Reduce(0, count, attn_arrays, attn_vmem, take(len(refs) - at))
    gather_ffn = Gather(0, count, ffn_vmem, ffn_outs, ffn_sems)
    gather_attn = Gather(0, count, attn_vmem, attn_outs, attn_sems)
    loads = [
        pltpu.make_async_copy(ffn_blocks[a], ffn_vmem[a], load_sem.at[a]) for a in range(ffn_size)
    ]
    for load in loads:
        load.start()
    axes = (("tensor", n, by_tensor), ("dp", count, by_dp), ("section", 2, by_core))
    barrier = pltpu.get_barrier_semaphore()
    peers = 0
    for axis, size, _ in axes:
        place = lax.axis_index(axis)
        for shift in range(1, size):
            pl.semaphore_signal(
                barrier, 1, device_id={axis: (place + shift) % size}, device_id_type=MESH
            )
            peers += 1
    pl.semaphore_wait(barrier, peers)

    def small(stage, shift):
        axis, size, slots = axes[stage]
        place = lax.axis_index(axis)
        ref = slots.at[place]
        return pltpu.make_async_remote_copy(
            ref,
            ref,
            small_sems[0].at[stage, shift],
            small_sems[1].at[stage, shift],
            device_id={axis: (place + shift) % size},
            device_id_type=MESH,
        )

    def small_start(stage, value):
        axis, size, slots = axes[stage]
        slots[lax.axis_index(axis)] = value
        for shift in range(1, size):
            small(stage, shift).start()

    def small_end(stage):
        _, size, slots = axes[stage]
        for shift in range(1, size):
            small(stage, shift).wait()
        value = slots[0]
        for index in range(1, size):
            value = value + slots[index]
        return value

    loads_done()
    small_start(0, jnp.concatenate([gain[...] for gain in gains], axis=0))
    for load in loads:
        load.wait()
    gather_ffn.start()
    reduce.start()
    core = lax.axis_index("section")

    def row_target(index):
        return (section_out, in_grad)[index // 2].at[core]

    def row_keep(index):
        return pltpu.make_async_copy(rows[index], row_target(index), row_sems[0].at[index])

    def row_send(index):
        return pltpu.make_async_remote_copy(
            rows[index],
            row_target(index),
            row_sems[1].at[index],
            row_sems[2].at[index],
            device_id={"section": 1 - core},
            device_id_type=MESH,
        )

    for index in range(4):

        @pl.when(core == index % 2)
        def _():
            row_keep(index).start()

        @pl.when(core != index % 2)
        def _():
            row_send(index).start()

    small_start(1, small_end(0))
    reduce.advance()
    small_start(2, small_end(1))
    gather_ffn.advance()
    reduce.finish()
    gather_attn.start()
    gains_out[...] = small_end(2)
    gather_attn.advance()
    gather_ffn.finish()
    gather_attn.finish()
    for index in range(4):

        @pl.when(core == index % 2)
        def _():
            row_keep(index).wait()
            row_send(index).wait_recv()

        @pl.when(core != index % 2)
        def _():
            row_send(index).wait_send()


def tail(n, count, gains, rows, ffn_blocks, attn_arrays, ffn_full, attn_full):
    sizes = (len(ffn_blocks), len(attn_arrays))
    args = [*gains, *rows, *ffn_blocks, *attn_arrays, *ffn_full, *attn_full]
    specs = [LOAD] * 8 + [HBM_SPEC] * (len(args) - 8)
    together = (4, gains[0].shape[1])
    outs = [(together, F32, VMEM_SPEC)]
    outs += [((2,) + rows[0].shape, BF16, HBM_SPEC)] * 2
    outs += [(full.shape, BF16, HBM_SPEC) for full in (*ffn_full, *attn_full)]
    scratch = [VMEM((size,) + together, F32) for size in (n, count, 2)]
    scratch += [DMA((3, max(n, count, 2)))] * 2
    scratch += [VMEM(block.shape, BF16) for block in ffn_blocks]
    scratch += [VMEM((2,) + array.shape[-2:], BF16) for array in attn_arrays]
    scratch += [DMA((sizes[0],))]
    scratch += gather_sems(count, sizes[0]) + gather_sems(count, sizes[1]) + [DMA((4,))] * 3
    scratch += reduce_scratch(count, [array.shape for array in attn_arrays])
    first = 8 + sizes[0] + sizes[1]
    aliases = {first + index: 3 + index for index in range(sum(sizes))}
    body = functools.partial(tail_kernel, n, count, sizes)
    return run_kernel(body, args, specs, outs, scratch, 9, 1 << 20, 16 << 20, "tail", aliases)


BLOCK = 256


def widen_kernel(mid_in, down_in, qkv_in, out_in, *refs):
    outs, (mid, down, qkv, o), wide, (in_sem, out_sem) = refs[:7], refs[7:11], refs[11:18], refs[18:]
    gate_w, up_w, down_w, q_w, k_w, v_w, out_w = wide
    blocks = mid.shape[1] // BLOCK
    half = mid.shape[2] // 2
    down_rows, out_rows = down.shape[1], o.shape[1]
    q_half, k_half = q_w.shape[1] // 2, k_w.shape[0] // 2

    def part(block):
        return pl.ds(pl.multiple_of(block * BLOCK, BLOCK), BLOCK)

    def mid_load(core, block):
        return pltpu.make_async_copy(
            mid_in.at[core, part(block)], mid.at[core, part(block)], in_sem.at[core, block]
        )

    def whole_load(index):
        source, target = ((down_in, down), (qkv_in, qkv), (out_in, o))[index]
        return pltpu.make_async_copy(
            source.at[pl.ds(0, 2)], target, in_sem.at[2, index]
        )

    def store(index, block=None):
        if block is None:
            return pltpu.make_async_copy(wide[index], outs[index], out_sem.at[index, 0])
        return pltpu.make_async_copy(
            wide[index].at[part(block)], outs[index].at[part(block)], out_sem.at[index, block]
        )

    @pl.loop(0, blocks)
    def _(block):
        for core in range(2):
            mid_load(core, block).start()

    for index in range(3):
        whole_load(index).start()

    @pl.loop(0, blocks)
    def _(block):
        for core in range(2):
            mid_load(core, block).wait()
            lanes = slice(core * half, (core + 1) * half)
            gate_w[part(block), lanes] = mid[core, part(block), :half].astype(F32)
            up_w[part(block), lanes] = mid[core, part(block), half:].astype(F32)
        store(0, block).start()
        store(1, block).start()

    whole_load(0).wait()
    for core in range(2):
        down_w[core * down_rows : (core + 1) * down_rows] = down[core].astype(F32)
    store(2).start()
    whole_load(1).wait()

    @pl.loop(0, qkv.shape[2] // BLOCK)
    def _(block):
        rows = jnp.concatenate(
            [qkv[core, :q_half, part(block)].astype(F32) for core in range(2)], axis=0
        )
        q_w[part(block)] = rows.T

    store(3).start()
    for core in range(2):
        rows = slice(core * k_half, (core + 1) * k_half)
        k_w[rows] = qkv[core, q_half : q_half + k_half].astype(F32)
        v_w[rows] = qkv[core, q_half + k_half :].astype(F32)
    store(4).start()
    store(5).start()
    whole_load(2).wait()
    for core in range(2):
        out_w[core * out_rows : (core + 1) * out_rows] = o[core].astype(F32)
    store(6).start()

    @pl.loop(0, blocks)
    def _(block):
        store(0, block).wait()
        store(1, block).wait()

    for index in range(2, 7):
        store(index).wait()


def widened(g_mid, g_down, g_qkv, g_out, q_size, k_size):
    width, hidden = g_mid.shape[1:]
    shapes = [(width, hidden)] * 2 + [(2 * g_down.shape[1], width), (width, q_size)]
    shapes += [(k_size, width)] * 2 + [(2 * g_out.shape[1], width)]
    blocks = width // BLOCK
    return pl.pallas_call(
        widen_kernel,
        name="widen",
        in_specs=[HBM_SPEC] * 4,
        out_shape=[jax.ShapeDtypeStruct(shape, F32) for shape in shapes],
        out_specs=[HBM_SPEC] * 7,
        scratch_shapes=[VMEM((2,) + array.shape[1:], BF16) for array in (g_mid, g_down, g_qkv, g_out)]
        + [VMEM(shape, F32) for shape in shapes]
        + [DMA((3, max(blocks, 3))), DMA((7, blocks))],
        compiler_params=pltpu.CompilerParams(vmem_limit_bytes=61 << 20),
    )(g_mid, g_down, g_qkv, g_out)


def swap(values):
    return lax.ppermute(values, "section", [(0, 1), (1, 0)])


def segment_tables(lengths_row, n, rows):
    full_rows = n * rows
    slot_count = lengths_row.shape[0]
    seq_ends = jnp.cumsum(lengths_row)
    row_index = jnp.arange(full_rows, dtype=jnp.int32)
    segment = jnp.sum((row_index[:, None] >= seq_ends[None, :]).astype(jnp.int32), axis=1)
    starts = jnp.concatenate([seq_ends - lengths_row, seq_ends[-1:]])
    chosen = segment[:, None] == jnp.arange(slot_count + 1, dtype=jnp.int32)[None, :]
    position = row_index - jnp.sum(jnp.where(chosen, starts[None, :], 0), axis=1)
    segment = jnp.where(segment < slot_count, segment, slot_count + row_index)
    lane = jnp.arange(LANES, dtype=jnp.int32)
    inner = lane % (LANES // 2)
    inverse = rope_base ** (-inner.astype(F32) * 2.0 / HEAD)
    angle = position.astype(F32)[:, None] * inverse[None, :]
    live = (inner < HALF)[None, :]
    sign = jnp.where(lane < LANES // 2, -1.0, 1.0)[None, :]
    cosine = jnp.where(live, jnp.cos(angle), 0.0)
    sine = jnp.where(live, sign * jnp.sin(angle), 0.0)
    shape = (n, rows, LANES)
    return cosine.reshape(shape), sine.reshape(shape), segment[:, None], segment[None, :]


def shards(
    inputs,
    cotangent,
    seq_lengths,
    gain_attn,
    w_query,
    w_key,
    w_value,
    w_out,
    gain_ffn,
    w_gate,
    w_up,
    w_down,
):
    section = lax.axis_index("section")
    first = section == 0
    n = lax.axis_size("tensor")
    rows = inputs.shape[1]
    attn_own = (w_query, jnp.swapaxes(w_key, 1, 2), jnp.swapaxes(w_value, 1, 2), w_out)
    ffn_own = (w_gate, w_up, w_down)
    gains = jnp.concatenate([gain_attn, gain_ffn], axis=0)
    gains_other = swap(gains)
    gains_by_layer = [
        jnp.where(first, gains, gains_other).astype(F32),
        jnp.where(first, gains_other, gains).astype(F32),
    ]
    tables = segment_tables(jnp.where(first, seq_lengths[0, 0], seq_lengths[0, 1]), n, rows)

    x = x_saved = inputs
    kept = []
    outs = []
    for layer in range(2):
        gain_a, gain_f = gains_by_layer[layer][0:1], gains_by_layer[layer][1:2]
        if layer == 0:
            h, h_saved, n_all, qkv, o, *swapped = attn_forward(
                layer, n, x, gain_a, tables, attn_own + ffn_own, None, None
            )
            attn_other, ffn_other = tuple(swapped[:4]), tuple(swapped[4:])
        else:
            h, h_saved, n_all, qkv, o, df_ahead = attn_forward(
                layer, n, x, gain_a, tables, attn_own, attn_other, cotangent
            )
        y, y_saved, n2_all, gate, up, hid = ffn_forward(layer, n, h, gain_f, ffn_own, ffn_other)
        kept.append((x_saved, h_saved, n_all, qkv, o, n2_all, gate, up, hid, gain_a, gain_f))
        outs.append(y_saved)
        x, x_saved = y, y_saved

    count = lax.axis_size("dp")
    cube = (2,) + (2,) * (count.bit_length() - 1)

    def weight_grad(left, right):
        left = left.reshape(-1, left.shape[-1])
        right = right.reshape(-1, right.shape[-1])
        return dot_tn(left, right).astype(BF16)

    def blocked(array):
        return array.reshape(*cube, -1, array.shape[-1])

    dy = cotangent
    in_grads = [None, None]
    gain_parts = [None, None]
    for layer in (1, 0):
        x, h, n_all, qkv, o, n2_all, gate, up, hid, gain_a, gain_f = kept[layer]
        if layer == 1:
            g_down = blocked(weight_grad(hid, df_ahead))
            plan = {"reduce": (1, [g_down])}
            dh, gf_part, dmid, sum_down = ffn_backward(
                layer, n, dy, h, gain_f, gate, up, ffn_own, ffn_other, Tasks(count, plan), df_ahead
            )
            g_mid = blocked(weight_grad(n2_all, dmid))
            plan = {"reduce": (1, [g_mid]), "gather": (1, [sum_down])}
        else:
            plan = {"reduce": (1, attn_grad), "gather": (1, [sum_mid])}
            dh, gf_part, df_all, dmid, *sum_attn, mid_full = ffn_backward(
                layer, n, dy, h, gain_f, gate, up, ffn_own, ffn_other, Tasks(count, plan), None
            )
            g_mid, g_down = blocked(weight_grad(n2_all, dmid)), blocked(weight_grad(hid, df_all))
            plan = {"reduce": (0, [g_mid, g_down]), "gather": (1, sum_attn)}
        dx, dx_saved, ga_part, da_all, dqkv, *more = attn_backward(
            layer, n, dh, x, gain_a, tables, qkv, attn_own, attn_other, Tasks(count, plan)
        )
        if layer == 1:
            sum_mid, down_full = more
        else:
            sum_ffn, attn_full = more[:2], more[2:]
        attn_grad = [blocked(weight_grad(dqkv, n_all)), blocked(weight_grad(o, da_all))]
        gain_parts[layer] = [ga_part, gf_part]
        in_grads[layer] = dx_saved
        dy = dx
    gain_sums, section_out, in_grad, g_mid, g_down, g_qkv, g_out = tail(
        n,
        count,
        gain_parts[0] + gain_parts[1],
        outs + in_grads,
        sum_ffn,
        attn_grad,
        [mid_full, down_full],
        attn_full,
    )
    gain_own = jnp.where(first, gain_sums[0:2], gain_sums[2:4])
    g_mid, g_down, g_qkv, g_out = (
        array.reshape(array.shape[0], -1, array.shape[-1])
        for array in (g_mid, g_down, g_qkv, g_out)
    )
    g_gate, g_up, g_down, g_query, g_key, g_value, g_out = (
        grad[None] for grad in widened(g_mid, g_down, g_qkv, g_out, w_query.shape[2], w_key.shape[2])
    )
    g_key, g_value = jnp.swapaxes(g_key, 1, 2), jnp.swapaxes(g_value, 1, 2)
    return (
        section_out[None],
        in_grad[None],
        gain_own[0:1],
        g_query,
        g_key,
        g_value,
        g_out,
        gain_own[1:2],
        g_gate,
        g_up,
        g_down,
    )


def solution(mesh):
    placed = (
        P(None, ("dp", "tensor"), None),
        P(None, ("dp", "tensor"), None),
        P("dp", None, None),
        P("section", None),
        P("section", None, "tensor"),
        P("section", None, "tensor"),
        P("section", None, "tensor"),
        P("section", "tensor", None),
        P("section", None),
        P("section", None, "tensor"),
        P("section", None, "tensor"),
        P("section", "tensor", None),
    )
    return jax.shard_map(
        shards,
        mesh=mesh,
        in_specs=placed,
        out_specs=(
            P("section", None, ("dp", "tensor"), None),
            P("section", None, ("dp", "tensor"), None),
            P("section", None),
            P("section", None, "tensor"),
            P("section", None, "tensor"),
            P("section", None, "tensor"),
            P("section", "tensor", None),
            P("section", None),
            P("section", None, "tensor"),
            P("section", None, "tensor"),
            P("section", "tensor", None),
        ),
        check_vma=False,
    )
```

```python
import functools

import jax
import jax.numpy as jnp
from jax import lax
from jax.experimental import pallas as pl
from jax.experimental.pallas import tpu as pltpu
from jax.sharding import PartitionSpec as P

HEAD = 96
HALF = HEAD // 2
LANES = 128
CHUNKS = 3
BF16 = jnp.bfloat16
F32 = jnp.float32
MESH = pl.DeviceIdType.MESH
VMEM = pltpu.VMEM
VMEM_SPEC = pl.BlockSpec(memory_space=pltpu.VMEM)
LOAD, LOAD_MINE = "load", "load mine"
VMEM_LIMITS = {"attn_fwd0": 61, "tail": 61}
HBM_SPEC = pl.BlockSpec(memory_space=pltpu.HBM)
DMA = pltpu.SemaphoreType.DMA

eps = 1e-05
rope_base = 100000.0
neg_fill = -1e30


def dot_nn(left, right):
    return lax.dot_general(left, right, (((1,), (0,)), ((), ())), preferred_element_type=F32)


def dot_nt(left, right):
    return lax.dot_general(left, right, (((1,), (1,)), ((), ())), preferred_element_type=F32)


def dot_tn(left, right):
    return lax.dot_general(left, right, (((0,), (0,)), ((), ())), preferred_element_type=F32)


def rms_scale(values):
    return lax.rsqrt(jnp.mean(values * values, axis=-1, keepdims=True) + eps)


def norm_back(d_normed, resid, gain):
    scale_rows = rms_scale(resid)
    unit_rows = resid * scale_rows
    gain_part = jnp.sum(d_normed * unit_rows, axis=0, keepdims=True)
    d_unit = d_normed * gain
    inner = jnp.mean(d_unit * unit_rows, axis=-1, keepdims=True)
    return scale_rows * (d_unit - unit_rows * inner), gain_part


class Line:
    def __init__(self, count, full, rbuf, sbuf, gs, gr, ss, sr):
        self.n = count
        self.core = lax.axis_index("section")
        self.me = lax.axis_index("tensor")
        self.full, self.rbuf, self.sbuf = full, rbuf, sbuf
        self.gs, self.gr, self.ss, self.sr = gs, gr, ss, sr
        self.rows = full.shape[1] // CHUNKS

    def span(self, c):
        return pl.ds(pl.multiple_of(c * self.rows, self.rows), self.rows)

    def neighbour(self, d):
        return self.me + 1 if d == 0 else self.me - 1

    def enter(self, also=()):
        me, n = self.me, self.n
        barrier = pltpu.get_barrier_semaphore()
        for peer in ({"section": 1 - self.core}, *also):
            pl.semaphore_signal(barrier, 1, device_id=peer, device_id_type=MESH)
        for d, there in ((1, me > 0), (0, me < n - 1)):

            @pl.when(there)
            def _():
                pl.semaphore_signal(
                    barrier, 1, device_id={"tensor": self.neighbour(d)}, device_id_type=MESH
                )

        peers = 1 + len(also) + (me > 0).astype(jnp.int32) + (me < n - 1).astype(jnp.int32)
        pl.semaphore_wait(barrier, peers)

    def gather_copy(self, d, step, shard, c):
        ref = self.full.at[shard, self.span(c)]
        return pltpu.make_async_remote_copy(
            ref,
            ref,
            self.gs.at[d, step, c],
            self.gr.at[d, step, c],
            device_id={"tensor": self.neighbour(d)},
            device_id_type=MESH,
        )

    def gather_step(self, step):
        me, n = self.me, self.n
        for c in range(CHUNKS):
            for d in range(2):
                shard = me - step if d == 0 else me + step
                holds = (shard >= 0) & (shard < n)
                onward = (me + 1 < n) if d == 0 else (me > 0)

                @pl.when(holds & (step > 0))
                def _():
                    self.gather_copy(d, step - 1, shard, c).wait_recv()

                @pl.when(holds & onward)
                def _():
                    self.gather_copy(d, step, shard, c).start()

    def gather_end(self):
        me, n = self.me, self.n

        @pl.loop(0, n - 1)
        def _(step):
            for c in range(CHUNKS):
                for d in range(2):
                    shard = me - step if d == 0 else me + step
                    onward = (me + 1 < n) if d == 0 else (me > 0)

                    @pl.when((shard >= 0) & (shard < n) & onward)
                    def _():
                        self.gather_copy(d, step, shard, c).wait_send()

    def sum_copy(self, d, shard, c):
        return pltpu.make_async_remote_copy(
            self.sbuf.at[shard, self.span(c)],
            self.rbuf.at[d, shard, self.span(c)],
            self.ss.at[d, shard, c],
            self.sr.at[d, shard, c],
            device_id={"tensor": self.neighbour(d)},
            device_id_type=MESH,
        )

    def sum_step(self, d, shard, partial):
        me, n = self.me, self.n
        goes = (shard > me) & (shard < n) if d == 0 else (shard >= 0) & (shard < me)
        first = (me == 0) if d == 0 else (me == n - 1)

        @pl.when(goes)
        def _():
            @pl.loop(0, CHUNKS)
            def _(c):
                mine = partial[shard, self.span(c)]

                @pl.when(first)
                def _():
                    self.sbuf[shard, self.span(c)] = mine.astype(BF16)

                @pl.when(jnp.logical_not(first))
                def _():
                    self.sum_copy(d, shard, c).wait_recv()
                    arrived = self.rbuf[d, shard, self.span(c)].astype(F32)
                    self.sbuf[shard, self.span(c)] = (mine + arrived).astype(BF16)

                self.sum_copy(d, shard, c).start()

    def sum_take(self, total):
        me, n = self.me, self.n
        for d, there in ((0, me > 0), (1, me < n - 1)):

            @pl.when(there)
            def _():
                @pl.loop(0, CHUNKS)
                def _(c):
                    self.sum_copy(d, me, c).wait_recv()
                    total[self.span(c)] += self.rbuf[d, me, self.span(c)].astype(F32)

    def sum_end(self):
        me, n = self.me, self.n

        @pl.loop(0, n)
        def _(shard):
            for d, goes in ((0, shard > me), (1, shard < me)):

                @pl.when(goes)
                def _():
                    for c in range(CHUNKS):
                        self.sum_copy(d, shard, c).wait_send()


def line_scratch(count, rows, width):
    return [
        VMEM((count, rows, width), BF16),
        VMEM((2, count, rows, width), BF16),
        VMEM((count, rows, width), BF16),
        DMA((2, count, CHUNKS)),
        DMA((2, count, CHUNKS)),
        DMA((2, count, CHUNKS)),
        DMA((2, count, CHUNKS)),
    ]


def rows_then_sums(line, compute, partial, halfway=lambda: None):
    me, n = line.me, line.n

    @pl.loop(0, 2 * n - 1)
    def _(step):
        @pl.when((step > 0) & (step < n))
        def _():
            line.gather_step(step)

        @pl.when(step == n - 1)
        def _():
            halfway()

        @pl.when(step < n)
        def _():
            @pl.loop(0, 2)
            def _(side):
                shard = jnp.where(side == 0, me - step, me + step)

                @pl.when((shard >= 0) & (shard < n) & ((step > 0) | (side == 0)))
                def _():
                    compute(shard)

        line.sum_step(0, step - me, partial)
        line.sum_step(1, 2 * (n - 1) - step - me, partial)


def later_shards(line, compute):
    me, n = line.me, line.n

    @pl.loop(0, n)
    def _(step):
        @pl.when(step > 0)
        def _():
            line.gather_step(step)

        @pl.loop(0, 2)
        def _(side):
            shard = jnp.where(side == 0, me - step, me + step)

            @pl.when((shard >= 0) & (shard < n) & ((step > 0) | (side == 0)))
            def _():
                compute(shard)


def sums_alone(line, compute, partial, each):
    me, n = line.me, line.n

    @pl.loop(0, n)
    def _(step):
        @pl.loop(0, 2)
        def _(side):
            shard = jnp.where(side == 0, me + n - 1 - step, step - (n - 1 - me))
            first = jnp.where(side == 0, me, 0)
            last = jnp.where(side == 0, n, me)

            @pl.when((shard >= first) & (shard < last))
            def _():
                compute(shard)

        line.sum_step(0, me + n - 1 - step, partial)
        line.sum_step(1, step - (n - 1 - me), partial)
        each(step)


class Weights:
    def __init__(self, layer, sems):
        self.own = lax.axis_index("section") == layer
        self.sems = sems
        self.wanted = []

    def want(self, mine, theirs, target):
        self.wanted.append((mine, theirs, target))

    def start_own(self):
        @pl.when(self.own)
        def _():
            for index, (mine, _theirs, target) in enumerate(self.wanted):
                pltpu.make_async_copy(mine, target, self.sems.at[index]).start()

    def start_other(self, before=lambda: None):
        @pl.when(jnp.logical_not(self.own))
        def _():
            before()
            for index, (_mine, theirs, target) in enumerate(self.wanted):
                pltpu.make_async_copy(theirs, target, self.sems.at[index]).start()

    def start(self):
        self.start_own()
        self.start_other()

    def wait(self):
        for index, (mine, _theirs, target) in enumerate(self.wanted):
            pltpu.make_async_copy(mine, target, self.sems.at[index]).wait()


class Pair:
    def __init__(self, local_sems, send_sems, recv_sems):
        self.core = lax.axis_index("section")
        self.sems = local_sems, send_sems, recv_sems
        self.kept, self.sent = [], []
        self.streams = []

    def keep(self, source, target):
        copy = pltpu.make_async_copy(source, target, self.sems[0].at[len(self.kept), 0])
        copy.start()
        self.kept.append(copy)

    def copy(self, source, target, index, part=0):
        return pltpu.make_async_remote_copy(
            source,
            target,
            self.sems[1].at[index, part],
            self.sems[2].at[index, part],
            device_id={"section": 1 - self.core},
            device_id_type=MESH,
        )

    def send(self, source, target):
        copy = self.copy(source, target, len(self.sent))
        copy.start()
        self.sent.append(copy)

    def share_half(self, halves, pair):
        self.keep(halves.at[self.core], pair.at[0])
        self.send(halves.at[1 - self.core], pair.at[1])

    def stream_keep(self, source, target):
        self.streams.append((source, target, len(self.kept), None))
        self.kept.append(None)

    def stream_share(self, source, pair):
        self.stream_keep(source, pair.at[0])
        self.streams.append((source, pair.at[1], None, len(self.sent)))
        self.sent.append(None)

    def stream_share_half(self, halves, pair):
        self.stream_keep(halves.at[self.core], pair.at[0])
        self.streams.append((halves.at[1 - self.core], pair.at[1], None, len(self.sent)))
        self.sent.append(None)

    def streamed(self, shard):
        copies = []
        for source, target, kept, sent in self.streams:
            pieces = source.at[shard], target.at[shard]
            if sent is None:
                copies.append(pltpu.make_async_copy(*pieces, self.sems[0].at[kept, shard]))
            else:
                copies.append(self.copy(*pieces, sent, shard))
        return copies

    def stream(self, shard):
        for copy in self.streamed(shard):
            copy.start()

    def wait(self, count=0):
        for copy in self.kept + self.sent:
            if copy is not None:
                copy.wait()
        if self.streams:

            @pl.loop(0, count)
            def _(shard):
                for copy in self.streamed(shard):
                    copy.wait()


def pair_scratch(count, kept, sent):
    return [DMA((max(kept, 1), count)), DMA((max(sent, 1), count)), DMA((max(sent, 1), count))]


class Cube:
    def __init__(self, layer, count):
        self.bits = count.bit_length() - 1
        assert count == 1 << self.bits
        self.me = lax.axis_index("dp")
        self.core = lax.axis_index("section")
        self.active = self.core == layer
        self.bit = [(self.me // (1 << b)) % 2 for b in range(self.bits)]
        self.down = list(range(self.bits - 1, -1, -1))

    def order(self, colour):
        return list(range(self.bits)) if colour == 0 else self.down

    def peer(self, b):
        return {"dp": self.me + (1 - 2 * self.bit[b]) * (1 << b)}

    def peers(self):
        return [self.peer(b) for b in range(self.bits)]


class Reduce(Cube):
    def __init__(self, layer, count, sources, outs, scratch):
        super().__init__(layer, count)
        self.sources, self.outs = sources, outs
        size = len(sources)
        self.accs = scratch[:size]
        self.recvs = [scratch[size * (t + 1) : size * (t + 2)] for t in range(self.bits)]
        self.local, self.ss, self.sr, self.fs = scratch[size * (self.bits + 1) :]
        self.t = 0
        self.place = [
            {b: slice(None) for b in self.down if b != self.order(c)[0]} for c in range(2)
        ]

    def items(self):
        return [(a, c) for a in range(len(self.sources)) for c in range(2)]

    def spot(self, c, changed=()):
        place = {**self.place[c], **dict(changed)}
        return (c, *(place[b] for b in self.down if b in place))

    def first_half(self, a, c, value):
        b = self.order(c)[0]
        index = [slice(None)] * self.bits
        index[self.down.index(b)] = value
        return self.sources[a].at[(c, *index)]

    def copy(self, a, c, t, source):
        return pltpu.make_async_remote_copy(
            source,
            self.recvs[t][a].at[c],
            self.ss.at[a, c, t],
            self.sr.at[a, c, t],
            device_id=self.peer(self.order(c)[t]),
            device_id_type=MESH,
        )

    def kept(self, a, c):
        mine = self.first_half(a, c, self.bit[self.order(c)[0]])
        return pltpu.make_async_copy(mine, self.accs[a].at[c], self.local.at[a, c])

    def start(self):
        for a, c in self.items():
            other = self.first_half(a, c, 1 - self.bit[self.order(c)[0]])
            self.copy(a, c, 0, other).start()
            self.kept(a, c).start()

    def advance(self):
        t = self.t
        if t >= self.bits:
            return
        for a, c in self.items():
            if t == 0:
                self.kept(a, c).wait()
            self.copy(a, c, t, self.recvs[t][a].at[c]).wait_recv()
            acc, spot = self.accs[a], self.spot(c)
            self.add(acc, spot, self.recvs[t][a], c)
            if t + 1 < self.bits:
                b = self.order(c)[t + 1]
                self.copy(a, c, t + 1, acc.at[self.spot(c, [(b, 1 - self.bit[b])])]).start()
        if t + 1 < self.bits:
            for c in range(2):
                b = self.order(c)[t + 1]
                self.place[c][b] = self.bit[b]
        self.t = t + 1

    def add(self, acc, spot, arrived, c):
        rows = acc.shape[-2]
        step = 32 if rows % 32 == 0 else rows

        @pl.loop(0, rows // step)
        def _(block):
            part = pl.ds(pl.multiple_of(block * step, step), step)
            free = (slice(None),) * (len(arrived.shape) - 3)
            total = acc[(*spot, part)].astype(F32) + arrived[(c, *free, part)].astype(F32)
            acc[(*spot, part)] = total.astype(BF16)

    def put_away(self, a, c):
        return pltpu.make_async_copy(
            self.accs[a].at[self.spot(c)], self.outs[a].at[c], self.fs.at[a, c]
        )

    def finish(self):
        while self.t < self.bits:
            self.advance()
        for a, c in self.items():
            self.put_away(a, c).start()
        for a, c in self.items():
            for t in range(self.bits):
                self.copy(a, c, t, self.recvs[t][a].at[c]).wait_send()
        for a, c in self.items():
            self.put_away(a, c).wait()


class Gather(Cube):
    def __init__(self, layer, count, blocks, outs, sems):
        super().__init__(layer, count)
        self.blocks, self.outs = blocks, outs
        self.keep, self.ss, self.sr, self.hs, self.hr = sems
        self.t = 0
        off_layer = 1 - self.core if layer == 1 else self.core
        self.slot = self.core * (1 - off_layer) + 2 * off_layer

    def items(self):
        return [(a, c) for a in range(len(self.blocks)) for c in range(2)]

    def order(self, colour):
        return super().order(colour)[::-1]

    def region(self, a, c, t, half, flipped=None):
        order = self.order(c)
        index = []
        for b in self.down:
            if b in order[:t]:
                index.append(slice(None))
            else:
                index.append(1 - self.bit[b] if flipped == order.index(b) else self.bit[b])
        return self.outs[a].at[(half, c, *index)]

    def copy(self, a, c, t):
        target = self.region(a, c, t, self.slot)
        return pltpu.make_async_remote_copy(
            self.blocks[a].at[c] if t == 0 else target,
            target,
            self.ss.at[a, c, t],
            self.sr.at[a, c, t],
            device_id=self.peer(self.order(c)[t]),
            device_id_type=MESH,
        )

    def kept(self, a, c):
        return pltpu.make_async_copy(
            self.blocks[a].at[c], self.region(a, c, 0, self.slot), self.keep.at[a, c]
        )

    def hand_over(self, a, c, t):
        if t == 0:
            source, target = self.blocks[a].at[c], self.region(a, c, 0, self.core)
        else:
            source = self.region(a, c, t - 1, self.slot, t - 1)
            target = self.region(a, c, t - 1, self.core, t - 1)
        return pltpu.make_async_remote_copy(
            source,
            target,
            self.hs.at[a, c, t],
            self.hr.at[a, c, t],
            device_id={"section": 1 - self.core},
            device_id_type=MESH,
        )

    def pass_on(self, t):
        @pl.when(jnp.logical_not(self.active))
        def _():
            for a, c in self.items():
                self.hand_over(a, c, t).start()

    def start(self):
        for a, c in self.items():
            self.copy(a, c, 0).start()
            self.kept(a, c).start()
        self.pass_on(0)

    def advance(self):
        t = self.t
        if t >= self.bits:
            return
        for a, c in self.items():
            if t == 0:
                self.kept(a, c).wait()
            self.copy(a, c, t).wait_recv()
            if t + 1 < self.bits:
                self.copy(a, c, t + 1).start()
        self.pass_on(t + 1)
        self.t = t + 1

    def finish(self):
        while self.t < self.bits:
            self.advance()
        for a, c in self.items():
            for t in range(self.bits):
                self.copy(a, c, t).wait_send()

        @pl.when(self.active)
        def _():
            for a, c in self.items():
                for t in range(self.bits + 1):
                    self.hand_over(a, c, t).wait_recv()

        @pl.when(jnp.logical_not(self.active))
        def _():
            for a, c in self.items():
                for t in range(self.bits + 1):
                    self.hand_over(a, c, t).wait_send()


def reduce_scratch(count, arrays):
    bits = count.bit_length() - 1
    scratch = []
    for level in (1, *range(1, bits + 1)):
        scratch += [VMEM((2,) + (2,) * (bits - level) + shape[-2:], BF16) for shape in arrays]
    size = len(arrays)
    return scratch + [
        DMA((size, 2)),
        DMA((size, 2, bits)),
        DMA((size, 2, bits)),
        DMA((size, 2)),
    ]


def gather_sems(count, size):
    bits = count.bit_length() - 1
    return [
        DMA((size, 2)),
        DMA((size, 2, bits)),
        DMA((size, 2, bits)),
        DMA((size, 2, bits + 1)),
        DMA((size, 2, bits + 1)),
    ]


class Tasks:
    def __init__(self, count, plan):
        self.count = count
        self.reduce = plan.get("reduce")
        self.gather = plan.get("gather")

    def arguments(self):
        args = list(self.reduce[1]) if self.reduce else []
        return args + (list(self.gather[1]) if self.gather else [])

    def outputs(self):
        outs = []
        if self.reduce:
            outs += [((2,) + ref.shape[-2:], BF16, HBM_SPEC) for ref in self.reduce[1]]
        if self.gather:
            middle = (2,) * (self.count.bit_length() - 1)
            outs += [
                ((3, 2) + middle + ref.shape[-2:], BF16, HBM_SPEC) for ref in self.gather[1]
            ]
        return outs

    def scratch(self):
        scratch = []
        if self.reduce:
            scratch += reduce_scratch(self.count, [ref.shape for ref in self.reduce[1]])
        if self.gather:
            scratch += [VMEM(ref.shape, BF16) for ref in self.gather[1]]
            scratch += [DMA((len(self.gather[1]),))]
            scratch += gather_sems(self.count, len(self.gather[1]))
        return scratch

    def bind(self, args, outs, scratch):
        self.running = []
        self.loads = []
        count = self.count
        if self.reduce:
            size = len(self.reduce[1])
            used = len(reduce_scratch(count, [ref.shape for ref in self.reduce[1]]))
            self.running.append(
                Reduce(self.reduce[0], count, args[:size], outs[:size], scratch[:used])
            )
            args, outs, scratch = args[size:], outs[size:], scratch[used:]
        if self.gather:
            size = len(self.gather[1])
            blocks = scratch[:size]
            self.loads = [
                pltpu.make_async_copy(args[a], blocks[a], scratch[size].at[a]) for a in range(size)
            ]
            self.running.append(
                Gather(self.gather[0], count, blocks, outs, scratch[size + 1 : size + 6])
            )
        for load in self.loads:
            load.start()

    def peers(self):
        return self.running[0].peers() if self.running else []

    def start(self):
        for load in self.loads:
            load.wait()
        for task in self.running:
            task.start()

    def advance(self):
        for task in self.running:
            task.advance()

    def finish(self):
        for task in self.running:
            task.finish()


def pick_split(columns):
    heads = columns // HEAD
    col = lax.broadcasted_iota(jnp.int32, (columns, heads * LANES), 1)
    row = lax.broadcasted_iota(jnp.int32, (columns, heads * LANES), 0)
    inner = col & 63
    source = (col >> 7) * HEAD + ((col >> 6) & 1) * HALF + inner
    return ((row == source) & (inner < HALF)).astype(F32).astype(BF16)


def pick_plain(columns):
    heads = columns // HEAD
    col = lax.broadcasted_iota(jnp.int32, (columns, heads * LANES), 1)
    row = lax.broadcasted_iota(jnp.int32, (columns, heads * LANES), 0)
    inner = col & 127
    return ((row == (col >> 7) * HEAD + inner) & (inner < HEAD)).astype(F32).astype(BF16)


def rotated(values, cosine, sine):
    return values * cosine + pltpu.roll(values, LANES // 2, 1) * sine


def spread_qkv(wq, wk, wv, wqkv):
    small = wk.shape[0]
    q_wide = wq.shape[1] // HEAD * LANES
    k_wide = small // HEAD * LANES
    pick_q, pick_k, pick_v = pick_split(wq.shape[1]), pick_split(small), pick_plain(small)
    size = 2 * LANES

    @pl.loop(0, wq.shape[0] // size)
    def _(block):
        rows = pl.ds(pl.multiple_of(block * size, size), size)
        wqkv[rows, :q_wide] = dot_nn(wq[rows], pick_q).astype(BF16)
        wqkv[rows, q_wide : q_wide + k_wide] = dot_tn(wk[:, rows], pick_k).astype(BF16)
        wqkv[rows, q_wide + k_wide :] = dot_tn(wv[:, rows], pick_v).astype(BF16)


def allowed_pairs(seg_col, seg_row):
    full_rows = seg_col.shape[0]
    row = lax.broadcasted_iota(jnp.int32, (full_rows, full_rows), 0)
    col = lax.broadcasted_iota(jnp.int32, (full_rows, full_rows), 1)
    return (seg_col[...] == seg_row[...]) & (col <= row)


def lane_block(index):
    return pl.ds(pl.multiple_of(index * LANES, LANES), LANES)


def head_rows(ref, index):
    return ref[:, :, lane_block(index)].reshape(-1, LANES)


def attn_weights(weights, wo, sources):
    wq0, wq1, wk0, wk1, wv0, wv1, wo0, wo1 = sources[:8]
    wq, wk, wv = sources[8:]
    weights.want(wq0.at[0], wq1.at[0], wq)
    weights.want(wk0.at[0], wk1.at[0], wk)
    weights.want(wv0.at[0], wv1.at[0], wv)
    for h in range(wo.shape[0]):
        rows = pl.ds(h * HEAD, HEAD)
        weights.want(wo0.at[0, rows], wo1.at[0, rows], wo.at[h, pl.ds(0, HEAD)])


def clear_pads(wo):
    for h in range(wo.shape[0]):
        wo[h, HEAD:] = jnp.zeros((LANES - HEAD, wo.shape[2]), BF16)


def probabilities(queries, keys, allowed):
    scores = jnp.where(allowed, dot_nt(queries, keys) * HEAD ** (-0.5), neg_fill)
    exp_scores = jnp.exp(scores - jnp.max(scores, axis=-1, keepdims=True))
    return exp_scores / jnp.sum(exp_scores, axis=-1, keepdims=True)


def attn_fwd_kernel(layer, n, heads, kv_heads, others, loads_done, *refs):
    ahead = layer == 1
    x, gain, cos, sin, seg_col, seg_row = refs[:6]
    at = 6
    if ahead:
        rows_ahead = refs[at]
        at += 1
    own = refs[at : at + others]
    at += others
    if layer == 0:
        h_out, h_save, n_out, qkv_out, o_out = refs[at : at + 5]
        other = refs[at + 5 : at + 5 + others]
    else:
        other = refs[at : at + others]
        h_out, h_save, n_out, qkv_out, o_out, ahead_out = refs[at + others : at + others + 6]
        at += 1
    at += 5 + others
    (wq, wk, wv, wo, wqkv, qkv, o, osmall, part, wsem) = refs[at : at + 10]
    pair = Pair(*refs[at + 10 : at + 13])
    at += 13
    if ahead:
        second = Line(n, refs[at], None, None, *refs[at + 1 : at + 3], None, None)
        at += 3
    line = Line(n, *refs[at:])
    me = line.me
    group = heads // kv_heads
    weights = Weights(layer, wsem)
    sources = [ref for both in zip(own[:4], other[:4]) for ref in both] + [wq, wk, wv]
    attn_weights(weights, wo, sources)
    if layer == 0:
        weights.start_own()
    else:
        weights.start()
    loads_done()
    resid = x[...].astype(F32)
    line.full[me] = (resid * rms_scale(resid) * gain[...]).astype(BF16)
    clear_pads(wo)
    if ahead:
        second.full[me] = rows_ahead[...]
    if layer == 0:
        line.enter()
        line.gather_step(0)
        for mine, theirs in zip(own, other):
            pair.send(mine, theirs)

        def arrived():
            for index in range(4):
                pair.copy(own[index], other[index], index).wait_recv()

        weights.start_other(arrived)
    else:
        line.enter()
        line.gather_step(0)
    weights.wait()
    spread_qkv(wq, wk, wv, wqkv)

    def compute(shard):
        products = dot_nn(line.full[shard], wqkv[...])
        for head in range(heads + kv_heads):
            lanes = slice(head * LANES, (head + 1) * LANES)
            qkv[shard, :, lanes] = rotated(products[:, lanes], cos[shard], sin[shard]).astype(BF16)
        lanes = slice((heads + kv_heads) * LANES, None)
        qkv[shard, :, lanes] = products[:, lanes].astype(BF16)
        pair.stream(shard)

    pair.stream_share(line.full, n_out)
    pair.stream_keep(qkv, qkv_out)
    later_shards(line, compute)
    if ahead:
        second.gather_step(0)
    allowed = allowed_pairs(seg_col, seg_row)

    @pl.loop(0, kv_heads)
    def _(g):
        keys = head_rows(qkv, heads + g)
        values = head_rows(qkv, heads + kv_heads + g)

        @pl.loop(0, group)
        def _(member):
            h = g * group + member
            probs = probabilities(head_rows(qkv, h), keys, allowed)
            attended = dot_nn(probs.astype(BF16), values).astype(BF16)
            o[:, :, lane_block(h)] = attended.reshape(n, -1, LANES)

        wide_heads = [head_rows(o, g * group + member) for member in range(group)]
        small = dot_nt(jnp.concatenate(wide_heads, axis=1), pick_plain(group * HEAD))
        osmall[g] = small.astype(BF16).reshape(osmall.shape[1:])

    pair.share_half(osmall, o_out)
    wide = wo.shape[0] * LANES

    def project(shard):
        part[shard] = dot_nn(o[shard], wo[...].reshape(wide, -1))

    if ahead:

        def each(step):
            @pl.when(step < n - 1)
            def _():
                second.gather_step(step + 1)

        sums_alone(line, project, part, each)
        pair.keep(second.full, ahead_out.at[0])
        pair.send(second.full, ahead_out.at[1])
    else:
        sums_alone(line, project, part, lambda step: None)
    h_out[...] = x[...].astype(F32) + part[me]
    line.sum_take(h_out)
    pair.keep(h_out, h_save)
    if ahead:
        second.gather_end()
    line.gather_end()
    line.sum_end()
    if layer == 0:
        for index, copy in enumerate(pair.sent[:others]):
            copy.wait_send()
            if index >= 4:
                copy.wait_recv()

        @pl.when(weights.own)
        def _():
            for index in range(4):
                pair.copy(own[index], other[index], index).wait_recv()

        pair.sent[:others] = [None] * others
    pair.wait(n)


def bound(tasks, sizes, refs):
    groups, at = [], 0
    for own, extra in sizes:
        groups.append((refs[at : at + own], refs[at + own : at + own + extra]))
        at += own + extra
    tasks.bind(*(list(extra) for _, extra in groups))
    return [ref for own, _ in groups for ref in own]


def attn_bwd_kernel(layer, n, heads, kv_heads, tasks, sizes, loads_done, *refs):
    refs = bound(tasks, sizes, refs)
    (dh, x, gain, cos, sin, seg_col, seg_row, qkv_in) = refs[:8]
    own, other = refs[8:12], refs[12:16]
    (dx_out, dx_save, gain_out, da_out, dqkv_out) = refs[16:21]
    (wq, wk, wv, wo, wqkv, qkv, d_o, dqkv, dsmall, part, dkv, wsem, tsem) = refs[21:34]
    pair = Pair(*refs[34:37])
    line = Line(n, *refs[37:])
    me = line.me
    group = heads // kv_heads
    weights = Weights(layer, wsem)
    sources = [ref for both in zip(own, other) for ref in both] + [wq, wk, wv]
    attn_weights(weights, wo, sources)
    weights.start()
    take = pltpu.make_async_copy(qkv_in, qkv, tsem)
    take.start()
    line.full[me] = dh[...].astype(BF16)
    clear_pads(wo)
    line.enter(tasks.peers())
    line.gather_step(0)
    tasks.start()
    loads_done()
    weights.wait()
    spread_qkv(wq, wk, wv, wqkv)
    take.wait()
    wide = wo.shape[0] * LANES

    def compute(shard):
        d_o[shard] = dot_nt(line.full[shard], wo[...].reshape(wide, -1)).astype(BF16)
        pair.stream(shard)

    pair.stream_share(line.full, da_out)
    later_shards(line, compute)
    allowed = allowed_pairs(seg_col, seg_row)
    cosine = cos[...].reshape(-1, LANES)
    sine = -sin[...].reshape(-1, LANES)
    scale = HEAD ** (-0.5)

    @pl.loop(0, kv_heads)
    def _(g):
        keys = head_rows(qkv, heads + g)
        values = head_rows(qkv, heads + kv_heads + g)
        dkv[...] = jnp.zeros_like(dkv)

        @pl.loop(0, group)
        def _(member):
            h = g * group + member
            queries = head_rows(qkv, h)
            d_out = head_rows(d_o, h)
            probs = probabilities(queries, keys, allowed)
            d_probs = dot_nt(d_out, values)
            inner = jnp.sum(probs * d_probs, axis=-1, keepdims=True)
            d_scores = (probs * (d_probs - inner)).astype(BF16)
            d_queries = dot_nn(d_scores, keys) * scale
            turned = rotated(d_queries, cosine, sine).astype(BF16)
            dqkv[:, :, lane_block(h)] = turned.reshape(n, -1, LANES)
            dkv[0] += dot_tn(d_scores, queries)
            dkv[1] += dot_tn(probs.astype(BF16), d_out)

        low_keys = rotated(dkv[0] * scale, cosine, sine).astype(BF16)
        low_values = dkv[1].astype(BF16)
        dqkv[:, :, lane_block(heads + g)] = low_keys.reshape(n, -1, LANES)
        dqkv[:, :, lane_block(heads + kv_heads + g)] = low_values.reshape(n, -1, LANES)
        wide_heads = [head_rows(dqkv, g * group + member) for member in range(group)] + [low_keys]
        small = dot_nt(jnp.concatenate(wide_heads, axis=1), pick_split((group + 1) * HEAD))
        small_values = dot_nt(low_values, pick_plain(HEAD))
        dsmall[g] = (
            jnp.concatenate([small, small_values], axis=1).astype(BF16).reshape(dsmall.shape[1:])
        )

    pair.share_half(dsmall, dqkv_out)

    def project(shard):
        part[shard] = dot_nt(dqkv[shard], wqkv[...])

    sums_alone(line, project, part, lambda step: pl.when(step == 0)(tasks.advance))
    line.sum_take(part.at[me])
    d_resid, gain_part = norm_back(part[me], x[...].astype(F32), gain[...])
    dx_out[...] = (dh[...] + d_resid).astype(BF16)
    gain_out[...] = gain_part
    pair.keep(dx_out, dx_save)
    line.gather_end()
    line.sum_end()
    pair.wait(n)
    tasks.finish()


def ffn_fwd_kernel(layer, n, loads_done, *refs):
    (h, gain, wg0, wg1, wu0, wu1, wd0, wd1) = refs[:8]
    (y_out, y_save, n_out, gate_out, up_out, hid_out) = refs[8:14]
    (wg, wu, wd, gate, up, hid, part, wsem) = refs[14:22]
    pair = Pair(*refs[22:25])
    line = Line(n, *refs[25:])
    me = line.me
    weights = Weights(layer, wsem)
    weights.want(wg0.at[0], wg1.at[0], wg)
    weights.want(wu0.at[0], wu1.at[0], wu)
    weights.want(wd0.at[0], wd1.at[0], wd)
    weights.start()
    loads_done()
    resid = h[...]
    line.full[me] = (resid * rms_scale(resid) * gain[...]).astype(BF16)
    line.enter()
    line.gather_step(0)
    weights.wait()
    middle = hid.shape[3]

    def compute(shard):
        part[shard] = jnp.zeros(part.shape[1:], F32)

        @pl.loop(0, 2)
        def _(core):
            lanes = pl.ds(pl.multiple_of(core * middle, middle), middle)
            rows = line.full[shard]
            g = dot_nn(rows, wg[:, lanes])
            u = dot_nn(rows, wu[:, lanes])
            gate[shard, :, lanes] = g
            up[shard, :, lanes] = u
            low = (g * jax.nn.sigmoid(g) * u).astype(BF16)
            hid[core, shard] = low
            part[shard] += dot_nn(low, wd[lanes])

        pair.stream(shard)

    pair.stream_share(line.full, n_out)
    pair.stream_share_half(hid, hid_out)
    pair.stream_keep(gate, gate_out)
    pair.stream_keep(up, up_out)
    rows_then_sums(line, compute, part)
    part[me] += h[...]
    line.sum_take(part.at[me])
    y_out[...] = part[me].astype(BF16)
    pair.keep(y_out, y_save)
    line.gather_end()
    line.sum_end()
    pair.wait(n)


def ffn_bwd_kernel(layer, n, tasks, sizes, loads_done, *refs):
    refs = bound(tasks, sizes, refs)
    gathered = layer == 1
    (dy, h, gain, gate_in, up_in, wg0, wg1, wu0, wu1, wd0, wd1) = refs[:11]
    if gathered:
        (df_all, dh_out, gain_out, dmid_out) = refs[11:15]
    else:
        (dh_out, gain_out, df_all, dmid_out) = refs[11:15]
    (wg, wu, wd, gate, up, dmid, part, wsem, tsem) = refs[15:24]
    pair = Pair(*refs[24:27])
    line = Line(n, *refs[27:])
    me = line.me
    weights = Weights(layer, wsem)
    weights.want(wd0.at[0], wd1.at[0], wd)
    weights.want(wg0.at[0], wg1.at[0], wg)
    weights.want(wu0.at[0], wu1.at[0], wu)
    weights.start()
    takes = [
        pltpu.make_async_copy(gate_in, gate, tsem.at[0]),
        pltpu.make_async_copy(up_in, up, tsem.at[1]),
    ]
    if gathered:
        takes.append(pltpu.make_async_copy(df_all.at[0], line.full, tsem.at[2]))
    for take in takes:
        take.start()
    loads_done()
    if gathered:
        line.enter(tasks.peers())
    else:
        line.full[me] = dy[...]
        line.enter(tasks.peers())
        line.gather_step(0)
    tasks.start()
    weights.wait()
    for take in takes:
        take.wait()
    middle = dmid.shape[3] // 2

    def compute(shard):
        part[shard] = jnp.zeros(part.shape[1:], F32)

        @pl.loop(0, 2)
        def _(core):
            lanes = pl.ds(pl.multiple_of(core * middle, middle), middle)
            d_hidden = dot_nt(line.full[shard], wd[lanes])
            g = gate[shard, :, lanes]
            sig = jax.nn.sigmoid(g)
            d_g = (d_hidden * up[shard, :, lanes] * sig * (1.0 + g * (1.0 - sig))).astype(BF16)
            d_u = (d_hidden * g * sig).astype(BF16)
            dmid[core, shard, :, :middle] = d_g
            dmid[core, shard, :, middle:] = d_u
            part[shard] += dot_nt(d_g, wg[:, lanes]) + dot_nt(d_u, wu[:, lanes])

        pair.stream(shard)

    pair.stream_share_half(dmid, dmid_out)
    if gathered:
        sums_alone(line, compute, part, lambda step: pl.when(step == n - 2)(tasks.advance))
    else:
        pair.stream_share(line.full, df_all)
        rows_then_sums(line, compute, part, tasks.advance)
    line.sum_take(part.at[me])
    d_resid, gain_part = norm_back(part[me], h[...], gain[...])
    dh_out[...] = dy[...].astype(F32) + d_resid
    gain_out[...] = gain_part
    if not gathered:
        line.gather_end()
    line.sum_end()
    pair.wait(n)
    tasks.finish()


def run_kernel(body, args, in_specs, outs, scratch, cid, flops, nbytes, name, aliases=None):
    loaded = [index for index, spec in enumerate(in_specs) if spec in (LOAD, LOAD_MINE)]
    buffers = [
        VMEM(args[index].shape[1:] if in_specs[index] == LOAD_MINE else args[index].shape, args[index].dtype)
        for index in loaded
    ]
    inputs, results, own = len(args), len(outs), len(scratch)

    def kernel(*refs):
        places = list(refs[: inputs + results + own])
        extra = refs[inputs + results + own :]
        copies = []
        for number, index in enumerate(loaded):
            source = refs[index]
            if in_specs[index] == LOAD_MINE:
                source = source.at[lax.axis_index("section")]
            copies.append(pltpu.make_async_copy(source, extra[number], extra[-1].at[number]))
            places[index] = extra[number]
        for copy in copies:
            copy.start()

        def loads_done():
            for copy in copies:
                copy.wait()

        body(loads_done, *places)

    return pl.pallas_call(
        kernel,
        name=name,
        in_specs=[HBM_SPEC if spec in (LOAD, LOAD_MINE) else spec for spec in in_specs],
        out_shape=[jax.ShapeDtypeStruct(shape, dtype) for shape, dtype, _ in outs],
        out_specs=[spec for _, _, spec in outs],
        scratch_shapes=[*scratch, *buffers, DMA((max(len(loaded), 1),))],
        input_output_aliases=aliases or {},
        cost_estimate=pl.CostEstimate(flops=flops, bytes_accessed=nbytes, transcendentals=0),
        compiler_params=pltpu.CompilerParams(
            collective_id=cid, has_side_effects=True, vmem_limit_bytes=VMEM_LIMITS.get(name, 44) << 20
        ),
    )(*args)


def attn_forward(layer, n, x, gain, tables, own, other, rows_ahead):
    rows, width = x.shape[-2:]
    heads = own[0].shape[2] // HEAD
    kv_heads = own[1].shape[1] // HEAD
    wide = (heads + 2 * kv_heads) * LANES
    small = heads // kv_heads * HEAD
    args = [x, gain, *tables]
    specs = [LOAD_MINE] + [VMEM_SPEC] * 5 if layer == 0 else [VMEM_SPEC] + [LOAD] * 5
    if layer == 1:
        args.append(rows_ahead)
        specs.append(LOAD_MINE)
    args += own
    specs += [HBM_SPEC] * len(own)
    outs = [
        ((rows, width), F32, VMEM_SPEC),
        ((rows, width), F32, HBM_SPEC),
        ((2, n, rows, width), BF16, HBM_SPEC),
        ((n, rows, wide), BF16, HBM_SPEC),
        ((2, n, rows, small), BF16, HBM_SPEC),
    ]
    if other is None:
        outs += [(weight.shape, weight.dtype, HBM_SPEC) for weight in own]
    else:
        args += [*other]
        specs += [HBM_SPEC] * len(other)
        outs.append(((2, n, rows, width), BF16, HBM_SPEC))
    scratch = (
        [
            VMEM((width, heads * HEAD), BF16),
            VMEM((kv_heads * HEAD, width), BF16),
            VMEM((kv_heads * HEAD, width), BF16),
            VMEM((heads, LANES, width), BF16),
            VMEM((width, wide), BF16),
            VMEM((n, rows, wide), BF16),
            VMEM((n, rows, heads * LANES), BF16),
            VMEM((kv_heads, n, rows, small), BF16),
            VMEM((n, rows, width), F32),
            DMA((3 + heads,)),
        ]
        + pair_scratch(n, 5, 3 + (len(own) if other is None else 0))
        + ([VMEM((n, rows, width), BF16)] + [DMA((2, n, CHUNKS))] * 2 if layer == 1 else [])
        + line_scratch(n, rows, width)
    )
    body = functools.partial(attn_fwd_kernel, layer, n, heads, kv_heads, len(own))
    flops = 2 * n * rows * width * wide * 3 // 2
    return run_kernel(body, args, specs, outs, scratch, 1 + layer, flops, 8 << 20, f"attn_fwd{layer}")


def attn_backward(layer, n, dh, x, gain, tables, qkv, own, other, tasks):
    rows, width = dh.shape
    heads = own[0].shape[2] // HEAD
    kv_heads = own[1].shape[1] // HEAD
    wide = (heads + 2 * kv_heads) * LANES
    small = (heads // kv_heads + 2) * HEAD
    args = [dh, x, gain, *tables, qkv, *own, *other]
    specs = [VMEM_SPEC, LOAD_MINE if x.ndim == 3 else LOAD] + [LOAD] * 5 + [HBM_SPEC] * 9
    outs = [
        ((rows, width), BF16, VMEM_SPEC),
        ((rows, width), BF16, HBM_SPEC),
        ((1, width), F32, VMEM_SPEC),
        ((2, n, rows, width), BF16, HBM_SPEC),
        ((2, n, rows, small), BF16, HBM_SPEC),
    ]
    scratch = (
        [
            VMEM((width, heads * HEAD), BF16),
            VMEM((kv_heads * HEAD, width), BF16),
            VMEM((kv_heads * HEAD, width), BF16),
            VMEM((heads, LANES, width), BF16),
            VMEM((width, wide), BF16),
            VMEM((n, rows, wide), BF16),
            VMEM((n, rows, heads * LANES), BF16),
            VMEM((n, rows, wide), BF16),
            VMEM((kv_heads, n, rows, small), BF16),
            VMEM((n, rows, width), F32),
            VMEM((2, n * rows, LANES), F32),
            DMA((3 + heads,)),
            DMA,
        ]
        + pair_scratch(n, 3, 2)
        + line_scratch(n, rows, width)
    )
    body = functools.partial(attn_bwd_kernel, layer, n, heads, kv_heads)
    flops = 2 * n * rows * width * wide * 2
    return run_with_tasks(
        body, tasks, args, specs, outs, scratch, 3 + layer, flops, 8 << 20, f"attn_bwd{layer}"
    )


def ffn_forward(layer, n, h, gain, own, other):
    rows, width = h.shape
    hidden = own[0].shape[2]
    args = [h, gain]
    for mine, theirs in zip(own, other):
        args += [mine, theirs]
    specs = [VMEM_SPEC, LOAD] + [HBM_SPEC] * 6
    outs = [
        ((rows, width), BF16, VMEM_SPEC),
        ((rows, width), BF16, HBM_SPEC),
        ((2, n, rows, width), BF16, HBM_SPEC),
        ((n, rows, hidden), F32, HBM_SPEC),
        ((n, rows, hidden), F32, HBM_SPEC),
        ((2, n, rows, hidden // 2), BF16, HBM_SPEC),
    ]
    scratch = (
        [
            VMEM((width, hidden), BF16),
            VMEM((width, hidden), BF16),
            VMEM((hidden, width), BF16),
            VMEM((n, rows, hidden), F32),
            VMEM((n, rows, hidden), F32),
            VMEM((2, n, rows, hidden // 2), BF16),
            VMEM((n, rows, width), F32),
            DMA((3,)),
        ]
        + pair_scratch(n, 5, 2)
        + line_scratch(n, rows, width)
    )
    body = functools.partial(ffn_fwd_kernel, layer, n)
    flops = 6 * n * rows * width * hidden
    return run_kernel(body, args, specs, outs, scratch, 5 + layer, flops, 16 << 20, f"ffn_fwd{layer}")


def ffn_backward(layer, n, dy, h, gain, gate, up, own, other, tasks, df_all):
    rows, width = h.shape
    hidden = own[0].shape[2]
    args = [dy, h, gain, gate, up]
    for mine, theirs in zip(own, other):
        args += [mine, theirs]
    specs = [LOAD_MINE if dy.ndim == 3 else VMEM_SPEC, LOAD, LOAD] + [HBM_SPEC] * 8
    outs = [
        ((rows, width), F32, VMEM_SPEC),
        ((1, width), F32, VMEM_SPEC),
        ((2, n, rows, hidden), BF16, HBM_SPEC),
    ]
    if layer == 1:
        args.append(df_all)
        specs.append(HBM_SPEC)
    else:
        outs.insert(2, ((2, n, rows, width), BF16, HBM_SPEC))
    scratch = (
        [
            VMEM((width, hidden), BF16),
            VMEM((width, hidden), BF16),
            VMEM((hidden, width), BF16),
            VMEM((n, rows, hidden), F32),
            VMEM((n, rows, hidden), F32),
            VMEM((2, n, rows, hidden), BF16),
            VMEM((n, rows, width), F32),
            DMA((3,)),
            DMA((3,)),
        ]
        + pair_scratch(n, 2, 2)
        + line_scratch(n, rows, width)
    )
    body = functools.partial(ffn_bwd_kernel, layer, n)
    flops = 6 * n * rows * width * hidden
    return run_with_tasks(
        body, tasks, args, specs, outs, scratch, 7 + layer, flops, 16 << 20, f"ffn_bwd{layer}"
    )


def run_with_tasks(body, tasks, args, specs, outs, scratch, cid, flops, nbytes, name):
    more_args, more_outs, more_scratch = tasks.arguments(), tasks.outputs(), tasks.scratch()
    sizes = (
        (len(args), len(more_args)),
        (len(outs), len(more_outs)),
        (len(scratch), len(more_scratch)),
    )
    return run_kernel(
        functools.partial(body, tasks, sizes),
        args + more_args,
        specs + [HBM_SPEC] * len(more_args),
        outs + more_outs,
        scratch + more_scratch,
        cid,
        flops,
        nbytes,
        name,
    )


def tail_kernel(n, count, sizes, loads_done, *refs):
    ffn_size, attn_size = sizes
    at = 0

    def take(number):
        nonlocal at
        at += number
        return list(refs[at - number : at])

    gains = take(4)
    rows = take(4)
    ffn_blocks, attn_arrays, _aliased = take(ffn_size), take(attn_size), take(ffn_size + attn_size)
    (gains_out, section_out, in_grad) = take(3)
    ffn_outs, attn_outs = take(ffn_size), take(attn_size)
    by_tensor, by_dp, by_core = take(3)
    small_sems = take(2)
    ffn_vmem, attn_vmem = take(ffn_size), take(attn_size)
    (load_sem,) = take(1)
    ffn_sems, attn_sems, row_sems = take(5), take(5), take(3)
    reduce = Reduce(0, count, attn_arrays, attn_vmem, take(len(refs) - at))
    gather_ffn = Gather(0, count, ffn_vmem, ffn_outs, ffn_sems)
    gather_attn = Gather(0, count, attn_vmem, attn_outs, attn_sems)
    loads = [
        pltpu.make_async_copy(ffn_blocks[a], ffn_vmem[a], load_sem.at[a]) for a in range(ffn_size)
    ]
    for load in loads:
        load.start()
    axes = (("tensor", n, by_tensor), ("dp", count, by_dp), ("section", 2, by_core))
    barrier = pltpu.get_barrier_semaphore()
    peers = 0
    for axis, size, _ in axes:
        place = lax.axis_index(axis)
        for shift in range(1, size):
            pl.semaphore_signal(
                barrier, 1, device_id={axis: (place + shift) % size}, device_id_type=MESH
            )
            peers += 1
    pl.semaphore_wait(barrier, peers)

    def small(stage, shift):
        axis, size, slots = axes[stage]
        place = lax.axis_index(axis)
        ref = slots.at[place]
        return pltpu.make_async_remote_copy(
            ref,
            ref,
            small_sems[0].at[stage, shift],
            small_sems[1].at[stage, shift],
            device_id={axis: (place + shift) % size},
            device_id_type=MESH,
        )

    def small_start(stage, value):
        axis, size, slots = axes[stage]
        slots[lax.axis_index(axis)] = value
        for shift in range(1, size):
            small(stage, shift).start()

    def small_end(stage):
        _, size, slots = axes[stage]
        for shift in range(1, size):
            small(stage, shift).wait()
        value = slots[0]
        for index in range(1, size):
            value = value + slots[index]
        return value

    loads_done()
    small_start(0, jnp.concatenate([gain[...] for gain in gains], axis=0))
    for load in loads:
        load.wait()
    gather_ffn.start()
    reduce.start()
    core = lax.axis_index("section")

    def row_target(index):
        return (section_out, in_grad)[index // 2].at[core]

    def row_keep(index):
        return pltpu.make_async_copy(rows[index], row_target(index), row_sems[0].at[index])

    def row_send(index):
        return pltpu.make_async_remote_copy(
            rows[index],
            row_target(index),
            row_sems[1].at[index],
            row_sems[2].at[index],
            device_id={"section": 1 - core},
            device_id_type=MESH,
        )

    for index in range(4):

        @pl.when(core == index % 2)
        def _():
            row_keep(index).start()

        @pl.when(core != index % 2)
        def _():
            row_send(index).start()

    small_start(1, small_end(0))
    reduce.advance()
    small_start(2, small_end(1))
    gather_ffn.advance()
    reduce.finish()
    gather_attn.start()
    gains_out[...] = small_end(2)
    gather_attn.advance()
    gather_ffn.finish()
    gather_attn.finish()
    for index in range(4):

        @pl.when(core == index % 2)
        def _():
            row_keep(index).wait()
            row_send(index).wait_recv()

        @pl.when(core != index % 2)
        def _():
            row_send(index).wait_send()


def tail(n, count, gains, rows, ffn_blocks, attn_arrays, ffn_full, attn_full):
    sizes = (len(ffn_blocks), len(attn_arrays))
    args = [*gains, *rows, *ffn_blocks, *attn_arrays, *ffn_full, *attn_full]
    specs = [LOAD] * 8 + [HBM_SPEC] * (len(args) - 8)
    together = (4, gains[0].shape[1])
    outs = [(together, F32, VMEM_SPEC)]
    outs += [((2,) + rows[0].shape, BF16, HBM_SPEC)] * 2
    outs += [(full.shape, BF16, HBM_SPEC) for full in (*ffn_full, *attn_full)]
    scratch = [VMEM((size,) + together, F32) for size in (n, count, 2)]
    scratch += [DMA((3, max(n, count, 2)))] * 2
    scratch += [VMEM(block.shape, BF16) for block in ffn_blocks]
    scratch += [VMEM((2,) + array.shape[-2:], BF16) for array in attn_arrays]
    scratch += [DMA((sizes[0],))]
    scratch += gather_sems(count, sizes[0]) + gather_sems(count, sizes[1]) + [DMA((4,))] * 3
    scratch += reduce_scratch(count, [array.shape for array in attn_arrays])
    first = 8 + sizes[0] + sizes[1]
    aliases = {first + index: 3 + index for index in range(sum(sizes))}
    body = functools.partial(tail_kernel, n, count, sizes)
    return run_kernel(body, args, specs, outs, scratch, 9, 1 << 20, 16 << 20, "tail", aliases)


BLOCK = 256


def widen_kernel(mid_in, down_in, qkv_in, out_in, *refs):
    outs, (mid, down, qkv, o), wide, (in_sem, out_sem) = refs[:7], refs[7:11], refs[11:18], refs[18:]
    gate_w, up_w, down_w, q_w, k_w, v_w, out_w = wide
    blocks = mid.shape[1] // BLOCK
    half = mid.shape[2] // 2
    down_rows, out_rows = down.shape[1], o.shape[1]
    q_half, k_half = q_w.shape[1] // 2, k_w.shape[0] // 2

    def part(block):
        return pl.ds(pl.multiple_of(block * BLOCK, BLOCK), BLOCK)

    def mid_load(core, block):
        return pltpu.make_async_copy(
            mid_in.at[core, part(block)], mid.at[core, part(block)], in_sem.at[core, block]
        )

    def whole_load(index):
        source, target = ((down_in, down), (qkv_in, qkv), (out_in, o))[index]
        return pltpu.make_async_copy(
            source.at[pl.ds(0, 2)], target, in_sem.at[2, index]
        )

    def store(index, block=None):
        if block is None:
            return pltpu.make_async_copy(wide[index], outs[index], out_sem.at[index, 0])
        return pltpu.make_async_copy(
            wide[index].at[part(block)], outs[index].at[part(block)], out_sem.at[index, block]
        )

    @pl.loop(0, blocks)
    def _(block):
        for core in range(2):
            mid_load(core, block).start()

    for index in range(3):
        whole_load(index).start()

    @pl.loop(0, blocks)
    def _(block):
        for core in range(2):
            mid_load(core, block).wait()
            lanes = slice(core * half, (core + 1) * half)
            gate_w[part(block), lanes] = mid[core, part(block), :half].astype(F32)
            up_w[part(block), lanes] = mid[core, part(block), half:].astype(F32)
        store(0, block).start()
        store(1, block).start()

    whole_load(0).wait()
    for core in range(2):
        down_w[core * down_rows : (core + 1) * down_rows] = down[core].astype(F32)
    store(2).start()
    whole_load(1).wait()

    @pl.loop(0, qkv.shape[2] // BLOCK)
    def _(block):
        rows = jnp.concatenate(
            [qkv[core, :q_half, part(block)].astype(F32) for core in range(2)], axis=0
        )
        q_w[part(block)] = rows.T

    store(3).start()
    for core in range(2):
        rows = slice(core * k_half, (core + 1) * k_half)
        k_w[rows] = qkv[core, q_half : q_half + k_half].astype(F32)
        v_w[rows] = qkv[core, q_half + k_half :].astype(F32)
    store(4).start()
    store(5).start()
    whole_load(2).wait()
    for core in range(2):
        out_w[core * out_rows : (core + 1) * out_rows] = o[core].astype(F32)
    store(6).start()

    @pl.loop(0, blocks)
    def _(block):
        store(0, block).wait()
        store(1, block).wait()

    for index in range(2, 7):
        store(index).wait()


def widened(g_mid, g_down, g_qkv, g_out, q_size, k_size):
    width, hidden = g_mid.shape[1:]
    shapes = [(width, hidden)] * 2 + [(2 * g_down.shape[1], width), (width, q_size)]
    shapes += [(k_size, width)] * 2 + [(2 * g_out.shape[1], width)]
    blocks = width // BLOCK
    return pl.pallas_call(
        widen_kernel,
        name="widen",
        in_specs=[HBM_SPEC] * 4,
        out_shape=[jax.ShapeDtypeStruct(shape, F32) for shape in shapes],
        out_specs=[HBM_SPEC] * 7,
        scratch_shapes=[VMEM((2,) + array.shape[1:], BF16) for array in (g_mid, g_down, g_qkv, g_out)]
        + [VMEM(shape, F32) for shape in shapes]
        + [DMA((3, max(blocks, 3))), DMA((7, blocks))],
        compiler_params=pltpu.CompilerParams(vmem_limit_bytes=61 << 20),
    )(g_mid, g_down, g_qkv, g_out)


def swap(values):
    return lax.ppermute(values, "section", [(0, 1), (1, 0)])


def segment_tables(lengths_row, n, rows):
    full_rows = n * rows
    slot_count = lengths_row.shape[0]
    seq_ends = jnp.cumsum(lengths_row)
    row_index = jnp.arange(full_rows, dtype=jnp.int32)
    segment = jnp.sum((row_index[:, None] >= seq_ends[None, :]).astype(jnp.int32), axis=1)
    starts = jnp.concatenate([seq_ends - lengths_row, seq_ends[-1:]])
    chosen = segment[:, None] == jnp.arange(slot_count + 1, dtype=jnp.int32)[None, :]
    position = row_index - jnp.sum(jnp.where(chosen, starts[None, :], 0), axis=1)
    segment = jnp.where(segment < slot_count, segment, slot_count + row_index)
    lane = jnp.arange(LANES, dtype=jnp.int32)
    inner = lane % (LANES // 2)
    inverse = rope_base ** (-inner.astype(F32) * 2.0 / HEAD)
    angle = position.astype(F32)[:, None] * inverse[None, :]
    live = (inner < HALF)[None, :]
    sign = jnp.where(lane < LANES // 2, -1.0, 1.0)[None, :]
    cosine = jnp.where(live, jnp.cos(angle), 0.0)
    sine = jnp.where(live, sign * jnp.sin(angle), 0.0)
    shape = (n, rows, LANES)
    return cosine.reshape(shape), sine.reshape(shape), segment[:, None], segment[None, :]


def shards(
    inputs,
    cotangent,
    seq_lengths,
    gain_attn,
    w_query,
    w_key,
    w_value,
    w_out,
    gain_ffn,
    w_gate,
    w_up,
    w_down,
):
    section = lax.axis_index("section")
    first = section == 0
    n = lax.axis_size("tensor")
    rows = inputs.shape[1]
    attn_own = (w_query, jnp.swapaxes(w_key, 1, 2), jnp.swapaxes(w_value, 1, 2), w_out)
    ffn_own = (w_gate, w_up, w_down)
    gains = jnp.concatenate([gain_attn, gain_ffn], axis=0)
    gains_other = swap(gains)
    gains_by_layer = [
        jnp.where(first, gains, gains_other).astype(F32),
        jnp.where(first, gains_other, gains).astype(F32),
    ]
    tables = segment_tables(jnp.where(first, seq_lengths[0, 0], seq_lengths[0, 1]), n, rows)

    x = x_saved = inputs
    kept = []
    outs = []
    for layer in range(2):
        gain_a, gain_f = gains_by_layer[layer][0:1], gains_by_layer[layer][1:2]
        if layer == 0:
            h, h_saved, n_all, qkv, o, *swapped = attn_forward(
                layer, n, x, gain_a, tables, attn_own + ffn_own, None, None
            )
            attn_other, ffn_other = tuple(swapped[:4]), tuple(swapped[4:])
        else:
            h, h_saved, n_all, qkv, o, df_ahead = attn_forward(
                layer, n, x, gain_a, tables, attn_own, attn_other, cotangent
            )
        y, y_saved, n2_all, gate, up, hid = ffn_forward(layer, n, h, gain_f, ffn_own, ffn_other)
        kept.append((x_saved, h_saved, n_all, qkv, o, n2_all, gate, up, hid, gain_a, gain_f))
        outs.append(y_saved)
        x, x_saved = y, y_saved

    count = lax.axis_size("dp")
    cube = (2,) + (2,) * (count.bit_length() - 1)

    def weight_grad(left, right):
        left = left.reshape(-1, left.shape[-1])
        right = right.reshape(-1, right.shape[-1])
        return dot_tn(left, right).astype(BF16)

    def blocked(array):
        return array.reshape(*cube, -1, array.shape[-1])

    dy = cotangent
    in_grads = [None, None]
    gain_parts = [None, None]
    for layer in (1, 0):
        x, h, n_all, qkv, o, n2_all, gate, up, hid, gain_a, gain_f = kept[layer]
        if layer == 1:
            g_down = blocked(weight_grad(hid, df_ahead))
            plan = {"reduce": (1, [g_down])}
            dh, gf_part, dmid, sum_down = ffn_backward(
                layer, n, dy, h, gain_f, gate, up, ffn_own, ffn_other, Tasks(count, plan), df_ahead
            )
            g_mid = blocked(weight_grad(n2_all, dmid))
            plan = {"reduce": (1, [g_mid]), "gather": (1, [sum_down])}
        else:
            plan = {"reduce": (1, attn_grad), "gather": (1, [sum_mid])}
            dh, gf_part, df_all, dmid, *sum_attn, mid_full = ffn_backward(
                layer, n, dy, h, gain_f, gate, up, ffn_own, ffn_other, Tasks(count, plan), None
            )
            g_mid, g_down = blocked(weight_grad(n2_all, dmid)), blocked(weight_grad(hid, df_all))
            plan = {"reduce": (0, [g_mid, g_down]), "gather": (1, sum_attn)}
        dx, dx_saved, ga_part, da_all, dqkv, *more = attn_backward(
            layer, n, dh, x, gain_a, tables, qkv, attn_own, attn_other, Tasks(count, plan)
        )
        if layer == 1:
            sum_mid, down_full = more
        else:
            sum_ffn, attn_full = more[:2], more[2:]
        attn_grad = [blocked(weight_grad(dqkv, n_all)), blocked(weight_grad(o, da_all))]
        gain_parts[layer] = [ga_part, gf_part]
        in_grads[layer] = dx_saved
        dy = dx
    gain_sums, section_out, in_grad, g_mid, g_down, g_qkv, g_out = tail(
        n,
        count,
        gain_parts[0] + gain_parts[1],
        outs + in_grads,
        sum_ffn,
        attn_grad,
        [mid_full, down_full],
        attn_full,
    )
    gain_own = jnp.where(first, gain_sums[0:2], gain_sums[2:4])
    g_mid, g_down, g_qkv, g_out = (
        array.reshape(array.shape[0], -1, array.shape[-1])
        for array in (g_mid, g_down, g_qkv, g_out)
    )
    g_gate, g_up, g_down, g_query, g_key, g_value, g_out = (
        grad[None] for grad in widened(g_mid, g_down, g_qkv, g_out, w_query.shape[2], w_key.shape[2])
    )
    g_key, g_value = jnp.swapaxes(g_key, 1, 2), jnp.swapaxes(g_value, 1, 2)
    return (
        section_out[None],
        in_grad[None],
        gain_own[0:1],
        g_query,
        g_key,
        g_value,
        g_out,
        gain_own[1:2],
        g_gate,
        g_up,
        g_down,
    )


def solution(mesh):
    placed = (
        P(None, ("dp", "tensor"), None),
        P(None, ("dp", "tensor"), None),
        P("dp", None, None),
        P("section", None),
        P("section", None, "tensor"),
        P("section", None, "tensor"),
        P("section", None, "tensor"),
        P("section", "tensor", None),
        P("section", None),
        P("section", None, "tensor"),
        P("section", None, "tensor"),
        P("section", "tensor", None),
    )
    return jax.shard_map(
        shards,
        mesh=mesh,
        in_specs=placed,
        out_specs=(
            P("section", None, ("dp", "tensor"), None),
            P("section", None, ("dp", "tensor"), None),
            P("section", None),
            P("section", None, "tensor"),
            P("section", None, "tensor"),
            P("section", None, "tensor"),
            P("section", "tensor", None),
            P("section", None),
            P("section", None, "tensor"),
            P("section", None, "tensor"),
            P("section", "tensor", None),
        ),
        check_vma=False,
    )
```

```python
import functools

import jax
import jax.numpy as jnp
from jax import lax
from jax.experimental import pallas as pl
from jax.experimental.pallas import tpu as pltpu
from jax.sharding import PartitionSpec as P

HEAD = 96
HALF = HEAD // 2
LANES = 128
CHUNKS = 3
BF16 = jnp.bfloat16
F32 = jnp.float32
MESH = pl.DeviceIdType.MESH
VMEM = pltpu.VMEM
VMEM_SPEC = pl.BlockSpec(memory_space=pltpu.VMEM)
LOAD, LOAD_MINE = "load", "load mine"
VMEM_LIMITS = {"attn_fwd0": 61, "tail": 61}
HBM_SPEC = pl.BlockSpec(memory_space=pltpu.HBM)
DMA = pltpu.SemaphoreType.DMA

eps = 1e-05
rope_base = 100000.0
neg_fill = -1e30


def dot_nn(left, right):
    return lax.dot_general(left, right, (((1,), (0,)), ((), ())), preferred_element_type=F32)


def dot_nt(left, right):
    return lax.dot_general(left, right, (((1,), (1,)), ((), ())), preferred_element_type=F32)


def dot_tn(left, right):
    return lax.dot_general(left, right, (((0,), (0,)), ((), ())), preferred_element_type=F32)


def rms_scale(values):
    return lax.rsqrt(jnp.mean(values * values, axis=-1, keepdims=True) + eps)


def norm_back(d_normed, resid, gain):
    scale_rows = rms_scale(resid)
    unit_rows = resid * scale_rows
    gain_part = jnp.sum(d_normed * unit_rows, axis=0, keepdims=True)
    d_unit = d_normed * gain
    inner = jnp.mean(d_unit * unit_rows, axis=-1, keepdims=True)
    return scale_rows * (d_unit - unit_rows * inner), gain_part


class Line:
    def __init__(self, count, full, rbuf, sbuf, gs, gr, ss, sr):
        self.n = count
        self.core = lax.axis_index("section")
        self.me = lax.axis_index("tensor")
        self.full, self.rbuf, self.sbuf = full, rbuf, sbuf
        self.gs, self.gr, self.ss, self.sr = gs, gr, ss, sr
        self.rows = full.shape[1] // CHUNKS

    def span(self, c):
        return pl.ds(pl.multiple_of(c * self.rows, self.rows), self.rows)

    def neighbour(self, d):
        return self.me + 1 if d == 0 else self.me - 1

    def enter(self, also=()):
        me, n = self.me, self.n
        barrier = pltpu.get_barrier_semaphore()
        for peer in ({"section": 1 - self.core}, *also):
            pl.semaphore_signal(barrier, 1, device_id=peer, device_id_type=MESH)
        for d, there in ((1, me > 0), (0, me < n - 1)):

            @pl.when(there)
            def _():
                pl.semaphore_signal(
                    barrier, 1, device_id={"tensor": self.neighbour(d)}, device_id_type=MESH
                )

        peers = 1 + len(also) + (me > 0).astype(jnp.int32) + (me < n - 1).astype(jnp.int32)
        pl.semaphore_wait(barrier, peers)

    def gather_copy(self, d, step, shard, c):
        ref = self.full.at[shard, self.span(c)]
        return pltpu.make_async_remote_copy(
            ref,
            ref,
            self.gs.at[d, step, c],
            self.gr.at[d, step, c],
            device_id={"tensor": self.neighbour(d)},
            device_id_type=MESH,
        )

    def gather_step(self, step):
        me, n = self.me, self.n
        for c in range(CHUNKS):
            for d in range(2):
                shard = me - step if d == 0 else me + step
                holds = (shard >= 0) & (shard < n)
                onward = (me + 1 < n) if d == 0 else (me > 0)

                @pl.when(holds & (step > 0))
                def _():
                    self.gather_copy(d, step - 1, shard, c).wait_recv()

                @pl.when(holds & onward)
                def _():
                    self.gather_copy(d, step, shard, c).start()

    def gather_end(self):
        me, n = self.me, self.n

        @pl.loop(0, n - 1)
        def _(step):
            for c in range(CHUNKS):
                for d in range(2):
                    shard = me - step if d == 0 else me + step
                    onward = (me + 1 < n) if d == 0 else (me > 0)

                    @pl.when((shard >= 0) & (shard < n) & onward)
                    def _():
                        self.gather_copy(d, step, shard, c).wait_send()

    def sum_copy(self, d, shard, c):
        return pltpu.make_async_remote_copy(
            self.sbuf.at[shard, self.span(c)],
            self.rbuf.at[d, shard, self.span(c)],
            self.ss.at[d, shard, c],
            self.sr.at[d, shard, c],
            device_id={"tensor": self.neighbour(d)},
            device_id_type=MESH,
        )

    def sum_step(self, d, shard, partial):
        me, n = self.me, self.n
        goes = (shard > me) & (shard < n) if d == 0 else (shard >= 0) & (shard < me)
        first = (me == 0) if d == 0 else (me == n - 1)

        @pl.when(goes)
        def _():
            @pl.loop(0, CHUNKS)
            def _(c):
                mine = partial[shard, self.span(c)]

                @pl.when(first)
                def _():
                    self.sbuf[shard, self.span(c)] = mine.astype(BF16)

                @pl.when(jnp.logical_not(first))
                def _():
                    self.sum_copy(d, shard, c).wait_recv()
                    arrived = self.rbuf[d, shard, self.span(c)].astype(F32)
                    self.sbuf[shard, self.span(c)] = (mine + arrived).astype(BF16)

                self.sum_copy(d, shard, c).start()

    def sum_take(self, total):
        me, n = self.me, self.n
        for d, there in ((0, me > 0), (1, me < n - 1)):

            @pl.when(there)
            def _():
                @pl.loop(0, CHUNKS)
                def _(c):
                    self.sum_copy(d, me, c).wait_recv()
                    total[self.span(c)] += self.rbuf[d, me, self.span(c)].astype(F32)

    def sum_end(self):
        me, n = self.me, self.n

        @pl.loop(0, n)
        def _(shard):
            for d, goes in ((0, shard > me), (1, shard < me)):

                @pl.when(goes)
                def _():
                    for c in range(CHUNKS):
                        self.sum_copy(d, shard, c).wait_send()


def line_scratch(count, rows, width):
    return [
        VMEM((count, rows, width), BF16),
        VMEM((2, count, rows, width), BF16),
        VMEM((count, rows, width), BF16),
        DMA((2, count, CHUNKS)),
        DMA((2, count, CHUNKS)),
        DMA((2, count, CHUNKS)),
        DMA((2, count, CHUNKS)),
    ]


def rows_then_sums(line, compute, partial, halfway=lambda: None):
    me, n = line.me, line.n

    @pl.loop(0, 2 * n - 1)
    def _(step):
        @pl.when((step > 0) & (step < n))
        def _():
            line.gather_step(step)

        @pl.when(step == n - 1)
        def _():
            halfway()

        @pl.when(step < n)
        def _():
            @pl.loop(0, 2)
            def _(side):
                shard = jnp.where(side == 0, me - step, me + step)

                @pl.when((shard >= 0) & (shard < n) & ((step > 0) | (side == 0)))
                def _():
                    compute(shard)

        line.sum_step(0, step - me, partial)
        line.sum_step(1, 2 * (n - 1) - step - me, partial)


def later_shards(line, compute):
    me, n = line.me, line.n

    @pl.loop(0, n)
    def _(step):
        @pl.when(step > 0)
        def _():
            line.gather_step(step)

        @pl.loop(0, 2)
        def _(side):
            shard = jnp.where(side == 0, me - step, me + step)

            @pl.when((shard >= 0) & (shard < n) & ((step > 0) | (side == 0)))
            def _():
                compute(shard)


def sums_alone(line, compute, partial, each):
    me, n = line.me, line.n

    @pl.loop(0, n)
    def _(step):
        @pl.loop(0, 2)
        def _(side):
            shard = jnp.where(side == 0, me + n - 1 - step, step - (n - 1 - me))
            first = jnp.where(side == 0, me, 0)
            last = jnp.where(side == 0, n, me)

            @pl.when((shard >= first) & (shard < last))
            def _():
                compute(shard)

        line.sum_step(0, me + n - 1 - step, partial)
        line.sum_step(1, step - (n - 1 - me), partial)
        each(step)


class Weights:
    def __init__(self, layer, sems):
        self.own = lax.axis_index("section") == layer
        self.sems = sems
        self.wanted = []

    def want(self, mine, theirs, target):
        self.wanted.append((mine, theirs, target))

    def start_own(self):
        @pl.when(self.own)
        def _():
            for index, (mine, _theirs, target) in enumerate(self.wanted):
                pltpu.make_async_copy(mine, target, self.sems.at[index]).start()

    def start_other(self, before=lambda: None):
        @pl.when(jnp.logical_not(self.own))
        def _():
            before()
            for index, (_mine, theirs, target) in enumerate(self.wanted):
                pltpu.make_async_copy(theirs, target, self.sems.at[index]).start()

    def start(self):
        self.start_own()
        self.start_other()

    def wait(self):
        for index, (mine, _theirs, target) in enumerate(self.wanted):
            pltpu.make_async_copy(mine, target, self.sems.at[index]).wait()


class Pair:
    def __init__(self, local_sems, send_sems, recv_sems):
        self.core = lax.axis_index("section")
        self.sems = local_sems, send_sems, recv_sems
        self.kept, self.sent = [], []
        self.streams = []

    def keep(self, source, target):
        copy = pltpu.make_async_copy(source, target, self.sems[0].at[len(self.kept), 0])
        copy.start()
        self.kept.append(copy)

    def copy(self, source, target, index, part=0):
        return pltpu.make_async_remote_copy(
            source,
            target,
            self.sems[1].at[index, part],
            self.sems[2].at[index, part],
            device_id={"section": 1 - self.core},
            device_id_type=MESH,
        )

    def send(self, source, target):
        copy = self.copy(source, target, len(self.sent))
        copy.start()
        self.sent.append(copy)

    def share_half(self, halves, pair):
        self.keep(halves.at[self.core], pair.at[0])
        self.send(halves.at[1 - self.core], pair.at[1])

    def stream_keep(self, source, target):
        self.streams.append((source, target, len(self.kept), None))
        self.kept.append(None)

    def stream_share(self, source, pair):
        self.stream_keep(source, pair.at[0])
        self.streams.append((source, pair.at[1], None, len(self.sent)))
        self.sent.append(None)

    def stream_share_half(self, halves, pair):
        self.stream_keep(halves.at[self.core], pair.at[0])
        self.streams.append((halves.at[1 - self.core], pair.at[1], None, len(self.sent)))
        self.sent.append(None)

    def streamed(self, shard):
        copies = []
        for source, target, kept, sent in self.streams:
            pieces = source.at[shard], target.at[shard]
            if sent is None:
                copies.append(pltpu.make_async_copy(*pieces, self.sems[0].at[kept, shard]))
            else:
                copies.append(self.copy(*pieces, sent, shard))
        return copies

    def stream(self, shard):
        for copy in self.streamed(shard):
            copy.start()

    def wait(self, count=0):
        for copy in self.kept + self.sent:
            if copy is not None:
                copy.wait()
        if self.streams:

            @pl.loop(0, count)
            def _(shard):
                for copy in self.streamed(shard):
                    copy.wait()


def pair_scratch(count, kept, sent):
    return [DMA((max(kept, 1), count)), DMA((max(sent, 1), count)), DMA((max(sent, 1), count))]


class Cube:
    def __init__(self, layer, count):
        self.bits = count.bit_length() - 1
        assert count == 1 << self.bits
        self.me = lax.axis_index("dp")
        self.core = lax.axis_index("section")
        self.active = self.core == layer
        self.bit = [(self.me // (1 << b)) % 2 for b in range(self.bits)]
        self.down = list(range(self.bits - 1, -1, -1))

    def order(self, colour):
        return list(range(self.bits)) if colour == 0 else self.down

    def peer(self, b):
        return {"dp": self.me + (1 - 2 * self.bit[b]) * (1 << b)}

    def peers(self):
        return [self.peer(b) for b in range(self.bits)]


class Reduce(Cube):
    def __init__(self, layer, count, sources, outs, scratch):
        super().__init__(layer, count)
        self.sources, self.outs = sources, outs
        size = len(sources)
        self.accs = scratch[:size]
        self.recvs = [scratch[size * (t + 1) : size * (t + 2)] for t in range(self.bits)]
        self.local, self.ss, self.sr, self.fs = scratch[size * (self.bits + 1) :]
        self.t = 0
        self.place = [
            {b: slice(None) for b in self.down if b != self.order(c)[0]} for c in range(2)
        ]

    def items(self):
        return [(a, c) for a in range(len(self.sources)) for c in range(2)]

    def spot(self, c, changed=()):
        place = {**self.place[c], **dict(changed)}
        return (c, *(place[b] for b in self.down if b in place))

    def first_half(self, a, c, value):
        b = self.order(c)[0]
        index = [slice(None)] * self.bits
        index[self.down.index(b)] = value
        return self.sources[a].at[(c, *index)]

    def copy(self, a, c, t, source):
        return pltpu.make_async_remote_copy(
            source,
            self.recvs[t][a].at[c],
            self.ss.at[a, c, t],
            self.sr.at[a, c, t],
            device_id=self.peer(self.order(c)[t]),
            device_id_type=MESH,
        )

    def kept(self, a, c):
        mine = self.first_half(a, c, self.bit[self.order(c)[0]])
        return pltpu.make_async_copy(mine, self.accs[a].at[c], self.local.at[a, c])

    def start(self):
        for a, c in self.items():
            other = self.first_half(a, c, 1 - self.bit[self.order(c)[0]])
            self.copy(a, c, 0, other).start()
            self.kept(a, c).start()

    def advance(self):
        t = self.t
        if t >= self.bits:
            return
        for a, c in self.items():
            if t == 0:
                self.kept(a, c).wait()
            self.copy(a, c, t, self.recvs[t][a].at[c]).wait_recv()
            acc, spot = self.accs[a], self.spot(c)
            self.add(acc, spot, self.recvs[t][a], c)
            if t + 1 < self.bits:
                b = self.order(c)[t + 1]
                self.copy(a, c, t + 1, acc.at[self.spot(c, [(b, 1 - self.bit[b])])]).start()
        if t + 1 < self.bits:
            for c in range(2):
                b = self.order(c)[t + 1]
                self.place[c][b] = self.bit[b]
        self.t = t + 1

    def add(self, acc, spot, arrived, c):
        rows = acc.shape[-2]
        step = 32 if rows % 32 == 0 else rows

        @pl.loop(0, rows // step)
        def _(block):
            part = pl.ds(pl.multiple_of(block * step, step), step)
            free = (slice(None),) * (len(arrived.shape) - 3)
            total = acc[(*spot, part)].astype(F32) + arrived[(c, *free, part)].astype(F32)
            acc[(*spot, part)] = total.astype(BF16)

    def put_away(self, a, c):
        return pltpu.make_async_copy(
            self.accs[a].at[self.spot(c)], self.outs[a].at[c], self.fs.at[a, c]
        )

    def finish(self):
        while self.t < self.bits:
            self.advance()
        for a, c in self.items():
            self.put_away(a, c).start()
        for a, c in self.items():
            for t in range(self.bits):
                self.copy(a, c, t, self.recvs[t][a].at[c]).wait_send()
        for a, c in self.items():
            self.put_away(a, c).wait()


class Gather(Cube):
    def __init__(self, layer, count, blocks, outs, sems):
        super().__init__(layer, count)
        self.blocks, self.outs = blocks, outs
        self.keep, self.ss, self.sr, self.hs, self.hr = sems
        self.t = 0
        off_layer = 1 - self.core if layer == 1 else self.core
        self.slot = self.core * (1 - off_layer) + 2 * off_layer

    def items(self):
        return [(a, c) for a in range(len(self.blocks)) for c in range(2)]

    def order(self, colour):
        return super().order(colour)[::-1]

    def region(self, a, c, t, half, flipped=None):
        order = self.order(c)
        index = []
        for b in self.down:
            if b in order[:t]:
                index.append(slice(None))
            else:
                index.append(1 - self.bit[b] if flipped == order.index(b) else self.bit[b])
        return self.outs[a].at[(half, c, *index)]

    def copy(self, a, c, t):
        target = self.region(a, c, t, self.slot)
        return pltpu.make_async_remote_copy(
            self.blocks[a].at[c] if t == 0 else target,
            target,
            self.ss.at[a, c, t],
            self.sr.at[a, c, t],
            device_id=self.peer(self.order(c)[t]),
            device_id_type=MESH,
        )

    def kept(self, a, c):
        return pltpu.make_async_copy(
            self.blocks[a].at[c], self.region(a, c, 0, self.slot), self.keep.at[a, c]
        )

    def hand_over(self, a, c, t):
        if t == 0:
            source, target = self.blocks[a].at[c], self.region(a, c, 0, self.core)
        else:
            source = self.region(a, c, t - 1, self.slot, t - 1)
            target = self.region(a, c, t - 1, self.core, t - 1)
        return pltpu.make_async_remote_copy(
            source,
            target,
            self.hs.at[a, c, t],
            self.hr.at[a, c, t],
            device_id={"section": 1 - self.core},
            device_id_type=MESH,
        )

    def pass_on(self, t):
        @pl.when(jnp.logical_not(self.active))
        def _():
            for a, c in self.items():
                self.hand_over(a, c, t).start()

    def start(self):
        for a, c in self.items():
            self.copy(a, c, 0).start()
            self.kept(a, c).start()
        self.pass_on(0)

    def advance(self):
        t = self.t
        if t >= self.bits:
            return
        for a, c in self.items():
            if t == 0:
                self.kept(a, c).wait()
            self.copy(a, c, t).wait_recv()
            if t + 1 < self.bits:
                self.copy(a, c, t + 1).start()
        self.pass_on(t + 1)
        self.t = t + 1

    def finish(self):
        while self.t < self.bits:
            self.advance()
        for a, c in self.items():
            for t in range(self.bits):
                self.copy(a, c, t).wait_send()

        @pl.when(self.active)
        def _():
            for a, c in self.items():
                for t in range(self.bits + 1):
                    self.hand_over(a, c, t).wait_recv()

        @pl.when(jnp.logical_not(self.active))
        def _():
            for a, c in self.items():
                for t in range(self.bits + 1):
                    self.hand_over(a, c, t).wait_send()


def reduce_scratch(count, arrays):
    bits = count.bit_length() - 1
    scratch = []
    for level in (1, *range(1, bits + 1)):
        scratch += [VMEM((2,) + (2,) * (bits - level) + shape[-2:], BF16) for shape in arrays]
    size = len(arrays)
    return scratch + [
        DMA((size, 2)),
        DMA((size, 2, bits)),
        DMA((size, 2, bits)),
        DMA((size, 2)),
    ]


def gather_sems(count, size):
    bits = count.bit_length() - 1
    return [
        DMA((size, 2)),
        DMA((size, 2, bits)),
        DMA((size, 2, bits)),
        DMA((size, 2, bits + 1)),
        DMA((size, 2, bits + 1)),
    ]


class Tasks:
    def __init__(self, count, plan):
        self.count = count
        self.reduce = plan.get("reduce")
        self.gather = plan.get("gather")

    def arguments(self):
        args = list(self.reduce[1]) if self.reduce else []
        return args + (list(self.gather[1]) if self.gather else [])

    def outputs(self):
        outs = []
        if self.reduce:
            outs += [((2,) + ref.shape[-2:], BF16, HBM_SPEC) for ref in self.reduce[1]]
        if self.gather:
            middle = (2,) * (self.count.bit_length() - 1)
            outs += [
                ((3, 2) + middle + ref.shape[-2:], BF16, HBM_SPEC) for ref in self.gather[1]
            ]
        return outs

    def scratch(self):
        scratch = []
        if self.reduce:
            scratch += reduce_scratch(self.count, [ref.shape for ref in self.reduce[1]])
        if self.gather:
            scratch += [VMEM(ref.shape, BF16) for ref in self.gather[1]]
            scratch += [DMA((len(self.gather[1]),))]
            scratch += gather_sems(self.count, len(self.gather[1]))
        return scratch

    def bind(self, args, outs, scratch):
        self.running = []
        self.loads = []
        count = self.count
        if self.reduce:
            size = len(self.reduce[1])
            used = len(reduce_scratch(count, [ref.shape for ref in self.reduce[1]]))
            self.running.append(
                Reduce(self.reduce[0], count, args[:size], outs[:size], scratch[:used])
            )
            args, outs, scratch = args[size:], outs[size:], scratch[used:]
        if self.gather:
            size = len(self.gather[1])
            blocks = scratch[:size]
            self.loads = [
                pltpu.make_async_copy(args[a], blocks[a], scratch[size].at[a]) for a in range(size)
            ]
            self.running.append(
                Gather(self.gather[0], count, blocks, outs, scratch[size + 1 : size + 6])
            )
        for load in self.loads:
            load.start()

    def peers(self):
        return self.running[0].peers() if self.running else []

    def start(self):
        for load in self.loads:
            load.wait()
        for task in self.running:
            task.start()

    def advance(self):
        for task in self.running:
            task.advance()

    def finish(self):
        for task in self.running:
            task.finish()


def pick_split(columns):
    heads = columns // HEAD
    col = lax.broadcasted_iota(jnp.int32, (columns, heads * LANES), 1)
    row = lax.broadcasted_iota(jnp.int32, (columns, heads * LANES), 0)
    inner = col & 63
    source = (col >> 7) * HEAD + ((col >> 6) & 1) * HALF + inner
    return ((row == source) & (inner < HALF)).astype(F32).astype(BF16)


def pick_plain(columns):
    heads = columns // HEAD
    col = lax.broadcasted_iota(jnp.int32, (columns, heads * LANES), 1)
    row = lax.broadcasted_iota(jnp.int32, (columns, heads * LANES), 0)
    inner = col & 127
    return ((row == (col >> 7) * HEAD + inner) & (inner < HEAD)).astype(F32).astype(BF16)


def rotated(values, cosine, sine):
    return values * cosine + pltpu.roll(values, LANES // 2, 1) * sine


def spread_qkv(wq, wk, wv, wqkv):
    small = wk.shape[0]
    q_wide = wq.shape[1] // HEAD * LANES
    k_wide = small // HEAD * LANES
    pick_q, pick_k, pick_v = pick_split(wq.shape[1]), pick_split(small), pick_plain(small)
    size = 2 * LANES

    @pl.loop(0, wq.shape[0] // size)
    def _(block):
        rows = pl.ds(pl.multiple_of(block * size, size), size)
        wqkv[rows, :q_wide] = dot_nn(wq[rows], pick_q).astype(BF16)
        wqkv[rows, q_wide : q_wide + k_wide] = dot_tn(wk[:, rows], pick_k).astype(BF16)
        wqkv[rows, q_wide + k_wide :] = dot_tn(wv[:, rows], pick_v).astype(BF16)


def allowed_pairs(seg_col, seg_row):
    full_rows = seg_col.shape[0]
    row = lax.broadcasted_iota(jnp.int32, (full_rows, full_rows), 0)
    col = lax.broadcasted_iota(jnp.int32, (full_rows, full_rows), 1)
    return (seg_col[...] == seg_row[...]) & (col <= row)


def lane_block(index):
    return pl.ds(pl.multiple_of(index * LANES, LANES), LANES)


def head_rows(ref, index):
    return ref[:, :, lane_block(index)].reshape(-1, LANES)


def attn_weights(weights, wo, sources):
    wq0, wq1, wk0, wk1, wv0, wv1, wo0, wo1 = sources[:8]
    wq, wk, wv = sources[8:]
    weights.want(wq0.at[0], wq1.at[0], wq)
    weights.want(wk0.at[0], wk1.at[0], wk)
    weights.want(wv0.at[0], wv1.at[0], wv)
    for h in range(wo.shape[0]):
        rows = pl.ds(h * HEAD, HEAD)
        weights.want(wo0.at[0, rows], wo1.at[0, rows], wo.at[h, pl.ds(0, HEAD)])


def clear_pads(wo):
    for h in range(wo.shape[0]):
        wo[h, HEAD:] = jnp.zeros((LANES - HEAD, wo.shape[2]), BF16)


def probabilities(queries, keys, allowed):
    scores = jnp.where(allowed, dot_nt(queries, keys) * HEAD ** (-0.5), neg_fill)
    exp_scores = jnp.exp(scores - jnp.max(scores, axis=-1, keepdims=True))
    return exp_scores / jnp.sum(exp_scores, axis=-1, keepdims=True)


def attn_fwd_kernel(layer, n, heads, kv_heads, others, loads_done, *refs):
    ahead = layer == 1
    x, gain, cos, sin, seg_col, seg_row = refs[:6]
    at = 6
    if ahead:
        rows_ahead = refs[at]
        at += 1
    own = refs[at : at + others]
    at += others
    if layer == 0:
        h_out, h_save, n_out, qkv_out, o_out = refs[at : at + 5]
        other = refs[at + 5 : at + 5 + others]
    else:
        other = refs[at : at + others]
        h_out, h_save, n_out, qkv_out, o_out, ahead_out = refs[at + others : at + others + 6]
        at += 1
    at += 5 + others
    (wq, wk, wv, wo, wqkv, qkv, o, osmall, part, wsem) = refs[at : at + 10]
    pair = Pair(*refs[at + 10 : at + 13])
    at += 13
    if ahead:
        second = Line(n, refs[at], None, None, *refs[at + 1 : at + 3], None, None)
        passed = Pair(*refs[at + 3 : at + 6])
        passed.stream_share(second.full, ahead_out)
        at += 6
    line = Line(n, *refs[at:])
    me = line.me
    group = heads // kv_heads
    weights = Weights(layer, wsem)
    sources = [ref for both in zip(own[:4], other[:4]) for ref in both] + [wq, wk, wv]
    attn_weights(weights, wo, sources)
    if layer == 0:
        weights.start_own()
    else:
        weights.start()
    loads_done()
    resid = x[...].astype(F32)
    line.full[me] = (resid * rms_scale(resid) * gain[...]).astype(BF16)
    clear_pads(wo)
    if ahead:
        second.full[me] = rows_ahead[...]
    if layer == 0:
        line.enter()
        line.gather_step(0)
        for mine, theirs in zip(own, other):
            pair.send(mine, theirs)

        def arrived():
            for index in range(4):
                pair.copy(own[index], other[index], index).wait_recv()

        weights.start_other(arrived)
    else:
        line.enter()
        line.gather_step(0)
    weights.wait()
    spread_qkv(wq, wk, wv, wqkv)

    def compute(shard):
        products = dot_nn(line.full[shard], wqkv[...])
        for head in range(heads + kv_heads):
            lanes = slice(head * LANES, (head + 1) * LANES)
            qkv[shard, :, lanes] = rotated(products[:, lanes], cos[shard], sin[shard]).astype(BF16)
        lanes = slice((heads + kv_heads) * LANES, None)
        qkv[shard, :, lanes] = products[:, lanes].astype(BF16)
        pair.stream(shard)

    pair.stream_share(line.full, n_out)
    pair.stream_keep(qkv, qkv_out)
    later_shards(line, compute)
    if ahead:
        second.gather_step(0)
        passed.stream(me)
    allowed = allowed_pairs(seg_col, seg_row)

    @pl.loop(0, kv_heads)
    def _(g):
        keys = head_rows(qkv, heads + g)
        values = head_rows(qkv, heads + kv_heads + g)

        @pl.loop(0, group)
        def _(member):
            h = g * group + member
            probs = probabilities(head_rows(qkv, h), keys, allowed)
            attended = dot_nn(probs.astype(BF16), values).astype(BF16)
            o[:, :, lane_block(h)] = attended.reshape(n, -1, LANES)

        wide_heads = [head_rows(o, g * group + member) for member in range(group)]
        small = dot_nt(jnp.concatenate(wide_heads, axis=1), pick_plain(group * HEAD))
        osmall[g] = small.astype(BF16).reshape(osmall.shape[1:])

    pair.share_half(osmall, o_out)
    wide = wo.shape[0] * LANES

    def project(shard):
        part[shard] = dot_nn(o[shard], wo[...].reshape(wide, -1))

    if ahead:

        def each(step):
            @pl.when(step < n - 1)
            def _():
                second.gather_step(step + 1)

                @pl.loop(0, 2)
                def _(side):
                    shard = jnp.where(side == 0, me - step - 1, me + step + 1)

                    @pl.when((shard >= 0) & (shard < n))
                    def _():
                        passed.stream(shard)

        sums_alone(line, project, part, each)
    else:
        sums_alone(line, project, part, lambda step: None)
    h_out[...] = x[...].astype(F32) + part[me]
    line.sum_take(h_out)
    pair.keep(h_out, h_save)
    if ahead:
        second.gather_end()
        passed.wait(n)
    line.gather_end()
    line.sum_end()
    if layer == 0:
        for index, copy in enumerate(pair.sent[:others]):
            copy.wait_send()
            if index >= 4:
                copy.wait_recv()

        @pl.when(weights.own)
        def _():
            for index in range(4):
                pair.copy(own[index], other[index], index).wait_recv()

        pair.sent[:others] = [None] * others
    pair.wait(n)


def bound(tasks, sizes, refs):
    groups, at = [], 0
    for own, extra in sizes:
        groups.append((refs[at : at + own], refs[at + own : at + own + extra]))
        at += own + extra
    tasks.bind(*(list(extra) for _, extra in groups))
    return [ref for own, _ in groups for ref in own]


def attn_bwd_kernel(layer, n, heads, kv_heads, tasks, sizes, loads_done, *refs):
    refs = bound(tasks, sizes, refs)
    (dh, x, gain, cos, sin, seg_col, seg_row, qkv_in) = refs[:8]
    own, other = refs[8:12], refs[12:16]
    (dx_out, dx_save, gain_out, da_out, dqkv_out) = refs[16:21]
    (wq, wk, wv, wo, wqkv, qkv, d_o, dqkv, dsmall, part, dkv, wsem, tsem) = refs[21:34]
    pair = Pair(*refs[34:37])
    line = Line(n, *refs[37:])
    me = line.me
    group = heads // kv_heads
    weights = Weights(layer, wsem)
    sources = [ref for both in zip(own, other) for ref in both] + [wq, wk, wv]
    attn_weights(weights, wo, sources)
    weights.start()
    take = pltpu.make_async_copy(qkv_in, qkv, tsem)
    take.start()
    line.full[me] = dh[...].astype(BF16)
    clear_pads(wo)
    line.enter(tasks.peers())
    line.gather_step(0)
    tasks.start()
    loads_done()
    weights.wait()
    spread_qkv(wq, wk, wv, wqkv)
    take.wait()
    wide = wo.shape[0] * LANES

    def compute(shard):
        d_o[shard] = dot_nt(line.full[shard], wo[...].reshape(wide, -1)).astype(BF16)
        pair.stream(shard)

    pair.stream_share(line.full, da_out)
    later_shards(line, compute)
    allowed = allowed_pairs(seg_col, seg_row)
    cosine = cos[...].reshape(-1, LANES)
    sine = -sin[...].reshape(-1, LANES)
    scale = HEAD ** (-0.5)

    @pl.loop(0, kv_heads)
    def _(g):
        keys = head_rows(qkv, heads + g)
        values = head_rows(qkv, heads + kv_heads + g)
        dkv[...] = jnp.zeros_like(dkv)

        @pl.loop(0, group)
        def _(member):
            h = g * group + member
            queries = head_rows(qkv, h)
            d_out = head_rows(d_o, h)
            probs = probabilities(queries, keys, allowed)
            d_probs = dot_nt(d_out, values)
            inner = jnp.sum(probs * d_probs, axis=-1, keepdims=True)
            d_scores = (probs * (d_probs - inner)).astype(BF16)
            d_queries = dot_nn(d_scores, keys) * scale
            turned = rotated(d_queries, cosine, sine).astype(BF16)
            dqkv[:, :, lane_block(h)] = turned.reshape(n, -1, LANES)
            dkv[0] += dot_tn(d_scores, queries)
            dkv[1] += dot_tn(probs.astype(BF16), d_out)

        low_keys = rotated(dkv[0] * scale, cosine, sine).astype(BF16)
        low_values = dkv[1].astype(BF16)
        dqkv[:, :, lane_block(heads + g)] = low_keys.reshape(n, -1, LANES)
        dqkv[:, :, lane_block(heads + kv_heads + g)] = low_values.reshape(n, -1, LANES)
        wide_heads = [head_rows(dqkv, g * group + member) for member in range(group)] + [low_keys]
        small = dot_nt(jnp.concatenate(wide_heads, axis=1), pick_split((group + 1) * HEAD))
        small_values = dot_nt(low_values, pick_plain(HEAD))
        dsmall[g] = (
            jnp.concatenate([small, small_values], axis=1).astype(BF16).reshape(dsmall.shape[1:])
        )

    pair.share_half(dsmall, dqkv_out)

    def project(shard):
        part[shard] = dot_nt(dqkv[shard], wqkv[...])

    sums_alone(line, project, part, lambda step: pl.when(step == 0)(tasks.advance))
    line.sum_take(part.at[me])
    d_resid, gain_part = norm_back(part[me], x[...].astype(F32), gain[...])
    dx_out[...] = (dh[...] + d_resid).astype(BF16)
    gain_out[...] = gain_part
    pair.keep(dx_out, dx_save)
    line.gather_end()
    line.sum_end()
    pair.wait(n)
    tasks.finish()


def ffn_fwd_kernel(layer, n, loads_done, *refs):
    (h, gain, wg0, wg1, wu0, wu1, wd0, wd1) = refs[:8]
    (y_out, y_save, n_out, gate_out, up_out, hid_out) = refs[8:14]
    (wg, wu, wd, gate, up, hid, part, wsem) = refs[14:22]
    pair = Pair(*refs[22:25])
    line = Line(n, *refs[25:])
    me = line.me
    weights = Weights(layer, wsem)
    weights.want(wg0.at[0], wg1.at[0], wg)
    weights.want(wu0.at[0], wu1.at[0], wu)
    weights.want(wd0.at[0], wd1.at[0], wd)
    weights.start()
    loads_done()
    resid = h[...]
    line.full[me] = (resid * rms_scale(resid) * gain[...]).astype(BF16)
    line.enter()
    line.gather_step(0)
    weights.wait()
    middle = hid.shape[3]

    def compute(shard):
        part[shard] = jnp.zeros(part.shape[1:], F32)

        @pl.loop(0, 2)
        def _(core):
            lanes = pl.ds(pl.multiple_of(core * middle, middle), middle)
            rows = line.full[shard]
            g = dot_nn(rows, wg[:, lanes])
            u = dot_nn(rows, wu[:, lanes])
            gate[shard, :, lanes] = g
            up[shard, :, lanes] = u
            low = (g * jax.nn.sigmoid(g) * u).astype(BF16)
            hid[core, shard] = low
            part[shard] += dot_nn(low, wd[lanes])

        pair.stream(shard)

    pair.stream_share(line.full, n_out)
    pair.stream_share_half(hid, hid_out)
    pair.stream_keep(gate, gate_out)
    pair.stream_keep(up, up_out)
    rows_then_sums(line, compute, part)
    part[me] += h[...]
    line.sum_take(part.at[me])
    y_out[...] = part[me].astype(BF16)
    pair.keep(y_out, y_save)
    line.gather_end()
    line.sum_end()
    pair.wait(n)


def ffn_bwd_kernel(layer, n, tasks, sizes, loads_done, *refs):
    refs = bound(tasks, sizes, refs)
    gathered = layer == 1
    (dy, h, gain, gate_in, up_in, wg0, wg1, wu0, wu1, wd0, wd1) = refs[:11]
    if gathered:
        (df_all, dh_out, gain_out, dmid_out) = refs[11:15]
    else:
        (dh_out, gain_out, df_all, dmid_out) = refs[11:15]
    (wg, wu, wd, gate, up, dmid, part, wsem, tsem) = refs[15:24]
    pair = Pair(*refs[24:27])
    line = Line(n, *refs[27:])
    me = line.me
    weights = Weights(layer, wsem)
    weights.want(wd0.at[0], wd1.at[0], wd)
    weights.want(wg0.at[0], wg1.at[0], wg)
    weights.want(wu0.at[0], wu1.at[0], wu)
    weights.start()
    takes = [
        pltpu.make_async_copy(gate_in, gate, tsem.at[0]),
        pltpu.make_async_copy(up_in, up, tsem.at[1]),
    ]
    if gathered:
        takes.append(pltpu.make_async_copy(df_all.at[0], line.full, tsem.at[2]))
    for take in takes:
        take.start()
    loads_done()
    if gathered:
        line.enter(tasks.peers())
    else:
        line.full[me] = dy[...]
        line.enter(tasks.peers())
        line.gather_step(0)
    tasks.start()
    weights.wait()
    for take in takes:
        take.wait()
    middle = dmid.shape[3] // 2

    def compute(shard):
        part[shard] = jnp.zeros(part.shape[1:], F32)

        @pl.loop(0, 2)
        def _(core):
            lanes = pl.ds(pl.multiple_of(core * middle, middle), middle)
            d_hidden = dot_nt(line.full[shard], wd[lanes])
            g = gate[shard, :, lanes]
            sig = jax.nn.sigmoid(g)
            d_g = (d_hidden * up[shard, :, lanes] * sig * (1.0 + g * (1.0 - sig))).astype(BF16)
            d_u = (d_hidden * g * sig).astype(BF16)
            dmid[core, shard, :, :middle] = d_g
            dmid[core, shard, :, middle:] = d_u
            part[shard] += dot_nt(d_g, wg[:, lanes]) + dot_nt(d_u, wu[:, lanes])

        pair.stream(shard)

    pair.stream_share_half(dmid, dmid_out)
    if gathered:
        sums_alone(line, compute, part, lambda step: pl.when(step == n - 2)(tasks.advance))
    else:
        pair.stream_share(line.full, df_all)
        rows_then_sums(line, compute, part, tasks.advance)
    line.sum_take(part.at[me])
    d_resid, gain_part = norm_back(part[me], h[...], gain[...])
    dh_out[...] = dy[...].astype(F32) + d_resid
    gain_out[...] = gain_part
    if not gathered:
        line.gather_end()
    line.sum_end()
    pair.wait(n)
    tasks.finish()


def run_kernel(body, args, in_specs, outs, scratch, cid, flops, nbytes, name, aliases=None):
    loaded = [index for index, spec in enumerate(in_specs) if spec in (LOAD, LOAD_MINE)]
    buffers = [
        VMEM(args[index].shape[1:] if in_specs[index] == LOAD_MINE else args[index].shape, args[index].dtype)
        for index in loaded
    ]
    inputs, results, own = len(args), len(outs), len(scratch)

    def kernel(*refs):
        places = list(refs[: inputs + results + own])
        extra = refs[inputs + results + own :]
        copies = []
        for number, index in enumerate(loaded):
            source = refs[index]
            if in_specs[index] == LOAD_MINE:
                source = source.at[lax.axis_index("section")]
            copies.append(pltpu.make_async_copy(source, extra[number], extra[-1].at[number]))
            places[index] = extra[number]
        for copy in copies:
            copy.start()

        def loads_done():
            for copy in copies:
                copy.wait()

        body(loads_done, *places)

    return pl.pallas_call(
        kernel,
        name=name,
        in_specs=[HBM_SPEC if spec in (LOAD, LOAD_MINE) else spec for spec in in_specs],
        out_shape=[jax.ShapeDtypeStruct(shape, dtype) for shape, dtype, _ in outs],
        out_specs=[spec for _, _, spec in outs],
        scratch_shapes=[*scratch, *buffers, DMA((max(len(loaded), 1),))],
        input_output_aliases=aliases or {},
        cost_estimate=pl.CostEstimate(flops=flops, bytes_accessed=nbytes, transcendentals=0),
        compiler_params=pltpu.CompilerParams(
            collective_id=cid, has_side_effects=True, vmem_limit_bytes=VMEM_LIMITS.get(name, 44) << 20
        ),
    )(*args)


def attn_forward(layer, n, x, gain, tables, own, other, rows_ahead):
    rows, width = x.shape[-2:]
    heads = own[0].shape[2] // HEAD
    kv_heads = own[1].shape[1] // HEAD
    wide = (heads + 2 * kv_heads) * LANES
    small = heads // kv_heads * HEAD
    args = [x, gain, *tables]
    specs = [LOAD_MINE] + [VMEM_SPEC] * 5 if layer == 0 else [VMEM_SPEC] + [LOAD] * 5
    if layer == 1:
        args.append(rows_ahead)
        specs.append(LOAD_MINE)
    args += own
    specs += [HBM_SPEC] * len(own)
    outs = [
        ((rows, width), F32, VMEM_SPEC),
        ((rows, width), F32, HBM_SPEC),
        ((2, n, rows, width), BF16, HBM_SPEC),
        ((n, rows, wide), BF16, HBM_SPEC),
        ((2, n, rows, small), BF16, HBM_SPEC),
    ]
    if other is None:
        outs += [(weight.shape, weight.dtype, HBM_SPEC) for weight in own]
    else:
        args += [*other]
        specs += [HBM_SPEC] * len(other)
        outs.append(((2, n, rows, width), BF16, HBM_SPEC))
    scratch = (
        [
            VMEM((width, heads * HEAD), BF16),
            VMEM((kv_heads * HEAD, width), BF16),
            VMEM((kv_heads * HEAD, width), BF16),
            VMEM((heads, LANES, width), BF16),
            VMEM((width, wide), BF16),
            VMEM((n, rows, wide), BF16),
            VMEM((n, rows, heads * LANES), BF16),
            VMEM((kv_heads, n, rows, small), BF16),
            VMEM((n, rows, width), F32),
            DMA((3 + heads,)),
        ]
        + pair_scratch(n, 5, 3 + (len(own) if other is None else 0))
        + (
            [VMEM((n, rows, width), BF16)] + [DMA((2, n, CHUNKS))] * 2 + pair_scratch(n, 1, 1)
            if layer == 1
            else []
        )
        + line_scratch(n, rows, width)
    )
    body = functools.partial(attn_fwd_kernel, layer, n, heads, kv_heads, len(own))
    flops = 2 * n * rows * width * wide * 3 // 2
    return run_kernel(body, args, specs, outs, scratch, 1 + layer, flops, 8 << 20, f"attn_fwd{layer}")


def attn_backward(layer, n, dh, x, gain, tables, qkv, own, other, tasks):
    rows, width = dh.shape
    heads = own[0].shape[2] // HEAD
    kv_heads = own[1].shape[1] // HEAD
    wide = (heads + 2 * kv_heads) * LANES
    small = (heads // kv_heads + 2) * HEAD
    args = [dh, x, gain, *tables, qkv, *own, *other]
    specs = [VMEM_SPEC, LOAD_MINE if x.ndim == 3 else LOAD] + [LOAD] * 5 + [HBM_SPEC] * 9
    outs = [
        ((rows, width), BF16, VMEM_SPEC),
        ((rows, width), BF16, HBM_SPEC),
        ((1, width), F32, VMEM_SPEC),
        ((2, n, rows, width), BF16, HBM_SPEC),
        ((2, n, rows, small), BF16, HBM_SPEC),
    ]
    scratch = (
        [
            VMEM((width, heads * HEAD), BF16),
            VMEM((kv_heads * HEAD, width), BF16),
            VMEM((kv_heads * HEAD, width), BF16),
            VMEM((heads, LANES, width), BF16),
            VMEM((width, wide), BF16),
            VMEM((n, rows, wide), BF16),
            VMEM((n, rows, heads * LANES), BF16),
            VMEM((n, rows, wide), BF16),
            VMEM((kv_heads, n, rows, small), BF16),
            VMEM((n, rows, width), F32),
            VMEM((2, n * rows, LANES), F32),
            DMA((3 + heads,)),
            DMA,
        ]
        + pair_scratch(n, 3, 2)
        + line_scratch(n, rows, width)
    )
    body = functools.partial(attn_bwd_kernel, layer, n, heads, kv_heads)
    flops = 2 * n * rows * width * wide * 2
    return run_with_tasks(
        body, tasks, args, specs, outs, scratch, 3 + layer, flops, 8 << 20, f"attn_bwd{layer}"
    )


def ffn_forward(layer, n, h, gain, own, other):
    rows, width = h.shape
    hidden = own[0].shape[2]
    args = [h, gain]
    for mine, theirs in zip(own, other):
        args += [mine, theirs]
    specs = [VMEM_SPEC, LOAD] + [HBM_SPEC] * 6
    outs = [
        ((rows, width), BF16, VMEM_SPEC),
        ((rows, width), BF16, HBM_SPEC),
        ((2, n, rows, width), BF16, HBM_SPEC),
        ((n, rows, hidden), F32, HBM_SPEC),
        ((n, rows, hidden), F32, HBM_SPEC),
        ((2, n, rows, hidden // 2), BF16, HBM_SPEC),
    ]
    scratch = (
        [
            VMEM((width, hidden), BF16),
            VMEM((width, hidden), BF16),
            VMEM((hidden, width), BF16),
            VMEM((n, rows, hidden), F32),
            VMEM((n, rows, hidden), F32),
            VMEM((2, n, rows, hidden // 2), BF16),
            VMEM((n, rows, width), F32),
            DMA((3,)),
        ]
        + pair_scratch(n, 5, 2)
        + line_scratch(n, rows, width)
    )
    body = functools.partial(ffn_fwd_kernel, layer, n)
    flops = 6 * n * rows * width * hidden
    return run_kernel(body, args, specs, outs, scratch, 5 + layer, flops, 16 << 20, f"ffn_fwd{layer}")


def ffn_backward(layer, n, dy, h, gain, gate, up, own, other, tasks, df_all):
    rows, width = h.shape
    hidden = own[0].shape[2]
    args = [dy, h, gain, gate, up]
    for mine, theirs in zip(own, other):
        args += [mine, theirs]
    specs = [LOAD_MINE if dy.ndim == 3 else VMEM_SPEC, LOAD, LOAD] + [HBM_SPEC] * 8
    outs = [
        ((rows, width), F32, VMEM_SPEC),
        ((1, width), F32, VMEM_SPEC),
        ((2, n, rows, hidden), BF16, HBM_SPEC),
    ]
    if layer == 1:
        args.append(df_all)
        specs.append(HBM_SPEC)
    else:
        outs.insert(2, ((2, n, rows, width), BF16, HBM_SPEC))
    scratch = (
        [
            VMEM((width, hidden), BF16),
            VMEM((width, hidden), BF16),
            VMEM((hidden, width), BF16),
            VMEM((n, rows, hidden), F32),
            VMEM((n, rows, hidden), F32),
            VMEM((2, n, rows, hidden), BF16),
            VMEM((n, rows, width), F32),
            DMA((3,)),
            DMA((3,)),
        ]
        + pair_scratch(n, 2, 2)
        + line_scratch(n, rows, width)
    )
    body = functools.partial(ffn_bwd_kernel, layer, n)
    flops = 6 * n * rows * width * hidden
    return run_with_tasks(
        body, tasks, args, specs, outs, scratch, 7 + layer, flops, 16 << 20, f"ffn_bwd{layer}"
    )


def run_with_tasks(body, tasks, args, specs, outs, scratch, cid, flops, nbytes, name):
    more_args, more_outs, more_scratch = tasks.arguments(), tasks.outputs(), tasks.scratch()
    sizes = (
        (len(args), len(more_args)),
        (len(outs), len(more_outs)),
        (len(scratch), len(more_scratch)),
    )
    return run_kernel(
        functools.partial(body, tasks, sizes),
        args + more_args,
        specs + [HBM_SPEC] * len(more_args),
        outs + more_outs,
        scratch + more_scratch,
        cid,
        flops,
        nbytes,
        name,
    )


def tail_kernel(n, count, sizes, loads_done, *refs):
    ffn_size, attn_size = sizes
    at = 0

    def take(number):
        nonlocal at
        at += number
        return list(refs[at - number : at])

    gains = take(4)
    rows = take(4)
    ffn_blocks, attn_arrays, _aliased = take(ffn_size), take(attn_size), take(ffn_size + attn_size)
    (gains_out, section_out, in_grad) = take(3)
    ffn_outs, attn_outs = take(ffn_size), take(attn_size)
    by_tensor, by_dp, by_core = take(3)
    small_sems = take(2)
    ffn_vmem, attn_vmem = take(ffn_size), take(attn_size)
    (load_sem,) = take(1)
    ffn_sems, attn_sems, row_sems = take(5), take(5), take(3)
    reduce = Reduce(0, count, attn_arrays, attn_vmem, take(len(refs) - at))
    gather_ffn = Gather(0, count, ffn_vmem, ffn_outs, ffn_sems)
    gather_attn = Gather(0, count, attn_vmem, attn_outs, attn_sems)
    loads = [
        pltpu.make_async_copy(ffn_blocks[a], ffn_vmem[a], load_sem.at[a]) for a in range(ffn_size)
    ]
    for load in loads:
        load.start()
    axes = (("tensor", n, by_tensor), ("dp", count, by_dp), ("section", 2, by_core))
    barrier = pltpu.get_barrier_semaphore()
    peers = 0
    for axis, size, _ in axes:
        place = lax.axis_index(axis)
        for shift in range(1, size):
            pl.semaphore_signal(
                barrier, 1, device_id={axis: (place + shift) % size}, device_id_type=MESH
            )
            peers += 1
    pl.semaphore_wait(barrier, peers)

    def small(stage, shift):
        axis, size, slots = axes[stage]
        place = lax.axis_index(axis)
        ref = slots.at[place]
        return pltpu.make_async_remote_copy(
            ref,
            ref,
            small_sems[0].at[stage, shift],
            small_sems[1].at[stage, shift],
            device_id={axis: (place + shift) % size},
            device_id_type=MESH,
        )

    def small_start(stage, value):
        axis, size, slots = axes[stage]
        slots[lax.axis_index(axis)] = value
        for shift in range(1, size):
            small(stage, shift).start()

    def small_end(stage):
        _, size, slots = axes[stage]
        for shift in range(1, size):
            small(stage, shift).wait()
        value = slots[0]
        for index in range(1, size):
            value = value + slots[index]
        return value

    loads_done()
    small_start(0, jnp.concatenate([gain[...] for gain in gains], axis=0))
    for load in loads:
        load.wait()
    gather_ffn.start()
    reduce.start()
    core = lax.axis_index("section")

    def row_target(index):
        return (section_out, in_grad)[index // 2].at[core]

    def row_keep(index):
        return pltpu.make_async_copy(rows[index], row_target(index), row_sems[0].at[index])

    def row_send(index):
        return pltpu.make_async_remote_copy(
            rows[index],
            row_target(index),
            row_sems[1].at[index],
            row_sems[2].at[index],
            device_id={"section": 1 - core},
            device_id_type=MESH,
        )

    for index in range(4):

        @pl.when(core == index % 2)
        def _():
            row_keep(index).start()

        @pl.when(core != index % 2)
        def _():
            row_send(index).start()

    small_start(1, small_end(0))
    reduce.advance()
    small_start(2, small_end(1))
    gather_ffn.advance()
    reduce.finish()
    gather_attn.start()
    gains_out[...] = small_end(2)
    gather_attn.advance()
    gather_ffn.finish()
    gather_attn.finish()
    for index in range(4):

        @pl.when(core == index % 2)
        def _():
            row_keep(index).wait()
            row_send(index).wait_recv()

        @pl.when(core != index % 2)
        def _():
            row_send(index).wait_send()


def tail(n, count, gains, rows, ffn_blocks, attn_arrays, ffn_full, attn_full):
    sizes = (len(ffn_blocks), len(attn_arrays))
    args = [*gains, *rows, *ffn_blocks, *attn_arrays, *ffn_full, *attn_full]
    specs = [LOAD] * 8 + [HBM_SPEC] * (len(args) - 8)
    together = (4, gains[0].shape[1])
    outs = [(together, F32, VMEM_SPEC)]
    outs += [((2,) + rows[0].shape, BF16, HBM_SPEC)] * 2
    outs += [(full.shape, BF16, HBM_SPEC) for full in (*ffn_full, *attn_full)]
    scratch = [VMEM((size,) + together, F32) for size in (n, count, 2)]
    scratch += [DMA((3, max(n, count, 2)))] * 2
    scratch += [VMEM(block.shape, BF16) for block in ffn_blocks]
    scratch += [VMEM((2,) + array.shape[-2:], BF16) for array in attn_arrays]
    scratch += [DMA((sizes[0],))]
    scratch += gather_sems(count, sizes[0]) + gather_sems(count, sizes[1]) + [DMA((4,))] * 3
    scratch += reduce_scratch(count, [array.shape for array in attn_arrays])
    first = 8 + sizes[0] + sizes[1]
    aliases = {first + index: 3 + index for index in range(sum(sizes))}
    body = functools.partial(tail_kernel, n, count, sizes)
    return run_kernel(body, args, specs, outs, scratch, 9, 1 << 20, 16 << 20, "tail", aliases)


BLOCK = 256


def widen_kernel(mid_in, down_in, qkv_in, out_in, *refs):
    outs, (mid, down, qkv, o), wide, (in_sem, out_sem) = refs[:7], refs[7:11], refs[11:18], refs[18:]
    gate_w, up_w, down_w, q_w, k_w, v_w, out_w = wide
    blocks = mid.shape[1] // BLOCK
    half = mid.shape[2] // 2
    down_rows, out_rows = down.shape[1], o.shape[1]
    q_half, k_half = q_w.shape[1] // 2, k_w.shape[0] // 2

    def part(block):
        return pl.ds(pl.multiple_of(block * BLOCK, BLOCK), BLOCK)

    def mid_load(core, block):
        return pltpu.make_async_copy(
            mid_in.at[core, part(block)], mid.at[core, part(block)], in_sem.at[core, block]
        )

    def whole_load(index):
        source, target = ((down_in, down), (qkv_in, qkv), (out_in, o))[index]
        return pltpu.make_async_copy(
            source.at[pl.ds(0, 2)], target, in_sem.at[2, index]
        )

    def store(index, block=None):
        if block is None:
            return pltpu.make_async_copy(wide[index], outs[index], out_sem.at[index, 0])
        return pltpu.make_async_copy(
            wide[index].at[part(block)], outs[index].at[part(block)], out_sem.at[index, block]
        )

    @pl.loop(0, blocks)
    def _(block):
        for core in range(2):
            mid_load(core, block).start()

    for index in range(3):
        whole_load(index).start()

    @pl.loop(0, blocks)
    def _(block):
        for core in range(2):
            mid_load(core, block).wait()
            lanes = slice(core * half, (core + 1) * half)
            gate_w[part(block), lanes] = mid[core, part(block), :half].astype(F32)
            up_w[part(block), lanes] = mid[core, part(block), half:].astype(F32)
        store(0, block).start()
        store(1, block).start()

    whole_load(0).wait()
    for core in range(2):
        down_w[core * down_rows : (core + 1) * down_rows] = down[core].astype(F32)
    store(2).start()
    whole_load(1).wait()

    @pl.loop(0, qkv.shape[2] // BLOCK)
    def _(block):
        rows = jnp.concatenate(
            [qkv[core, :q_half, part(block)].astype(F32) for core in range(2)], axis=0
        )
        q_w[part(block)] = rows.T

    store(3).start()
    for core in range(2):
        rows = slice(core * k_half, (core + 1) * k_half)
        k_w[rows] = qkv[core, q_half : q_half + k_half].astype(F32)
        v_w[rows] = qkv[core, q_half + k_half :].astype(F32)
    store(4).start()
    store(5).start()
    whole_load(2).wait()
    for core in range(2):
        out_w[core * out_rows : (core + 1) * out_rows] = o[core].astype(F32)
    store(6).start()

    @pl.loop(0, blocks)
    def _(block):
        store(0, block).wait()
        store(1, block).wait()

    for index in range(2, 7):
        store(index).wait()


def widened(g_mid, g_down, g_qkv, g_out, q_size, k_size):
    width, hidden = g_mid.shape[1:]
    shapes = [(width, hidden)] * 2 + [(2 * g_down.shape[1], width), (width, q_size)]
    shapes += [(k_size, width)] * 2 + [(2 * g_out.shape[1], width)]
    blocks = width // BLOCK
    return pl.pallas_call(
        widen_kernel,
        name="widen",
        in_specs=[HBM_SPEC] * 4,
        out_shape=[jax.ShapeDtypeStruct(shape, F32) for shape in shapes],
        out_specs=[HBM_SPEC] * 7,
        scratch_shapes=[VMEM((2,) + array.shape[1:], BF16) for array in (g_mid, g_down, g_qkv, g_out)]
        + [VMEM(shape, F32) for shape in shapes]
        + [DMA((3, max(blocks, 3))), DMA((7, blocks))],
        compiler_params=pltpu.CompilerParams(vmem_limit_bytes=61 << 20),
    )(g_mid, g_down, g_qkv, g_out)


def swap(values):
    return lax.ppermute(values, "section", [(0, 1), (1, 0)])


def segment_tables(lengths_row, n, rows):
    full_rows = n * rows
    slot_count = lengths_row.shape[0]
    seq_ends = jnp.cumsum(lengths_row)
    row_index = jnp.arange(full_rows, dtype=jnp.int32)
    segment = jnp.sum((row_index[:, None] >= seq_ends[None, :]).astype(jnp.int32), axis=1)
    starts = jnp.concatenate([seq_ends - lengths_row, seq_ends[-1:]])
    chosen = segment[:, None] == jnp.arange(slot_count + 1, dtype=jnp.int32)[None, :]
    position = row_index - jnp.sum(jnp.where(chosen, starts[None, :], 0), axis=1)
    segment = jnp.where(segment < slot_count, segment, slot_count + row_index)
    lane = jnp.arange(LANES, dtype=jnp.int32)
    inner = lane % (LANES // 2)
    inverse = rope_base ** (-inner.astype(F32) * 2.0 / HEAD)
    angle = position.astype(F32)[:, None] * inverse[None, :]
    live = (inner < HALF)[None, :]
    sign = jnp.where(lane < LANES // 2, -1.0, 1.0)[None, :]
    cosine = jnp.where(live, jnp.cos(angle), 0.0)
    sine = jnp.where(live, sign * jnp.sin(angle), 0.0)
    shape = (n, rows, LANES)
    return cosine.reshape(shape), sine.reshape(shape), segment[:, None], segment[None, :]


def shards(
    inputs,
    cotangent,
    seq_lengths,
    gain_attn,
    w_query,
    w_key,
    w_value,
    w_out,
    gain_ffn,
    w_gate,
    w_up,
    w_down,
):
    section = lax.axis_index("section")
    first = section == 0
    n = lax.axis_size("tensor")
    rows = inputs.shape[1]
    attn_own = (w_query, jnp.swapaxes(w_key, 1, 2), jnp.swapaxes(w_value, 1, 2), w_out)
    ffn_own = (w_gate, w_up, w_down)
    gains = jnp.concatenate([gain_attn, gain_ffn], axis=0)
    gains_other = swap(gains)
    gains_by_layer = [
        jnp.where(first, gains, gains_other).astype(F32),
        jnp.where(first, gains_other, gains).astype(F32),
    ]
    tables = segment_tables(jnp.where(first, seq_lengths[0, 0], seq_lengths[0, 1]), n, rows)

    x = x_saved = inputs
    kept = []
    outs = []
    for layer in range(2):
        gain_a, gain_f = gains_by_layer[layer][0:1], gains_by_layer[layer][1:2]
        if layer == 0:
            h, h_saved, n_all, qkv, o, *swapped = attn_forward(
                layer, n, x, gain_a, tables, attn_own + ffn_own, None, None
            )
            attn_other, ffn_other = tuple(swapped[:4]), tuple(swapped[4:])
        else:
            h, h_saved, n_all, qkv, o, df_ahead = attn_forward(
                layer, n, x, gain_a, tables, attn_own, attn_other, cotangent
            )
        y, y_saved, n2_all, gate, up, hid = ffn_forward(layer, n, h, gain_f, ffn_own, ffn_other)
        kept.append((x_saved, h_saved, n_all, qkv, o, n2_all, gate, up, hid, gain_a, gain_f))
        outs.append(y_saved)
        x, x_saved = y, y_saved

    count = lax.axis_size("dp")
    cube = (2,) + (2,) * (count.bit_length() - 1)

    def weight_grad(left, right):
        left = left.reshape(-1, left.shape[-1])
        right = right.reshape(-1, right.shape[-1])
        return dot_tn(left, right).astype(BF16)

    def blocked(array):
        return array.reshape(*cube, -1, array.shape[-1])

    dy = cotangent
    in_grads = [None, None]
    gain_parts = [None, None]
    for layer in (1, 0):
        x, h, n_all, qkv, o, n2_all, gate, up, hid, gain_a, gain_f = kept[layer]
        if layer == 1:
            g_down = blocked(weight_grad(hid, df_ahead))
            plan = {"reduce": (1, [g_down])}
            dh, gf_part, dmid, sum_down = ffn_backward(
                layer, n, dy, h, gain_f, gate, up, ffn_own, ffn_other, Tasks(count, plan), df_ahead
            )
            g_mid = blocked(weight_grad(n2_all, dmid))
            plan = {"reduce": (1, [g_mid]), "gather": (1, [sum_down])}
        else:
            plan = {"reduce": (1, attn_grad), "gather": (1, [sum_mid])}
            dh, gf_part, df_all, dmid, *sum_attn, mid_full = ffn_backward(
                layer, n, dy, h, gain_f, gate, up, ffn_own, ffn_other, Tasks(count, plan), None
            )
            g_mid, g_down = blocked(weight_grad(n2_all, dmid)), blocked(weight_grad(hid, df_all))
            plan = {"reduce": (0, [g_mid, g_down]), "gather": (1, sum_attn)}
        dx, dx_saved, ga_part, da_all, dqkv, *more = attn_backward(
            layer, n, dh, x, gain_a, tables, qkv, attn_own, attn_other, Tasks(count, plan)
        )
        if layer == 1:
            sum_mid, down_full = more
        else:
            sum_ffn, attn_full = more[:2], more[2:]
        attn_grad = [blocked(weight_grad(dqkv, n_all)), blocked(weight_grad(o, da_all))]
        gain_parts[layer] = [ga_part, gf_part]
        in_grads[layer] = dx_saved
        dy = dx
    gain_sums, section_out, in_grad, g_mid, g_down, g_qkv, g_out = tail(
        n,
        count,
        gain_parts[0] + gain_parts[1],
        outs + in_grads,
        sum_ffn,
        attn_grad,
        [mid_full, down_full],
        attn_full,
    )
    gain_own = jnp.where(first, gain_sums[0:2], gain_sums[2:4])
    g_mid, g_down, g_qkv, g_out = (
        array.reshape(array.shape[0], -1, array.shape[-1])
        for array in (g_mid, g_down, g_qkv, g_out)
    )
    g_gate, g_up, g_down, g_query, g_key, g_value, g_out = (
        grad[None] for grad in widened(g_mid, g_down, g_qkv, g_out, w_query.shape[2], w_key.shape[2])
    )
    g_key, g_value = jnp.swapaxes(g_key, 1, 2), jnp.swapaxes(g_value, 1, 2)
    return (
        section_out[None],
        in_grad[None],
        gain_own[0:1],
        g_query,
        g_key,
        g_value,
        g_out,
        gain_own[1:2],
        g_gate,
        g_up,
        g_down,
    )


def solution(mesh):
    placed = (
        P(None, ("dp", "tensor"), None),
        P(None, ("dp", "tensor"), None),
        P("dp", None, None),
        P("section", None),
        P("section", None, "tensor"),
        P("section", None, "tensor"),
        P("section", None, "tensor"),
        P("section", "tensor", None),
        P("section", None),
        P("section", None, "tensor"),
        P("section", None, "tensor"),
        P("section", "tensor", None),
    )
    return jax.shard_map(
        shards,
        mesh=mesh,
        in_specs=placed,
        out_specs=(
            P("section", None, ("dp", "tensor"), None),
            P("section", None, ("dp", "tensor"), None),
            P("section", None),
            P("section", None, "tensor"),
            P("section", None, "tensor"),
            P("section", None, "tensor"),
            P("section", "tensor", None),
            P("section", None),
            P("section", None, "tensor"),
            P("section", None, "tensor"),
            P("section", "tensor", None),
        ),
        check_vma=False,
    )
```
